8 devices in a mesh: dp: 1 (over z), cp: 8 (over y, x, core).
Axes of the slice: x: 2, y: 2, z: 1, core: 2. Of those that a mesh axis runs over, the one named last changes fastest.
Arguments:
- q_tok: bfloat16 [8192, 2, 128], P(('dp', 'cp'))
- k_tok: bfloat16 [8192, 128], P(('dp', 'cp'))
- v_tok: bfloat16 [8192, 128], P(('dp', 'cp'))
- fwd_out: bfloat16 [8192, 2, 128], P(('dp', 'cp'))
- d_out: bfloat16 [8192, 2, 128], P(('dp', 'cp'))
- lse_row: float32 [8192, 2], P(('dp', 'cp'))
Outputs:
- output 1: bfloat16 [8192, 2, 128], P(('dp', 'cp'))
- output 2: bfloat16 [8192, 128], P(('dp', 'cp'))
- output 3: bfloat16 [8192, 128], P(('dp', 'cp'))
All inputs are finite; a program needn't handle non-finite values.
Results may differ from the reference program's by a relative error of at most 0.001.
Values are sent between devices in bfloat16 or wider.
A program may use at most 1 GiB of HBM per device.

```python
import jax
import jax.numpy as jnp
from jax import lax

TOK_DEV = 1024
CP = 8
GQA = 2
HEAD = 128

SEQ = CP * TOK_DEV
Q_BLOCK = min(TOK_DEV, 128)
SOFTMAX_SCALE = HEAD ** -0.5
GRAD_GAIN = 0.25 * SEQ ** 0.5


def attention_forward(q_tok, k_tok, v_tok):
    k_full = k_tok.astype(jnp.float32)
    v_full = v_tok.astype(jnp.float32)
    columns = jnp.arange(SEQ)
    n_blocks = SEQ // Q_BLOCK

    def one_block(block_in):
        q_block, row_ids = block_in
        logits = jnp.einsum('rgd,cd->rgc', q_block.astype(jnp.float32), k_full) * SOFTMAX_SCALE
        allowed = columns[None, :] <= row_ids[:, None]
        logits = jnp.where(allowed[:, None, :], logits, -jnp.inf)
        lse_block = jax.nn.logsumexp(logits, axis=-1)
        prob_mat = jnp.exp(logits - lse_block[:, :, None])
        out_block = jnp.einsum('rgc,cd->rgd', prob_mat, v_full)
        return out_block.astype(jnp.bfloat16), lse_block

    out_blocks, lse_blocks = lax.map(one_block, (q_tok.reshape(n_blocks, Q_BLOCK, GQA, HEAD), columns.reshape(n_blocks, Q_BLOCK)))
    return out_blocks.reshape(SEQ, GQA, HEAD), lse_blocks.reshape(SEQ, GQA)


def setup_inputs(seed: int = 0, part: int = 0) -> dict:
    base_key = jax.random.fold_in(jax.random.key(seed), part)
    key_q, key_k, key_v, key_m, key_g = jax.random.split(base_key, 5)
    q_tok = jax.random.normal(key_q, (SEQ, GQA, HEAD), jnp.float32).astype(jnp.bfloat16)
    k_tok = jax.random.normal(key_k, (SEQ, HEAD), jnp.float32).astype(jnp.bfloat16)
    v_mean = jax.random.normal(key_m, (HEAD,), jnp.float32)
    v_tok = (v_mean[None, :] + jax.random.normal(key_v, (SEQ, HEAD), jnp.float32)).astype(jnp.bfloat16)
    d_out = (GRAD_GAIN * jax.random.normal(key_g, (SEQ, GQA, HEAD), jnp.float32)).astype(jnp.bfloat16)
    fwd_out, lse_row = attention_forward(q_tok, k_tok, v_tok)
    return {'q_tok': q_tok, 'k_tok': k_tok, 'v_tok': v_tok, 'fwd_out': fwd_out, 'd_out': d_out, 'lse_row': lse_row}


def reference(q_tok, k_tok, v_tok, fwd_out, d_out, lse_row):
    row_delta = jnp.sum(d_out.astype(jnp.float32) * fwd_out.astype(jnp.float32), axis=-1)
    k_full = k_tok.astype(jnp.float32)
    v_full = v_tok.astype(jnp.float32)
    columns = jnp.arange(SEQ)
    n_blocks = SEQ // Q_BLOCK

    def one_block(carry, block_in):
        dk_acc, dv_acc = carry
        q_block, do_block, lse_block, delta_block, row_ids = block_in
        q_wide = q_block.astype(jnp.float32)
        do_wide = do_block.astype(jnp.float32)
        logits = jnp.einsum('rgd,cd->rgc', q_wide, k_full) * SOFTMAX_SCALE
        allowed = columns[None, :] <= row_ids[:, None]
        prob_mat = jnp.exp(jnp.where(allowed[:, None, :], logits - lse_block[:, :, None], -jnp.inf))
        d_prob = jnp.einsum('rgd,cd->rgc', do_wide, v_full)
        d_score = prob_mat * (d_prob - delta_block[:, :, None])
        prob_low = prob_mat.astype(jnp.bfloat16).astype(jnp.float32)
        score_low = d_score.astype(jnp.bfloat16).astype(jnp.float32)
        dq_block = jnp.einsum('rgc,cd->rgd', score_low, k_full) * SOFTMAX_SCALE
        dk_acc = dk_acc + jnp.einsum('rgc,rgd->cd', score_low, q_wide)
        dv_acc = dv_acc + jnp.einsum('rgc,rgd->cd', prob_low, do_wide)
        return (dk_acc, dv_acc), dq_block.astype(jnp.bfloat16)

    acc_start = (jnp.zeros((SEQ, HEAD), jnp.float32), jnp.zeros((SEQ, HEAD), jnp.float32))
    block_inputs = (q_tok.reshape(n_blocks, Q_BLOCK, GQA, HEAD), d_out.reshape(n_blocks, Q_BLOCK, GQA, HEAD), lse_row.reshape(n_blocks, Q_BLOCK, GQA), row_delta.reshape(n_blocks, Q_BLOCK, GQA), columns.reshape(n_blocks, Q_BLOCK))
    (dk_acc, dv_acc), dq_blocks = lax.scan(one_block, acc_start, block_inputs)
    grad_q = dq_blocks.reshape(SEQ, GQA, HEAD)
    grad_k = (dk_acc * SOFTMAX_SCALE).astype(jnp.bfloat16)
    grad_v = dv_acc.astype(jnp.bfloat16)
    return (grad_q, grad_k, grad_v)
```

```python
import functools
import math

import jax
import jax.numpy as jnp
from jax import lax
from jax.experimental import pallas as pl
from jax.experimental.pallas import tpu as pltpu
from jax.sharding import PartitionSpec as P

BF16, F32 = jnp.bfloat16, jnp.float32
NT = (((1,), (1,)), ((), ()))
CHUNKS = 4
COLS = 256


def dot(a, b):
    return jnp.dot(a, b, preferred_element_type=F32)


def dot_nt(a, b):
    return lax.dot_general(a, b, NT, preferred_element_type=F32)


def kernel(rows, keys, head, q_hbm, k_hbm, v_hbm, o_hbm, do_hbm, lse_hbm, dq_ref, dk_ref, dv_ref,
           qbuf, kvbuf, obuf, auxr, own_aux, chunk_aux, k_one, v_one, q_t, do_t, dq_acc, dk_t, dv_t,
           stage_sem, recv_sem, aux_recv, own_send, own_aux_send, pair_send, pair_aux_send,
           x_send, y_send, x_aux_send):
    me = lax.axis_index('cp')
    core, px, py = me % 2, (me // 2) % 2, me // 4
    pair = me + 1 - 2 * core
    nx = me + 2 - 4 * px
    ny = me + 4 - 8 * py
    diag = nx + 4 - 8 * py
    other = pair - me
    mid = (px + py) == 1
    qc, kc = rows // CHUNKS, keys // CHUNKS
    scale = head ** -0.5
    exp_scale = scale * math.log2(math.e)

    def q_copy(slot, n, dest, send, recv):
        part = pl.ds(n * qc, qc)
        return pltpu.make_async_remote_copy(
            qbuf.at[slot, :, part], qbuf.at[slot, :, part], send, recv,
            device_id={'cp': dest}, device_id_type=pl.DeviceIdType.MESH)

    def kv_copy(slot, n, dest, send, recv):
        part = pl.ds(n * kc, kc)
        return pltpu.make_async_remote_copy(
            kvbuf.at[slot, :, part], kvbuf.at[slot, :, part], send, recv,
            device_id={'cp': dest}, device_id_type=pl.DeviceIdType.MESH)

    def aux_copy(slot, dest, send):
        return pltpu.make_async_remote_copy(
            auxr.at[slot], auxr.at[slot], send, aux_recv.at[slot],
            device_id={'cp': dest}, device_id_type=pl.DeviceIdType.MESH)

    stages = [
        pltpu.make_async_copy(k_hbm, kvbuf.at[me, 0], stage_sem.at[0]),
        pltpu.make_async_copy(v_hbm, kvbuf.at[me, 1], stage_sem.at[1]),
        pltpu.make_async_copy(q_hbm, qbuf.at[me, 0], stage_sem.at[2]),
        pltpu.make_async_copy(do_hbm, qbuf.at[me, 1], stage_sem.at[3]),
        pltpu.make_async_copy(o_hbm, obuf, stage_sem.at[4]),
        pltpu.make_async_copy(lse_hbm, auxr.at[me, :, pl.ds(0, 4)], stage_sem.at[5]),
    ]
    for s in stages:
        s.start()

    barrier = pltpu.get_barrier_semaphore()
    for dest in (pair, nx, ny):
        pl.semaphore_signal(barrier, inc=1, device_id={'cp': dest}, device_id_type=pl.DeviceIdType.MESH)
    pl.semaphore_wait(barrier, 3)

    def order(d, n):
        return (n + 2) % CHUNKS if d == 1 else n

    dests = (pair, nx, ny)
    for s in stages[:4]:
        s.wait()
    for d, dest in enumerate(dests):
        @pl.when(dest > me)
        def _():
            for n in range(CHUNKS):
                c = order(d, n)
                kv_copy(me, c, dest, own_send.at[d, c], recv_sem.at[me, c]).start()

        @pl.when(dest < me)
        def _():
            c = order(d, 0)
            q_copy(me, c, dest, own_send.at[d, c], recv_sem.at[me, c]).start()

    lane = lax.broadcasted_iota(jnp.int32, (COLS, head), 1)
    k_one[...] = jnp.where(lane < 3, -1.0, 0.0).astype(BF16)
    v_one[...] = jnp.where((lane >= 3) & (lane < 6), -1.0, 0.0).astype(BF16)
    dq_acc[...] = jnp.zeros_like(dq_acc)
    dk_t[...] = jnp.zeros_like(dk_t)
    dv_t[...] = jnp.zeros_like(dv_t)
    for s in stages[4:]:
        s.wait()

    def delta_rows(n, _):
        auxr[me, n, 0:4] = auxr[me, n, 0:4] * (1.0 / scale)
        for g in range(qc // 128):
            part = pl.ds(pl.multiple_of(n * qc + g * 128, 128), 128)
            d = jnp.sum(qbuf[me, 1, part].astype(F32) * obuf[part].astype(F32), axis=1, keepdims=True)
            auxr[me, n, 4 + g:5 + g] = jnp.transpose(jnp.broadcast_to(d, (128, 128)))[0:1]
        return 0

    lax.fori_loop(0, CHUNKS, delta_rows, 0)

    def fill_aux(slot, n, dst, base):
        a = auxr[slot, n]
        hi = a.astype(BF16).astype(F32)
        r = a - hi
        md = r.astype(BF16).astype(F32)
        lo = r - md
        sub = lax.broadcasted_iota(jnp.int32, (8, 128), 0)
        for g in range(qc // 128):
            m = jnp.zeros((8, 128), F32)
            for i, row in enumerate((hi[g:g + 1], md[g:g + 1], lo[g:g + 1],
                                     hi[4 + g:5 + g], md[4 + g:5 + g], lo[4 + g:5 + g])):
                m = jnp.where(sub == i, row, m)
            m = jnp.concatenate([m, jnp.zeros((120, 128), F32)], axis=0)
            dst[pl.ds(base + g * 128, 128)] = jnp.transpose(m).astype(BF16)

    def own_fill(n, _):
        fill_aux(me, n, own_aux, pl.multiple_of(n * qc, 128))
        return 0

    lax.fori_loop(0, CHUNKS, own_fill, 0)

    def scores(q, do, aux, k, v):
        s = dot_nt(jnp.concatenate([q, aux], axis=1), jnp.concatenate([k, k_one[...]], axis=1))
        p = jnp.exp2(s * exp_scale)
        d = dot_nt(jnp.concatenate([do, aux], axis=1), jnp.concatenate([v, v_one[...]], axis=1))
        return p, d

    for rb in range(CHUNKS):
        rpart = pl.ds(rb * qc, qc)
        q, do, aux = qbuf[me, 0, rpart], qbuf[me, 1, rpart], own_aux[rpart]
        qt, dot_ = jnp.transpose(q), jnp.transpose(do)
        dq = None
        for cb in range(rb + 1):
            cpart = pl.ds(cb * kc, kc)
            k, v = kvbuf[me, 0, cpart], kvbuf[me, 1, cpart]
            p, d = scores(q, do, aux, k, v)
            if cb == rb:
                row = lax.broadcasted_iota(jnp.int32, (qc, kc), 0)
                col = lax.broadcasted_iota(jnp.int32, (qc, kc), 1)
                p = jnp.where(2 * col <= row, p, 0.0)
            ds = (p * d).astype(BF16)
            dv_t[:, cpart] += dot(dot_, p.astype(BF16))
            dk_t[:, cpart] += dot(qt, ds)
            term = dot(ds, k)
            dq = term if dq is None else dq + term
        dq_acc[rpart] = dq

    for d, dest in enumerate(dests):
        @pl.when(dest < me)
        def _():
            aux_copy(me, dest, own_aux_send.at[d]).start()
            for n in range(1, CHUNKS):
                c = order(d, n)
                q_copy(me, c, dest, own_send.at[d, c], recv_sem.at[me, c]).start()

    def plan(t):
        ta, tb = t - 4, t - 20
        na, ka = ta // 4, ta % 4
        nb, kb = tb // 2, tb % 2
        first, second = t < 4, t < 20
        dn = jnp.where(mid, nb, (nb % 2) * 2 + nb // 2)
        n = jnp.where(first, t, jnp.where(second, na, nb))
        src_a = jnp.where(ka % 2 == 0, nx, ny) + jnp.where(ka >= 2, other, 0)
        src_b = diag + jnp.where(kb == 1, other, 0)
        src = jnp.where(first, pair, jnp.where(second, src_a, src_b))
        pa = jnp.where(ka % 2 == 0, (na + 2) % CHUNKS, na)
        piece = jnp.where(first, t, jnp.where(second, pa, dn))
        stream = jnp.where(first, 3, jnp.where(second, jnp.where(ka < 2, ka, 3), jnp.where(kb == 0, 2, 3)))
        return stream, src, piece, n

    def forwards(stream, piece):
        to_pair = stream < 3
        to_x = (stream == 1) & (jnp.logical_not(mid) | (piece < 2))
        to_y = (stream == 0) & mid & (piece >= 2)
        return to_pair, to_x, to_y

    def step(t, _):
        stream, src, piece, n = plan(t)
        to_pair, to_x, to_y = forwards(stream, piece)
        idx = jnp.minimum(stream, 2)
        recv = recv_sem.at[src, piece]

        @pl.when(src > me)
        def _():
            @pl.when(n == 0)
            def _():
                aux_copy(src, me, own_aux_send.at[0]).wait_recv()

                @pl.when(to_pair)
                def _():
                    aux_copy(src, pair, pair_aux_send.at[idx]).start()

                @pl.when(to_x)
                def _():
                    aux_copy(src, nx, x_aux_send).start()

            q_copy(src, piece, me, x_send.at[piece], recv).wait_recv()

            @pl.when(to_x)
            def _():
                q_copy(src, piece, nx, x_send.at[piece], recv).start()

            @pl.when(to_y)
            def _():
                q_copy(src, piece, ny, y_send.at[piece], recv).start()

            @pl.when(to_pair)
            def _():
                q_copy(src, piece, pair, pair_send.at[idx, piece], recv).start()

            fill_aux(src, piece, chunk_aux, 0)
            rpart = pl.ds(pl.multiple_of(piece * qc, qc), qc)
            q, do, aux = qbuf[src, 0, rpart], qbuf[src, 1, rpart], chunk_aux[...]
            q_t[...] = jnp.transpose(q)
            do_t[...] = jnp.transpose(do)
            for cb in range(keys // COLS):
                cpart = pl.ds(cb * COLS, COLS)
                p, d = scores(q, do, aux, kvbuf[me, 0, cpart], kvbuf[me, 1, cpart])
                ds = (p * d).astype(BF16)
                dv_t[:, cpart] += dot(do_t[...], p.astype(BF16))
                dk_t[:, cpart] += dot(q_t[...], ds)

        @pl.when(src < me)
        def _():
            kv_copy(src, piece, me, x_send.at[piece], recv).wait_recv()

            @pl.when(to_x)
            def _():
                kv_copy(src, piece, nx, x_send.at[piece], recv).start()

            @pl.when(to_y)
            def _():
                kv_copy(src, piece, ny, y_send.at[piece], recv).start()

            @pl.when(to_pair)
            def _():
                kv_copy(src, piece, pair, pair_send.at[idx, piece], recv).start()

            cpart = pl.ds(pl.multiple_of(piece * kc, kc), kc)
            k, v = kvbuf[src, 0, cpart], kvbuf[src, 1, cpart]
            for rb in range(CHUNKS):
                rpart = pl.ds(rb * qc, qc)
                p, d = scores(qbuf[me, 0, rpart], qbuf[me, 1, rpart], own_aux[rpart], k, v)
                ds = (p * d).astype(BF16)
                dq_acc[rpart] += dot(ds, k)

        return 0

    lax.fori_loop(0, 28, step, 0)

    dq_ref[...] = (dq_acc[...] * scale).astype(BF16)
    dk_ref[...] = (jnp.transpose(dk_t[...]) * scale).astype(BF16)
    dv_ref[...] = jnp.transpose(dv_t[...]).astype(BF16)

    for d, dest in enumerate(dests):
        @pl.when(dest > me)
        def _():
            for c in range(CHUNKS):
                kv_copy(me, c, dest, own_send.at[d, c], recv_sem.at[me, c]).wait_send()

        @pl.when(dest < me)
        def _():
            aux_copy(me, dest, own_aux_send.at[d]).wait_send()
            for c in range(CHUNKS):
                q_copy(me, c, dest, own_send.at[d, c], recv_sem.at[me, c]).wait_send()

    def drain(t, _):
        stream, src, piece, n = plan(t)
        to_pair, to_x, to_y = forwards(stream, piece)
        idx = jnp.minimum(stream, 2)
        recv = recv_sem.at[src, piece]
        for make, is_q in ((q_copy, True), (kv_copy, False)):
            @pl.when((src > me) if is_q else (src < me))
            def _():
                @pl.when(to_x)
                def _():
                    make(src, piece, nx, x_send.at[piece], recv).wait_send()

                @pl.when(to_y)
                def _():
                    make(src, piece, ny, y_send.at[piece], recv).wait_send()

                @pl.when(to_pair)
                def _():
                    make(src, piece, pair, pair_send.at[idx, piece], recv).wait_send()

                if is_q:
                    @pl.when((n == 0) & to_pair)
                    def _():
                        aux_copy(src, pair, pair_aux_send.at[idx]).wait_send()

                    @pl.when((n == 0) & to_x)
                    def _():
                        aux_copy(src, nx, x_aux_send).wait_send()
        return 0

    lax.fori_loop(4, 28, drain, 0)


def solution(mesh):
    n_dev = mesh.shape['cp']
    row_spec = P(('dp', 'cp'))

    def local_fn(q_tok, k_tok, v_tok, fwd_out, d_out, lse_row):
        tokens, groups, head = q_tok.shape
        rows = tokens * groups
        flat = lambda x: x.reshape(rows, head)
        lse = lse_row.reshape(CHUNKS, rows // CHUNKS // 128, 128)
        dma = pltpu.SemaphoreType.DMA
        grad_q, grad_k, grad_v = pl.pallas_call(
            functools.partial(kernel, rows, tokens, head),
            out_shape=(jax.ShapeDtypeStruct((rows, head), BF16),
                       jax.ShapeDtypeStruct((tokens, head), BF16),
                       jax.ShapeDtypeStruct((tokens, head), BF16)),
            in_specs=[pl.BlockSpec(memory_space=pl.ANY)] * 6,
            out_specs=(pl.BlockSpec(memory_space=pltpu.VMEM),) * 3,
            scratch_shapes=[
                pltpu.VMEM((n_dev, 2, rows, head), BF16),
                pltpu.VMEM((n_dev, 2, tokens, head), BF16),
                pltpu.VMEM((rows, head), BF16),
                pltpu.VMEM((n_dev, CHUNKS, 8, 128), F32),
                pltpu.VMEM((rows, head), BF16),
                pltpu.VMEM((rows // CHUNKS, head), BF16),
                pltpu.VMEM((COLS, head), BF16),
                pltpu.VMEM((COLS, head), BF16),
                pltpu.VMEM((head, rows // CHUNKS), BF16),
                pltpu.VMEM((head, rows // CHUNKS), BF16),
                pltpu.VMEM((rows, head), F32),
                pltpu.VMEM((head, tokens), F32),
                pltpu.VMEM((head, tokens), F32),
                dma((6,)),
                dma((n_dev, CHUNKS)),
                dma((n_dev,)),
                dma((3, CHUNKS)),
                dma((3,)),
                dma((3, CHUNKS)),
                dma((3,)),
                dma((CHUNKS,)),
                dma((CHUNKS,)),
                dma,
            ],
            compiler_params=pltpu.CompilerParams(
                collective_id=0, has_side_effects=True),
            name='attention_backward',
        )(flat(q_tok), k_tok, v_tok, flat(fwd_out), flat(d_out), lse)
        return grad_q.reshape(tokens, groups, head), grad_k, grad_v

    return jax.shard_map(local_fn, mesh=mesh, in_specs=(row_spec,) * 6, out_specs=(row_spec,) * 3, check_vma=False)
```

```python
import functools
import math

import jax
import jax.numpy as jnp
from jax import lax
from jax.experimental import pallas as pl
from jax.experimental.pallas import tpu as pltpu
from jax.sharding import PartitionSpec as P

BF16, F32 = jnp.bfloat16, jnp.float32
CHUNKS = 4
COLS = 256
STEPS = 14
MESH = pl.DeviceIdType.MESH


def dot(a, b):
    return jnp.dot(a, b, preferred_element_type=F32)


def beside(a, b):
    return jnp.concatenate([a, b], axis=1)


def parts(x):
    hi = x.astype(BF16).astype(F32)
    rest = x - hi
    md = rest.astype(BF16).astype(F32)
    return hi, md, rest - md


def kernel(rows, keys, head, n_dev, q_hbm, k_hbm, v_hbm, o_hbm, do_hbm, lse_hbm, dq_ref, dk_ref, dv_ref,
           qbuf, kvbuf, obuf, lse_in, auxr, own_aux, chunk_aux, k_one, v_one, own_qt, own_dot, own_kt, own_vt,
           q_t, do_t, dq_acc, dq_t, dk_t, dv_t,
           stage_sem, recv_sem, aux_recv, own_send, own_aux_send, pair_send, x_send, y_send):
    me = lax.axis_index('cp')
    core, px, py = me % 2, (me // 2) % 2, me // 4
    pair = me + 1 - 2 * core
    nx = me + 2 - 4 * px
    ny = me + 4 - 8 * py
    diag = nx + 4 - 8 * py
    other = pair - me
    mid = (px + py) == 1
    qc, kc = rows // CHUNKS, keys // CHUNKS
    scale = head ** -0.5
    exp_scale = scale * math.log2(math.e)

    def q_copy(slot, n, dest, send, recv):
        part = pl.ds(n * qc, qc)
        return pltpu.make_async_remote_copy(
            qbuf.at[slot, :, part], qbuf.at[slot, :, part], send, recv,
            device_id={'cp': dest}, device_id_type=MESH)

    def kv_copy(slot, n, dest, send, recv):
        part = pl.ds(n * kc, kc)
        return pltpu.make_async_remote_copy(
            kvbuf.at[slot, :, part], kvbuf.at[slot, :, part], send, recv,
            device_id={'cp': dest}, device_id_type=MESH)

    def aux_copy(slot, dest, send):
        return pltpu.make_async_remote_copy(
            auxr.at[slot], auxr.at[slot], send, aux_recv.at[slot],
            device_id={'cp': dest}, device_id_type=MESH)

    stages = [
        pltpu.make_async_copy(k_hbm, kvbuf.at[me, 0], stage_sem.at[0]),
        pltpu.make_async_copy(v_hbm, kvbuf.at[me, 1], stage_sem.at[1]),
        pltpu.make_async_copy(q_hbm, qbuf.at[me, 0], stage_sem.at[2]),
        pltpu.make_async_copy(do_hbm, qbuf.at[me, 1], stage_sem.at[3]),
        pltpu.make_async_copy(o_hbm, obuf, stage_sem.at[4]),
        pltpu.make_async_copy(lse_hbm, lse_in, stage_sem.at[5]),
    ]
    for s in stages:
        s.start()

    barrier = pltpu.get_barrier_semaphore()
    for peer in range(n_dev):
        @pl.when(peer != me)
        def _():
            pl.semaphore_signal(barrier, inc=1, device_id={'cp': peer}, device_id_type=MESH)
    pl.semaphore_wait(barrier, n_dev - 1)

    def order(d, n):
        return (n + 2) % CHUNKS if d == 1 else n

    dests = (pair, nx, ny)
    for s in stages[:4]:
        s.wait()
    for d, dest in enumerate(dests):
        @pl.when(dest > me)
        def _():
            for n in range(CHUNKS):
                c = order(d, n)
                kv_copy(me, c, dest, own_send.at[d, c], recv_sem.at[me, c]).start()

        @pl.when(dest < me)
        def _():
            c = order(d, 0)
            q_copy(me, c, dest, own_send.at[d, c], recv_sem.at[me, c]).start()

    for s in stages[4:]:
        s.wait()

    at_row = lax.broadcasted_iota(jnp.int32, (COLS, COLS), 0)
    at_col = lax.broadcasted_iota(jnp.int32, (COLS, COLS), 1)
    weave = jnp.where(at_col == 2 * (at_row % 128) + at_row // 128, 1.0, 0.0).astype(BF16)
    sub = lax.broadcasted_iota(jnp.int32, (16, 128), 0)
    for g in range(rows // 256):
        sides = []
        for h in range(2):
            row = lse_in[h:h + 1, g * 128:(g + 1) * 128] * (1.0 / scale)
            hi, md, lo = parts(row)
            sides.append(jnp.where(sub == 0, hi, jnp.where(sub == 1, md, jnp.where(sub == 2, lo, 0.0))))
        woven = dot(beside(*sides).astype(BF16), weave)
        row = woven[0:1] + (woven[1:2] + woven[2:3])
        n, at = g // 2, (g % 2) * 2
        auxr[me, n, at:at + 1] = row[:, 0:128]
        auxr[me, n, at + 1:at + 2] = row[:, 128:256]

    def delta_rows(n, _):
        for g in range(qc // 128):
            part = pl.ds(pl.multiple_of(n * qc + g * 128, 128), 128)
            d = jnp.sum(qbuf[me, 1, part].astype(F32) * obuf[part].astype(F32), axis=1, keepdims=True)
            auxr[me, n, 4 + g:5 + g] = jnp.transpose(jnp.broadcast_to(d, (128, 128)))[0:1]
        return 0

    lax.fori_loop(0, CHUNKS, delta_rows, 0)

    def aux_lines(slot, n):
        hi, md, lo = parts(auxr[slot, n])
        sub = lax.broadcasted_iota(jnp.int32, (8, 128), 0)
        lines = []
        for g in range(qc // 128):
            m = jnp.zeros((8, 128), F32)
            for i, row in enumerate((hi[g:g + 1], md[g:g + 1], lo[g:g + 1],
                                     hi[4 + g:5 + g], md[4 + g:5 + g], lo[4 + g:5 + g])):
                m = jnp.where(sub == i, row, m)
            lines.append(jnp.concatenate([m, jnp.zeros((120, 128), F32)], axis=0))
        return lines

    def fill_aux(slot, n, dst, base):
        for g, m in enumerate(aux_lines(slot, n)):
            dst[pl.ds(base + g * 128, 128)] = jnp.transpose(m).astype(BF16)

    lane = lax.broadcasted_iota(jnp.int32, (COLS, head), 1)
    line = lax.broadcasted_iota(jnp.int32, (head, keys), 0)
    k_one[...] = jnp.where(lane < 3, -1.0, 0.0).astype(BF16)
    v_one[...] = jnp.where((lane >= 3) & (lane < 6), -1.0, 0.0).astype(BF16)
    own_kt[head:] = jnp.where(line < 3, -1.0, 0.0).astype(BF16)
    own_vt[head:] = jnp.where((line >= 3) & (line < 6), -1.0, 0.0).astype(BF16)
    dk_t[...] = jnp.zeros_like(dk_t)
    dv_t[...] = jnp.zeros_like(dv_t)
    dq_t[...] = jnp.zeros_like(dq_t)

    def own_fill(n, _):
        base = pl.multiple_of(n * qc, 128)
        part, kpart = pl.ds(base, qc), pl.ds(pl.multiple_of(n * kc, 128), kc)
        for g, m in enumerate(aux_lines(me, n)):
            at = pl.ds(pl.multiple_of(base + g * 128, 128), 128)
            own_aux[at] = jnp.transpose(m).astype(BF16)
            own_qt[head:, at] = m.astype(BF16)
            own_dot[head:, at] = m.astype(BF16)
        own_qt[:head, part] = jnp.transpose(qbuf[me, 0, part])
        own_dot[:head, part] = jnp.transpose(qbuf[me, 1, part])
        own_kt[:head, kpart] = jnp.transpose(kvbuf[me, 0, kpart])
        own_vt[:head, kpart] = jnp.transpose(kvbuf[me, 1, kpart])
        return 0

    lax.fori_loop(0, CHUNKS, own_fill, 0)

    for rb in range(CHUNKS):
        rpart = pl.ds(rb * qc, qc)
        aux = own_aux[rpart]
        q, do = beside(qbuf[me, 0, rpart], aux), beside(qbuf[me, 1, rpart], aux)
        dq = None
        for cb in range(rb + 1):
            cpart = pl.ds(cb * kc, kc)
            p = jnp.exp2(dot(q, own_kt[:, cpart]) * exp_scale)
            d = dot(do, own_vt[:, cpart])
            if cb == rb:
                row = lax.broadcasted_iota(jnp.int32, (qc, kc), 0)
                col = lax.broadcasted_iota(jnp.int32, (qc, kc), 1)
                p = jnp.where(2 * col <= row, p, 0.0)
            ds = (p * d).astype(BF16)
            dv_t[:, cpart] += dot(own_dot[:head, rpart], p.astype(BF16))
            dk_t[:, cpart] += dot(own_qt[:head, rpart], ds)
            term = dot(ds, kvbuf[me, 0, cpart])
            dq = term if dq is None else dq + term
        dq_acc[rpart] = dq

    for peer in range(n_dev):
        @pl.when(peer < me)
        def _():
            aux_copy(me, peer, own_aux_send.at[peer]).start()
    for d, dest in enumerate(dests):
        @pl.when(dest < me)
        def _():
            for n in range(1, CHUNKS):
                c = order(d, n)
                q_copy(me, c, dest, own_send.at[d, c], recv_sem.at[me, c]).start()

    def plan(t):
        na, ka = (t - 2) // 2, t % 2
        nb = (t - 10) // 2
        first, second = t < 2, t < 10
        hop = jnp.where(ka == 1, other, 0)

        def pick(a, b, c):
            return jnp.where(first, a, jnp.where(second, b, c))

        stream_a = pick(3, jnp.where(ka == 0, 0, 3), jnp.where(ka == 0, 2, 3))
        stream_b = pick(3, jnp.where(ka == 0, 1, 3), jnp.where(ka == 0, 2, 3))
        src_a = pick(pair, nx + hop, diag + hop)
        src_b = pick(pair, ny + hop, diag + hop)
        piece_a = pick(2 * t, (na + 2) % CHUNKS, jnp.where(mid, 2 * nb, nb))
        piece_b = pick(2 * t + 1, na, jnp.where(mid, 2 * nb + 1, nb + 2))
        swap = (src_a > me) & (src_b < me)

        def swapped(a, b):
            return jnp.where(swap, b, a), jnp.where(swap, a, b)

        stream_a, stream_b = swapped(stream_a, stream_b)
        src_a, src_b = swapped(src_a, src_b)
        piece_a, piece_b = swapped(piece_a, piece_b)
        return (stream_a, src_a, piece_a), (stream_b, src_b, piece_b)

    def sends(item, do):
        stream, src, piece = item
        idx = jnp.minimum(stream, 2)
        recv = recv_sem.at[src, piece]
        to_x = (stream == 1) & (jnp.logical_not(mid) | (piece < 2))
        to_y = (stream == 0) & mid & (piece >= 2)
        for make, want in ((q_copy, src > me), (kv_copy, src < me)):
            @pl.when(want)
            def _():
                do(make(src, piece, me, x_send.at[piece], recv), 'recv')

                @pl.when(to_x)
                def _():
                    do(make(src, piece, nx, x_send.at[piece], recv), 'send')

                @pl.when(to_y)
                def _():
                    do(make(src, piece, ny, y_send.at[piece], recv), 'send')

                @pl.when(stream < 3)
                def _():
                    do(make(src, piece, pair, pair_send.at[idx, piece], recv), 'send')

    def arrive(copy, what):
        copy.wait_recv() if what == 'recv' else copy.start()

    def leave(copy, what):
        if what == 'send':
            copy.wait_send()

    def add_keys_grads(items, cur):
        loaded = []
        for idx, (_, src, piece) in items:
            part = pl.ds(pl.multiple_of(piece * qc, qc), qc)
            q, do, aux = qbuf[src, 0, part], qbuf[src, 1, part], chunk_aux[cur, idx]
            q_t[idx] = jnp.transpose(q)
            do_t[idx] = jnp.transpose(do)
            loaded.append((idx, beside(q, aux), beside(do, aux)))
        for cb in range(keys // COLS):
            cpart = pl.ds(cb * COLS, COLS)
            dv = dk = None
            for idx, q, do in loaded:
                p = jnp.exp2(dot(q, own_kt[:, cpart]) * exp_scale)
                ds = (p * dot(do, own_vt[:, cpart])).astype(BF16)
                tv, tk = dot(do_t[idx], p.astype(BF16)), dot(q_t[idx], ds)
                dv, dk = (tv, tk) if dv is None else (dv + tv, dk + tk)
            dv_t[:, cpart] += dv
            dk_t[:, cpart] += dk

    def add_rows_grad(items):
        ks, vs = [], []
        for idx, (_, src, piece) in items:
            part = pl.ds(pl.multiple_of(piece * kc, kc), kc)
            ks.append(kvbuf[src, 0, part])
            vs.append(kvbuf[src, 1, part])
        k_ts = [jnp.transpose(k) for k in ks]
        k = jnp.concatenate([beside(k, k_one[...]) for k in ks], axis=0)
        v = jnp.concatenate([beside(v, v_one[...]) for v in vs], axis=0)
        k_t = k_ts[0] if len(k_ts) == 1 else beside(*k_ts)
        for rb in range(rows // COLS):
            part = pl.ds(rb * COLS, COLS)
            p = jnp.exp2(dot(k, own_qt[:, part]) * exp_scale)
            ds = (p * dot(v, own_dot[:, part])).astype(BF16)
            dq_t[:, part] += dot(k_t, ds)

    def prefetch(t, idx):
        _, src, piece = plan(t)[idx]
        fill_aux(jnp.where(src > me, src, me), piece, chunk_aux.at[t % 2, idx], 0)

    @pl.when(pair > me)
    def _():
        aux_copy(pair, me, own_aux_send.at[0]).wait_recv()
        for idx in range(2):
            prefetch(0, idx)

    def step(t, _):
        a, b = plan(t)
        cur = t % 2

        @pl.when(t == 1)
        def _():
            for peer in range(n_dev):
                @pl.when((peer > me) & (peer != pair))
                def _():
                    aux_copy(peer, me, own_aux_send.at[0]).wait_recv()

        sends(a, arrive)
        sends(b, arrive)
        a_keys, b_keys = a[1] < me, b[1] < me
        later = jnp.minimum(t + 1, STEPS - 1)

        def ahead():
            for idx in range(2):
                _, src, piece = plan(later)[idx]
                fill_aux(jnp.where(src > me, src, me), piece, chunk_aux.at[1 - cur, idx], 0)

        @pl.when(jnp.logical_not(a_keys))
        def _():
            add_keys_grads(((0, a), (1, b)), cur)
            ahead()

        @pl.when(a_keys & b_keys)
        def _():
            add_rows_grad(((0, a), (1, b)))
            ahead()

        @pl.when(a_keys & jnp.logical_not(b_keys))
        def _():
            add_rows_grad(((0, a),))
            add_keys_grads(((1, b),), cur)
            ahead()

        return 0

    lax.fori_loop(0, STEPS, step, 0)

    dq_ref[...] = ((dq_acc[...] + jnp.transpose(dq_t[...])) * scale).astype(BF16)
    dk_ref[...] = (jnp.transpose(dk_t[...]) * scale).astype(BF16)
    dv_ref[...] = jnp.transpose(dv_t[...]).astype(BF16)

    for peer in range(n_dev):
        @pl.when(peer < me)
        def _():
            aux_copy(me, peer, own_aux_send.at[peer]).wait_send()
    for d, dest in enumerate(dests):
        for make, want in ((kv_copy, dest > me), (q_copy, dest < me)):
            @pl.when(want)
            def _():
                for c in range(CHUNKS):
                    make(me, c, dest, own_send.at[d, c], recv_sem.at[me, c]).wait_send()

    def drain(t, _):
        for item in plan(t):
            sends(item, leave)
        return 0

    lax.fori_loop(2, STEPS, drain, 0)


def solution(mesh):
    n_dev = mesh.shape['cp']
    row_spec = P(('dp', 'cp'))

    def local_fn(q_tok, k_tok, v_tok, fwd_out, d_out, lse_row):
        tokens, groups, head = q_tok.shape
        rows = tokens * groups
        piece = rows // CHUNKS
        flat = lambda x: x.reshape(rows, head)
        dma = pltpu.SemaphoreType.DMA
        vmem = pltpu.VMEM
        grad_q, grad_k, grad_v = pl.pallas_call(
            functools.partial(kernel, rows, tokens, head, n_dev),
            out_shape=(jax.ShapeDtypeStruct((rows, head), BF16),
                       jax.ShapeDtypeStruct((tokens, head), BF16),
                       jax.ShapeDtypeStruct((tokens, head), BF16)),
            in_specs=[pl.BlockSpec(memory_space=pltpu.HBM)] * 6,
            out_specs=(pl.BlockSpec(memory_space=vmem),) * 3,
            scratch_shapes=[
                vmem((n_dev, 2, rows, head), BF16),
                vmem((n_dev, 2, tokens, head), BF16),
                vmem((rows, head), BF16),
                vmem((groups, tokens), F32),
                vmem((n_dev, CHUNKS, 8, 128), F32),
                vmem((rows, head), BF16),
                vmem((2, 2, piece, head), BF16),
                vmem((COLS, head), BF16),
                vmem((COLS, head), BF16),
                vmem((2 * head, rows), BF16),
                vmem((2 * head, rows), BF16),
                vmem((2 * head, tokens), BF16),
                vmem((2 * head, tokens), BF16),
                vmem((2, head, piece), BF16),
                vmem((2, head, piece), BF16),
                vmem((rows, head), F32),
                vmem((head, rows), F32),
                vmem((head, tokens), F32),
                vmem((head, tokens), F32),
                dma((6,)),
                dma((n_dev, CHUNKS)),
                dma((n_dev,)),
                dma((3, CHUNKS)),
                dma((n_dev,)),
                dma((3, CHUNKS)),
                dma((CHUNKS,)),
                dma((CHUNKS,)),
            ],
            compiler_params=pltpu.CompilerParams(
                collective_id=0, has_side_effects=True, vmem_limit_bytes=48 * 1024 * 1024),
            name='attention_backward',
        )(flat(q_tok), k_tok, v_tok, flat(fwd_out), flat(d_out), lse_row.T)
        return grad_q.reshape(tokens, groups, head), grad_k, grad_v

    return jax.shard_map(local_fn, mesh=mesh, in_specs=(row_spec,) * 6, out_specs=(row_spec,) * 3, check_vma=False)
```

```python
import functools
import math

import jax
import jax.numpy as jnp
from jax import lax
from jax.experimental import pallas as pl
from jax.experimental.pallas import tpu as pltpu
from jax.sharding import PartitionSpec as P

BF16, F32 = jnp.bfloat16, jnp.float32
CHUNKS = 4
COLS = 256
STEPS = 14
MESH = pl.DeviceIdType.MESH


def dot(a, b):
    return jnp.dot(a, b, preferred_element_type=F32)


def beside(a, b):
    return jnp.concatenate([a, b], axis=1)


def parts(x):
    hi = x.astype(BF16).astype(F32)
    rest = x - hi
    md = rest.astype(BF16).astype(F32)
    return hi, md, rest - md


def kernel(rows, keys, head, n_dev, q_hbm, k_hbm, v_hbm, o_hbm, do_hbm, lse_hbm, dq_ref, dk_ref, dv_ref,
           qbuf, kvbuf, obuf, lse_in, auxr, own_aux, chunk_aux, k_one, v_one, own_qt, own_dot, own_kt, own_vt,
           q_t, do_t, dq_acc, dq_t, dk_t, dv_t,
           stage_sem, recv_sem, aux_recv, own_send, own_aux_send, pair_send, x_send, y_send):
    me = lax.axis_index('cp')
    core, px, py = me % 2, (me // 2) % 2, me // 4
    pair = me + 1 - 2 * core
    nx = me + 2 - 4 * px
    ny = me + 4 - 8 * py
    diag = nx + 4 - 8 * py
    other = pair - me
    mid = (px + py) == 1
    qc, kc = rows // CHUNKS, keys // CHUNKS
    scale = head ** -0.5
    exp_scale = scale * math.log2(math.e)

    def q_copy(slot, n, dest, send, recv):
        part = pl.ds(n * qc, qc)
        return pltpu.make_async_remote_copy(
            qbuf.at[slot, :, part], qbuf.at[slot, :, part], send, recv,
            device_id={'cp': dest}, device_id_type=MESH)

    def kv_copy(slot, n, dest, send, recv):
        part = pl.ds(n * kc, kc)
        return pltpu.make_async_remote_copy(
            kvbuf.at[slot, :, part], kvbuf.at[slot, :, part], send, recv,
            device_id={'cp': dest}, device_id_type=MESH)

    def aux_copy(slot, dest, send):
        return pltpu.make_async_remote_copy(
            auxr.at[slot], auxr.at[slot], send, aux_recv.at[slot],
            device_id={'cp': dest}, device_id_type=MESH)

    stages = [
        pltpu.make_async_copy(k_hbm, kvbuf.at[me, 0], stage_sem.at[0]),
        pltpu.make_async_copy(v_hbm, kvbuf.at[me, 1], stage_sem.at[1]),
        pltpu.make_async_copy(q_hbm, qbuf.at[me, 0], stage_sem.at[2]),
        pltpu.make_async_copy(do_hbm, qbuf.at[me, 1], stage_sem.at[3]),
        pltpu.make_async_copy(o_hbm, obuf, stage_sem.at[4]),
        pltpu.make_async_copy(lse_hbm, lse_in, stage_sem.at[5]),
    ]
    for s in stages:
        s.start()

    barrier = pltpu.get_barrier_semaphore()
    for peer in range(n_dev):
        @pl.when(peer != me)
        def _():
            pl.semaphore_signal(barrier, inc=1, device_id={'cp': peer}, device_id_type=MESH)
    pl.semaphore_wait(barrier, n_dev - 1)

    def order(d, n):
        return (n + 2) % CHUNKS if d == 1 else n

    dests = (pair, nx, ny)
    for s in stages[:4]:
        s.wait()
    for d, dest in enumerate(dests):
        @pl.when(dest > me)
        def _():
            for n in range(CHUNKS):
                c = order(d, n)
                kv_copy(me, c, dest, own_send.at[d, c], recv_sem.at[me, c]).start()

        @pl.when(dest < me)
        def _():
            c = order(d, 0)
            q_copy(me, c, dest, own_send.at[d, c], recv_sem.at[me, c]).start()

    for s in stages[4:]:
        s.wait()

    at_row = lax.broadcasted_iota(jnp.int32, (COLS, COLS), 0)
    at_col = lax.broadcasted_iota(jnp.int32, (COLS, COLS), 1)
    weave = jnp.where(at_col == 2 * (at_row % 128) + at_row // 128, 1.0, 0.0).astype(BF16)
    sub = lax.broadcasted_iota(jnp.int32, (16, 128), 0)
    for g in range(rows // 256):
        sides = []
        for h in range(2):
            row = lse_in[h:h + 1, g * 128:(g + 1) * 128] * (1.0 / scale)
            hi, md, lo = parts(row)
            sides.append(jnp.where(sub == 0, hi, jnp.where(sub == 1, md, jnp.where(sub == 2, lo, 0.0))))
        woven = dot(beside(*sides).astype(BF16), weave)
        row = woven[0:1] + (woven[1:2] + woven[2:3])
        n, at = g // 2, (g % 2) * 2
        auxr[me, n, at:at + 1] = row[:, 0:128]
        auxr[me, n, at + 1:at + 2] = row[:, 128:256]

    def delta_rows(n, _):
        for g in range(qc // 128):
            part = pl.ds(pl.multiple_of(n * qc + g * 128, 128), 128)
            d = jnp.sum(qbuf[me, 1, part].astype(F32) * obuf[part].astype(F32), axis=1, keepdims=True)
            auxr[me, n, 4 + g:5 + g] = jnp.transpose(jnp.broadcast_to(d, (128, 128)))[0:1]
        return 0

    lax.fori_loop(0, CHUNKS, delta_rows, 0)

    def aux_lines(slot, n):
        hi, md, lo = parts(auxr[slot, n])
        sub = lax.broadcasted_iota(jnp.int32, (8, 128), 0)
        lines = []
        for g in range(qc // 128):
            m = jnp.zeros((8, 128), F32)
            for i, row in enumerate((hi[g:g + 1], md[g:g + 1], lo[g:g + 1],
                                     hi[4 + g:5 + g], md[4 + g:5 + g], lo[4 + g:5 + g])):
                m = jnp.where(sub == i, row, m)
            lines.append(jnp.concatenate([m, jnp.zeros((120, 128), F32)], axis=0))
        return lines

    def fill_aux(slot, n, dst, base):
        for g, m in enumerate(aux_lines(slot, n)):
            dst[pl.ds(base + g * 128, 128)] = jnp.transpose(m).astype(BF16)

    lane = lax.broadcasted_iota(jnp.int32, (COLS, head), 1)
    line = lax.broadcasted_iota(jnp.int32, (head, keys), 0)
    k_one[...] = jnp.where(lane < 3, -1.0, 0.0).astype(BF16)
    v_one[...] = jnp.where((lane >= 3) & (lane < 6), -1.0, 0.0).astype(BF16)
    own_kt[head:] = jnp.where(line < 3, -1.0, 0.0).astype(BF16)
    own_vt[head:] = jnp.where((line >= 3) & (line < 6), -1.0, 0.0).astype(BF16)
    dk_t[...] = jnp.zeros_like(dk_t)
    dv_t[...] = jnp.zeros_like(dv_t)
    dq_t[...] = jnp.zeros_like(dq_t)

    def own_fill(n, _):
        base = pl.multiple_of(n * qc, 128)
        part, kpart = pl.ds(base, qc), pl.ds(pl.multiple_of(n * kc, 128), kc)
        for g, m in enumerate(aux_lines(me, n)):
            at = pl.ds(pl.multiple_of(base + g * 128, 128), 128)
            own_aux[at] = jnp.transpose(m).astype(BF16)
            own_qt[head:, at] = m.astype(BF16)
            own_dot[head:, at] = m.astype(BF16)
        own_qt[:head, part] = jnp.transpose(qbuf[me, 0, part])
        own_dot[:head, part] = jnp.transpose(qbuf[me, 1, part])
        own_kt[:head, kpart] = jnp.transpose(kvbuf[me, 0, kpart])
        own_vt[:head, kpart] = jnp.transpose(kvbuf[me, 1, kpart])
        return 0

    lax.fori_loop(0, CHUNKS, own_fill, 0)

    for rb in range(CHUNKS):
        rpart = pl.ds(rb * qc, qc)
        aux = own_aux[rpart]
        q, do = beside(qbuf[me, 0, rpart], aux), beside(qbuf[me, 1, rpart], aux)
        dq = None
        for cb in range(rb + 1):
            cpart = pl.ds(cb * kc, kc)
            p = jnp.exp2(dot(q, own_kt[:, cpart]) * exp_scale)
            d = dot(do, own_vt[:, cpart])
            if cb == rb:
                row = lax.broadcasted_iota(jnp.int32, (qc, kc), 0)
                col = lax.broadcasted_iota(jnp.int32, (qc, kc), 1)
                p = jnp.where(2 * col <= row, p, 0.0)
            ds = (p * d).astype(BF16)
            dv_t[:, cpart] += dot(own_dot[:head, rpart], p.astype(BF16))
            dk_t[:, cpart] += dot(own_qt[:head, rpart], ds)
            term = dot(ds, kvbuf[me, 0, cpart])
            dq = term if dq is None else dq + term
        dq_acc[rpart] = dq

    for peer in range(n_dev):
        @pl.when(peer < me)
        def _():
            aux_copy(me, peer, own_aux_send.at[peer]).start()
    for d, dest in enumerate(dests):
        @pl.when(dest < me)
        def _():
            for n in range(1, CHUNKS):
                c = order(d, n)
                q_copy(me, c, dest, own_send.at[d, c], recv_sem.at[me, c]).start()

    def plan(t):
        na, ka = (t - 2) // 2, t % 2
        nb = (t - 10) // 2
        first, second = t < 2, t < 10
        hop = jnp.where(ka == 1, other, 0)

        def pick(a, b, c):
            return jnp.where(first, a, jnp.where(second, b, c))

        stream_a = pick(3, jnp.where(ka == 0, 0, 3), jnp.where(ka == 0, 2, 3))
        stream_b = pick(3, jnp.where(ka == 0, 1, 3), jnp.where(ka == 0, 2, 3))
        src_a = pick(pair, nx + hop, diag + hop)
        src_b = pick(pair, ny + hop, diag + hop)
        piece_a = pick(2 * t, (na + 2) % CHUNKS, jnp.where(mid, 2 * nb, nb))
        piece_b = pick(2 * t + 1, na, jnp.where(mid, 2 * nb + 1, nb + 2))
        swap = (src_a > me) & (src_b < me)

        def swapped(a, b):
            return jnp.where(swap, b, a), jnp.where(swap, a, b)

        stream_a, stream_b = swapped(stream_a, stream_b)
        src_a, src_b = swapped(src_a, src_b)
        piece_a, piece_b = swapped(piece_a, piece_b)
        return (stream_a, src_a, piece_a), (stream_b, src_b, piece_b)

    def sends(item, do):
        stream, src, piece = item
        idx = jnp.minimum(stream, 2)
        recv = recv_sem.at[src, piece]
        to_x = (stream == 1) & (jnp.logical_not(mid) | (piece < 2))
        to_y = (stream == 0) & mid & (piece >= 2)
        for make, want in ((q_copy, src > me), (kv_copy, src < me)):
            @pl.when(want)
            def _():
                do(make(src, piece, me, x_send.at[piece], recv), 'recv')

                @pl.when(to_x)
                def _():
                    do(make(src, piece, nx, x_send.at[piece], recv), 'send')

                @pl.when(to_y)
                def _():
                    do(make(src, piece, ny, y_send.at[piece], recv), 'send')

                @pl.when(stream < 3)
                def _():
                    do(make(src, piece, pair, pair_send.at[idx, piece], recv), 'send')

    def arrive(copy, what):
        copy.wait_recv() if what == 'recv' else copy.start()

    def leave(copy, what):
        if what == 'send':
            copy.wait_send()

    def add_keys_grads(items, cur):
        loaded = []
        for idx, (_, src, piece) in items:
            part = pl.ds(pl.multiple_of(piece * qc, qc), qc)
            q, do, aux = qbuf[src, 0, part], qbuf[src, 1, part], chunk_aux[cur, idx]
            q_t[idx] = jnp.transpose(q)
            do_t[idx] = jnp.transpose(do)
            loaded.append((idx, beside(q, aux), beside(do, aux)))
        for cb in range(keys // COLS):
            cpart = pl.ds(cb * COLS, COLS)
            dv = dk = None
            for idx, q, do in loaded:
                p = jnp.exp2(dot(q, own_kt[:, cpart]) * exp_scale)
                ds = (p * dot(do, own_vt[:, cpart])).astype(BF16)
                tv, tk = dot(do_t[idx], p.astype(BF16)), dot(q_t[idx], ds)
                dv, dk = (tv, tk) if dv is None else (dv + tv, dk + tk)
            dv_t[:, cpart] += dv
            dk_t[:, cpart] += dk

    def add_rows_grad(items):
        ks, vs = [], []
        for idx, (_, src, piece) in items:
            part = pl.ds(pl.multiple_of(piece * kc, kc), kc)
            ks.append(kvbuf[src, 0, part])
            vs.append(kvbuf[src, 1, part])
        k_ts = [jnp.transpose(k) for k in ks]
        k = jnp.concatenate([beside(k, k_one[...]) for k in ks], axis=0)
        v = jnp.concatenate([beside(v, v_one[...]) for v in vs], axis=0)
        k_t = k_ts[0] if len(k_ts) == 1 else beside(*k_ts)
        for rb in range(rows // 512):
            part = pl.ds(rb * 512, 512)
            p = jnp.exp2(dot(k, own_qt[:, part]) * exp_scale)
            ds = (p * dot(v, own_dot[:, part])).astype(BF16)
            dq_t[:, part] += dot(k_t, ds)

    def prefetch(t, idx):
        _, src, piece = plan(t)[idx]
        fill_aux(jnp.where(src > me, src, me), piece, chunk_aux.at[t % 2, idx], 0)

    @pl.when(pair > me)
    def _():
        aux_copy(pair, me, own_aux_send.at[0]).wait_recv()
        for idx in range(2):
            prefetch(0, idx)

    def step(t, _):
        a, b = plan(t)
        cur = t % 2

        @pl.when(t == 1)
        def _():
            for peer in range(n_dev):
                @pl.when((peer > me) & (peer != pair))
                def _():
                    aux_copy(peer, me, own_aux_send.at[0]).wait_recv()

        sends(a, arrive)
        sends(b, arrive)
        a_keys, b_keys = a[1] < me, b[1] < me
        later = jnp.minimum(t + 1, STEPS - 1)

        def ahead():
            for idx in range(2):
                _, src, piece = plan(later)[idx]
                fill_aux(jnp.where(src > me, src, me), piece, chunk_aux.at[1 - cur, idx], 0)

        @pl.when(jnp.logical_not(a_keys))
        def _():
            add_keys_grads(((0, a), (1, b)), cur)
            ahead()

        @pl.when(a_keys & b_keys)
        def _():
            add_rows_grad(((0, a), (1, b)))
            ahead()

        @pl.when(a_keys & jnp.logical_not(b_keys))
        def _():
            add_rows_grad(((0, a),))
            add_keys_grads(((1, b),), cur)
            ahead()

        return 0

    lax.fori_loop(0, STEPS, step, 0)

    dq_ref[...] = ((dq_acc[...] + jnp.transpose(dq_t[...])) * scale).astype(BF16)
    dk_ref[...] = (jnp.transpose(dk_t[...]) * scale).astype(BF16)
    dv_ref[...] = jnp.transpose(dv_t[...]).astype(BF16)

    for peer in range(n_dev):
        @pl.when(peer < me)
        def _():
            aux_copy(me, peer, own_aux_send.at[peer]).wait_send()
    for d, dest in enumerate(dests):
        for make, want in ((kv_copy, dest > me), (q_copy, dest < me)):
            @pl.when(want)
            def _():
                for c in range(CHUNKS):
                    make(me, c, dest, own_send.at[d, c], recv_sem.at[me, c]).wait_send()

    def drain(t, _):
        for item in plan(t):
            sends(item, leave)
        return 0

    lax.fori_loop(2, STEPS, drain, 0)


def store(*refs):
    n = len(refs) // 2
    copies = [pltpu.make_async_copy(refs[i], refs[n + i], refs[-1].at[i]) for i in range(n)]
    for c in copies:
        c.start()
    for c in copies:
        c.wait()


def solution(mesh):
    n_dev = mesh.shape['cp']
    row_spec = P(('dp', 'cp'))

    def local_fn(q_tok, k_tok, v_tok, fwd_out, d_out, lse_row):
        tokens, groups, head = q_tok.shape
        rows = tokens * groups
        piece = rows // CHUNKS
        flat = lambda x: x.reshape(rows, head)
        dma = pltpu.SemaphoreType.DMA
        vmem = pltpu.VMEM
        grad_q, grad_k, grad_v = pl.pallas_call(
            functools.partial(kernel, rows, tokens, head, n_dev),
            out_shape=(jax.ShapeDtypeStruct((rows, head), BF16),
                       jax.ShapeDtypeStruct((tokens, head), BF16),
                       jax.ShapeDtypeStruct((tokens, head), BF16)),
            in_specs=[pl.BlockSpec(memory_space=pltpu.HBM)] * 6,
            out_specs=(pl.BlockSpec(memory_space=vmem),) * 3,
            scratch_shapes=[
                vmem((n_dev, 2, rows, head), BF16),
                vmem((n_dev, 2, tokens, head), BF16),
                vmem((rows, head), BF16),
                vmem((groups, tokens), F32),
                vmem((n_dev, CHUNKS, 8, 128), F32),
                vmem((rows, head), BF16),
                vmem((2, 2, piece, head), BF16),
                vmem((COLS, head), BF16),
                vmem((COLS, head), BF16),
                vmem((2 * head, rows), BF16),
                vmem((2 * head, rows), BF16),
                vmem((2 * head, tokens), BF16),
                vmem((2 * head, tokens), BF16),
                vmem((2, head, piece), BF16),
                vmem((2, head, piece), BF16),
                vmem((rows, head), F32),
                vmem((head, rows), F32),
                vmem((head, tokens), F32),
                vmem((head, tokens), F32),
                dma((6,)),
                dma((n_dev, CHUNKS)),
                dma((n_dev,)),
                dma((3, CHUNKS)),
                dma((n_dev,)),
                dma((3, CHUNKS)),
                dma((CHUNKS,)),
                dma((CHUNKS,)),
            ],
            compiler_params=pltpu.CompilerParams(
                collective_id=0, has_side_effects=True, vmem_limit_bytes=48 * 1024 * 1024),
            name='attention_backward',
        )(*[pltpu.with_memory_space_constraint(x, pltpu.HBM) for x in (flat(q_tok), k_tok, v_tok, flat(fwd_out), flat(d_out), lse_row.T)])
        grads = (grad_q, grad_k, grad_v)
        any_space = pl.BlockSpec(memory_space=pl.ANY)
        grad_q, grad_k, grad_v = pl.pallas_call(
            store,
            out_shape=tuple(jax.ShapeDtypeStruct(g.shape, g.dtype) for g in grads),
            in_specs=[any_space] * 3,
            out_specs=(any_space,) * 3,
            scratch_shapes=[dma((3,))],
            compiler_params=pltpu.CompilerParams(vmem_limit_bytes=1024 * 1024),
            name='store_grads',
        )(*[pltpu.with_memory_space_constraint(g, vmem) for g in grads])
        return grad_q.reshape(tokens, groups, head), grad_k, grad_v

    return jax.shard_map(local_fn, mesh=mesh, in_specs=(row_spec,) * 6, out_specs=(row_spec,) * 3, check_vma=False)
```

```python
import functools
import math

import jax
import jax.numpy as jnp
from jax import lax
from jax.experimental import pallas as pl
from jax.experimental.pallas import tpu as pltpu
from jax.sharding import PartitionSpec as P

BF16, F32 = jnp.bfloat16, jnp.float32
CHUNKS = 4
COLS = 256
STEPS = 14
MESH = pl.DeviceIdType.MESH


def dot(a, b):
    return jnp.dot(a, b, preferred_element_type=F32)


def beside(a, b):
    return jnp.concatenate([a, b], axis=1)


def parts(x):
    hi = x.astype(BF16).astype(F32)
    rest = x - hi
    md = rest.astype(BF16).astype(F32)
    return hi, md, rest - md


def kernel(rows, keys, head, n_dev, q_hbm, k_hbm, v_hbm, o_hbm, do_hbm, lse_hbm, dq_ref, dk_ref, dv_ref,
           qbuf, kvbuf, obuf, lse_in, auxr, own_aux, chunk_aux, k_one, v_one, own_qt, own_dot, own_kt, own_vt,
           q_t, do_t, dq_acc, dq_t, dk_t, dv_t,
           stage_sem, recv_sem, aux_recv, own_send, own_aux_send, pair_send, x_send, y_send):
    me = lax.axis_index('cp')
    core, px, py = me % 2, (me // 2) % 2, me // 4
    pair = me + 1 - 2 * core
    nx = me + 2 - 4 * px
    ny = me + 4 - 8 * py
    diag = nx + 4 - 8 * py
    other = pair - me
    mid = (px + py) == 1
    qc, kc = rows // CHUNKS, keys // CHUNKS
    scale = head ** -0.5
    exp_scale = scale * math.log2(math.e)

    def q_copy(slot, n, dest, send, recv):
        part = pl.ds(n * qc, qc)
        return pltpu.make_async_remote_copy(
            qbuf.at[slot, :, part], qbuf.at[slot, :, part], send, recv,
            device_id={'cp': dest}, device_id_type=MESH)

    def kv_copy(slot, n, dest, send, recv):
        part = pl.ds(n * kc, kc)
        return pltpu.make_async_remote_copy(
            kvbuf.at[slot, :, part], kvbuf.at[slot, :, part], send, recv,
            device_id={'cp': dest}, device_id_type=MESH)

    def aux_copy(slot, dest, send):
        return pltpu.make_async_remote_copy(
            auxr.at[slot], auxr.at[slot], send, aux_recv.at[slot],
            device_id={'cp': dest}, device_id_type=MESH)

    stages = [
        pltpu.make_async_copy(k_hbm, kvbuf.at[me, 0], stage_sem.at[0]),
        pltpu.make_async_copy(v_hbm, kvbuf.at[me, 1], stage_sem.at[1]),
        pltpu.make_async_copy(q_hbm, qbuf.at[me, 0], stage_sem.at[2]),
        pltpu.make_async_copy(do_hbm, qbuf.at[me, 1], stage_sem.at[3]),
        pltpu.make_async_copy(o_hbm, obuf, stage_sem.at[4]),
        pltpu.make_async_copy(lse_hbm, lse_in, stage_sem.at[5]),
    ]
    for s in stages:
        s.start()

    barrier = pltpu.get_barrier_semaphore()
    for peer in range(n_dev):
        @pl.when(peer != me)
        def _():
            pl.semaphore_signal(barrier, inc=1, device_id={'cp': peer}, device_id_type=MESH)
    pl.semaphore_wait(barrier, n_dev - 1)

    def order(d, n):
        return (n + 2) % CHUNKS if d == 1 else n

    dests = (pair, nx, ny)
    for s in stages[:4]:
        s.wait()
    for d, dest in enumerate(dests):
        @pl.when(dest > me)
        def _():
            for n in range(CHUNKS):
                c = order(d, n)
                kv_copy(me, c, dest, own_send.at[d], recv_sem.at[me, c]).start()

        @pl.when(dest < me)
        def _():
            c = order(d, 0)
            q_copy(me, c, dest, own_send.at[d], recv_sem.at[me, c]).start()

    for s in stages[4:]:
        s.wait()

    at_row = lax.broadcasted_iota(jnp.int32, (COLS, COLS), 0)
    at_col = lax.broadcasted_iota(jnp.int32, (COLS, COLS), 1)
    weave = jnp.where(at_col == 2 * (at_row % 128) + at_row // 128, 1.0, 0.0).astype(BF16)
    sub = lax.broadcasted_iota(jnp.int32, (16, 128), 0)
    for g in range(rows // 256):
        sides = []
        for h in range(2):
            row = lse_in[h:h + 1, g * 128:(g + 1) * 128] * (1.0 / scale)
            hi, md, lo = parts(row)
            sides.append(jnp.where(sub == 0, hi, jnp.where(sub == 1, md, jnp.where(sub == 2, lo, 0.0))))
        woven = dot(beside(*sides).astype(BF16), weave)
        row = woven[0:1] + (woven[1:2] + woven[2:3])
        n, at = g // 2, (g % 2) * 2
        auxr[me, n, at:at + 1] = row[:, 0:128]
        auxr[me, n, at + 1:at + 2] = row[:, 128:256]

    def delta_rows(n, _):
        for g in range(qc // 128):
            part = pl.ds(pl.multiple_of(n * qc + g * 128, 128), 128)
            d = jnp.sum(qbuf[me, 1, part].astype(F32) * obuf[part].astype(F32), axis=1, keepdims=True)
            auxr[me, n, 4 + g:5 + g] = jnp.transpose(jnp.broadcast_to(d, (128, 128)))[0:1]
        return 0

    lax.fori_loop(0, CHUNKS, delta_rows, 0)

    def aux_lines(slot, n):
        hi, md, lo = parts(auxr[slot, n])
        sub = lax.broadcasted_iota(jnp.int32, (8, 128), 0)
        lines = []
        for g in range(qc // 128):
            m = jnp.zeros((8, 128), F32)
            for i, row in enumerate((hi[g:g + 1], md[g:g + 1], lo[g:g + 1],
                                     hi[4 + g:5 + g], md[4 + g:5 + g], lo[4 + g:5 + g])):
                m = jnp.where(sub == i, row, m)
            lines.append(jnp.concatenate([m, jnp.zeros((120, 128), F32)], axis=0))
        return lines

    def fill_aux(slot, n, dst, base):
        for g, m in enumerate(aux_lines(slot, n)):
            dst[pl.ds(base + g * 128, 128)] = jnp.transpose(m).astype(BF16)

    lane = lax.broadcasted_iota(jnp.int32, (COLS, head), 1)
    line = lax.broadcasted_iota(jnp.int32, (head, keys), 0)
    k_one[...] = jnp.where(lane < 3, -1.0, 0.0).astype(BF16)
    v_one[...] = jnp.where((lane >= 3) & (lane < 6), -1.0, 0.0).astype(BF16)
    own_kt[head:] = jnp.where(line < 3, -1.0, 0.0).astype(BF16)
    own_vt[head:] = jnp.where((line >= 3) & (line < 6), -1.0, 0.0).astype(BF16)
    dk_t[...] = jnp.zeros_like(dk_t)
    dv_t[...] = jnp.zeros_like(dv_t)
    dq_t[...] = jnp.zeros_like(dq_t)

    def own_fill(n, _):
        base = pl.multiple_of(n * qc, 128)
        part, kpart = pl.ds(base, qc), pl.ds(pl.multiple_of(n * kc, 128), kc)
        for g, m in enumerate(aux_lines(me, n)):
            at = pl.ds(pl.multiple_of(base + g * 128, 128), 128)
            own_aux[at] = jnp.transpose(m).astype(BF16)
            own_qt[head:, at] = m.astype(BF16)
            own_dot[head:, at] = m.astype(BF16)
        own_qt[:head, part] = jnp.transpose(qbuf[me, 0, part])
        own_dot[:head, part] = jnp.transpose(qbuf[me, 1, part])
        own_kt[:head, kpart] = jnp.transpose(kvbuf[me, 0, kpart])
        own_vt[:head, kpart] = jnp.transpose(kvbuf[me, 1, kpart])
        return 0

    lax.fori_loop(0, CHUNKS, own_fill, 0)

    for peer in range(n_dev):
        @pl.when(peer < me)
        def _():
            aux_copy(me, peer, own_aux_send.at[peer]).start()
    for d, dest in enumerate(dests):
        @pl.when(dest < me)
        def _():
            for n in range(1, CHUNKS):
                c = order(d, n)
                q_copy(me, c, dest, own_send.at[d], recv_sem.at[me, c]).start()

    for rb in range(CHUNKS):
        rpart = pl.ds(rb * qc, qc)
        aux = own_aux[rpart]
        q, do = beside(qbuf[me, 0, rpart], aux), beside(qbuf[me, 1, rpart], aux)
        dq = None
        for cb in range(rb + 1):
            cpart = pl.ds(cb * kc, kc)
            p = jnp.exp2(dot(q, own_kt[:, cpart]) * exp_scale)
            d = dot(do, own_vt[:, cpart])
            if cb == rb:
                row = lax.broadcasted_iota(jnp.int32, (qc, kc), 0)
                col = lax.broadcasted_iota(jnp.int32, (qc, kc), 1)
                p = jnp.where(2 * col <= row, p, 0.0)
            ds = (p * d).astype(BF16)
            dv_t[:, cpart] += dot(own_dot[:head, rpart], p.astype(BF16))
            dk_t[:, cpart] += dot(own_qt[:head, rpart], ds)
            term = dot(ds, kvbuf[me, 0, cpart])
            dq = term if dq is None else dq + term
        dq_acc[rpart] = dq

    def plan(t):
        na, ka = (t - 2) // 2, t % 2
        nb = (t - 10) // 2
        first, second = t < 2, t < 10
        hop = jnp.where(ka == 1, other, 0)

        def pick(a, b, c):
            return jnp.where(first, a, jnp.where(second, b, c))

        stream_a = pick(3, jnp.where(ka == 0, 0, 3), jnp.where(ka == 0, 2, 3))
        stream_b = pick(3, jnp.where(ka == 0, 1, 3), jnp.where(ka == 0, 2, 3))
        src_a = pick(pair, nx + hop, diag + hop)
        src_b = pick(pair, ny + hop, diag + hop)
        piece_a = pick(2 * t, (na + 2) % CHUNKS, jnp.where(mid, 2 * nb, nb))
        piece_b = pick(2 * t + 1, na, jnp.where(mid, 2 * nb + 1, nb + 2))
        swap = (src_a > me) & (src_b < me)

        def swapped(a, b):
            return jnp.where(swap, b, a), jnp.where(swap, a, b)

        stream_a, stream_b = swapped(stream_a, stream_b)
        src_a, src_b = swapped(src_a, src_b)
        piece_a, piece_b = swapped(piece_a, piece_b)
        return (stream_a, src_a, piece_a), (stream_b, src_b, piece_b)

    def arrive(item):
        stream, src, piece = item
        idx = jnp.minimum(stream, 2)
        recv = recv_sem.at[src, piece]
        to_x = (stream == 1) & (jnp.logical_not(mid) | (piece < 2))
        to_y = (stream == 0) & mid & (piece >= 2)
        for make, want in ((q_copy, src > me), (kv_copy, src < me)):
            @pl.when(want)
            def _():
                make(src, piece, me, x_send, recv).wait_recv()

                @pl.when(to_x)
                def _():
                    make(src, piece, nx, x_send, recv).start()

                @pl.when(to_y)
                def _():
                    make(src, piece, ny, y_send, recv).start()

                @pl.when(stream < 3)
                def _():
                    make(src, piece, pair, pair_send.at[idx], recv).start()

    def add_keys_grads(items, cur):
        loaded = []
        for idx, (_, src, piece) in items:
            part = pl.ds(pl.multiple_of(piece * qc, qc), qc)
            q, do, aux = qbuf[src, 0, part], qbuf[src, 1, part], chunk_aux[cur, idx]
            q_t[idx] = jnp.transpose(q)
            do_t[idx] = jnp.transpose(do)
            loaded.append((idx, beside(q, aux), beside(do, aux)))
        for cb in range(keys // COLS):
            cpart = pl.ds(cb * COLS, COLS)
            dv = dk = None
            for idx, q, do in loaded:
                p = jnp.exp2(dot(q, own_kt[:, cpart]) * exp_scale)
                ds = (p * dot(do, own_vt[:, cpart])).astype(BF16)
                tv, tk = dot(do_t[idx], p.astype(BF16)), dot(q_t[idx], ds)
                dv, dk = (tv, tk) if dv is None else (dv + tv, dk + tk)
            dv_t[:, cpart] += dv
            dk_t[:, cpart] += dk

    def add_rows_grad(items):
        ks, vs = [], []
        for idx, (_, src, piece) in items:
            part = pl.ds(pl.multiple_of(piece * kc, kc), kc)
            ks.append(kvbuf[src, 0, part])
            vs.append(kvbuf[src, 1, part])
        k_ts = [jnp.transpose(k) for k in ks]
        k = jnp.concatenate([beside(k, k_one[...]) for k in ks], axis=0)
        v = jnp.concatenate([beside(v, v_one[...]) for v in vs], axis=0)
        k_t = k_ts[0] if len(k_ts) == 1 else beside(*k_ts)
        for rb in range(rows // 512):
            part = pl.ds(rb * 512, 512)
            p = jnp.exp2(dot(k, own_qt[:, part]) * exp_scale)
            ds = (p * dot(v, own_dot[:, part])).astype(BF16)
            dq_t[:, part] += dot(k_t, ds)

    def prefetch(t, idx):
        _, src, piece = plan(t)[idx]
        fill_aux(jnp.where(src > me, src, me), piece, chunk_aux.at[t % 2, idx], 0)

    @pl.when(pair > me)
    def _():
        aux_copy(pair, me, own_aux_send.at[0]).wait_recv()
        for idx in range(2):
            prefetch(0, idx)

    def step(t, _):
        a, b = plan(t)
        cur = t % 2

        @pl.when(t == 1)
        def _():
            for peer in range(n_dev):
                @pl.when((peer > me) & (peer != pair))
                def _():
                    aux_copy(peer, me, own_aux_send.at[0]).wait_recv()

        arrive(a)
        arrive(b)
        a_keys, b_keys = a[1] < me, b[1] < me
        later = jnp.minimum(t + 1, STEPS - 1)

        def ahead():
            for idx in range(2):
                _, src, piece = plan(later)[idx]
                fill_aux(jnp.where(src > me, src, me), piece, chunk_aux.at[1 - cur, idx], 0)

        @pl.when(jnp.logical_not(a_keys))
        def _():
            add_keys_grads(((0, a), (1, b)), cur)
            ahead()

        @pl.when(a_keys & b_keys)
        def _():
            add_rows_grad(((0, a), (1, b)))
            ahead()

        @pl.when(a_keys & jnp.logical_not(b_keys))
        def _():
            add_rows_grad(((0, a),))
            add_keys_grads(((1, b),), cur)
            ahead()

        return 0

    lax.fori_loop(0, STEPS, step, 0)

    dq_ref[...] = ((dq_acc[...] + jnp.transpose(dq_t[...])) * scale).astype(BF16)
    dk_ref[...] = (jnp.transpose(dk_t[...]) * scale).astype(BF16)
    dv_ref[...] = jnp.transpose(dv_t[...]).astype(BF16)

    for peer in range(n_dev):
        @pl.when(peer < me)
        def _():
            aux_copy(me, peer, own_aux_send.at[peer]).wait_send()

    def left(buf, slot, length, send, want):
        @pl.when(want)
        def _():
            block = buf.at[slot, :, pl.ds(0, length)]
            pltpu.make_async_remote_copy(block, block, send, recv_sem.at[slot, 0],
                                         device_id={'cp': pair}, device_id_type=MESH).wait_send()

    for buf, size, sign in ((qbuf, rows, 1), (kvbuf, keys, -1)):
        for d, dest in enumerate(dests):
            left(buf, me, size, own_send.at[d], sign * dest < sign * me)
        for d, src in enumerate((nx, ny, diag)):
            left(buf, src, size, pair_send.at[d], sign * src > sign * me)
        left(buf, ny, size, x_send, (sign * ny > sign * me) & jnp.logical_not(mid))
        left(buf, ny, size // 2, x_send, (sign * ny > sign * me) & mid)
        left(buf, nx, size // 2, y_send, (sign * nx > sign * me) & mid)


def store(*refs):
    n = len(refs) // 2
    copies = [pltpu.make_async_copy(refs[i], refs[n + i], refs[-1].at[i]) for i in range(n)]
    for c in copies:
        c.start()
    for c in copies:
        c.wait()


def solution(mesh):
    n_dev = mesh.shape['cp']
    row_spec = P(('dp', 'cp'))

    def local_fn(q_tok, k_tok, v_tok, fwd_out, d_out, lse_row):
        tokens, groups, head = q_tok.shape
        rows = tokens * groups
        piece = rows // CHUNKS
        flat = lambda x: x.reshape(rows, head)
        dma = pltpu.SemaphoreType.DMA
        vmem = pltpu.VMEM
        grad_q, grad_k, grad_v = pl.pallas_call(
            functools.partial(kernel, rows, tokens, head, n_dev),
            out_shape=(jax.ShapeDtypeStruct((rows, head), BF16),
                       jax.ShapeDtypeStruct((tokens, head), BF16),
                       jax.ShapeDtypeStruct((tokens, head), BF16)),
            in_specs=[pl.BlockSpec(memory_space=pltpu.HBM)] * 6,
            out_specs=(pl.BlockSpec(memory_space=vmem),) * 3,
            scratch_shapes=[
                vmem((n_dev, 2, rows, head), BF16),
                vmem((n_dev, 2, tokens, head), BF16),
                vmem((rows, head), BF16),
                vmem((groups, tokens), F32),
                vmem((n_dev, CHUNKS, 8, 128), F32),
                vmem((rows, head), BF16),
                vmem((2, 2, piece, head), BF16),
                vmem((COLS, head), BF16),
                vmem((COLS, head), BF16),
                vmem((2 * head, rows), BF16),
                vmem((2 * head, rows), BF16),
                vmem((2 * head, tokens), BF16),
                vmem((2 * head, tokens), BF16),
                vmem((2, head, piece), BF16),
                vmem((2, head, piece), BF16),
                vmem((rows, head), F32),
                vmem((head, rows), F32),
                vmem((head, tokens), F32),
                vmem((head, tokens), F32),
                dma((6,)),
                dma((n_dev, CHUNKS)),
                dma((n_dev,)),
                dma((3,)),
                dma((n_dev,)),
                dma((3,)),
                dma,
                dma,
            ],
            compiler_params=pltpu.CompilerParams(
                collective_id=0, has_side_effects=True, vmem_limit_bytes=48 * 1024 * 1024),
            name='attention_backward',
        )(*[pltpu.with_memory_space_constraint(x, pltpu.HBM) for x in (flat(q_tok), k_tok, v_tok, flat(fwd_out), flat(d_out), lse_row.T)])
        grads = (grad_q, grad_k, grad_v)
        any_space = pl.BlockSpec(memory_space=pl.ANY)
        grad_q, grad_k, grad_v = pl.pallas_call(
            store,
            out_shape=tuple(jax.ShapeDtypeStruct(g.shape, g.dtype) for g in grads),
            in_specs=[any_space] * 3,
            out_specs=(any_space,) * 3,
            scratch_shapes=[dma((3,))],
            compiler_params=pltpu.CompilerParams(vmem_limit_bytes=1024 * 1024),
            name='store_grads',
        )(*[pltpu.with_memory_space_constraint(g, vmem) for g in grads])
        return grad_q.reshape(tokens, groups, head), grad_k, grad_v

    return jax.shard_map(local_fn, mesh=mesh, in_specs=(row_spec,) * 6, out_specs=(row_spec,) * 3, check_vma=False)
```

```python
import functools
import math

import jax
import jax.numpy as jnp
from jax import lax
from jax.experimental import pallas as pl
from jax.experimental.pallas import tpu as pltpu
from jax.sharding import PartitionSpec as P

BF16, F32 = jnp.bfloat16, jnp.float32
CHUNKS = 4
COLS = 256
STEPS = 14
LEAD_Q, LEAD_K, LEAD_M = 4, 4, 2
LEAD_D = 2
WIDTH_K, WIDTH_M = 256, 512
MESH = pl.DeviceIdType.MESH


def dot(a, b):
    return jnp.dot(a, b, preferred_element_type=F32)


def beside(a, b):
    return jnp.concatenate([a, b], axis=1)


def parts(x):
    hi = x.astype(BF16).astype(F32)
    rest = x - hi
    md = rest.astype(BF16).astype(F32)
    return hi, md, rest - md


def kernel(rows, keys, head, n_dev, q_hbm, k_hbm, v_hbm, o_hbm, do_hbm, lse_hbm, dq_ref, dk_ref, dv_ref,
           qbuf, kvbuf, obuf, lse_in, auxr, own_aux, chunk_aux, k_one, v_one, own_qt, own_dot, own_kt, own_vt,
           q_t, do_t, dq_acc, dq_t, dk_t, dv_t,
           stage_sem, recv_sem, aux_recv, own_send, own_aux_send, pair_send, x_send, y_send):
    me = lax.axis_index('cp')
    core, px, py = me % 2, (me // 2) % 2, me // 4
    pair = me + 1 - 2 * core
    nx = me + 2 - 4 * px
    ny = me + 4 - 8 * py
    diag = nx + 4 - 8 * py
    other = pair - me
    mid = (px + py) == 1
    qc, kc = rows // CHUNKS, keys // CHUNKS
    scale = head ** -0.5
    exp_scale = scale * math.log2(math.e)

    def q_copy(slot, n, dest, send, recv):
        part = pl.ds(n * qc, qc)
        return pltpu.make_async_remote_copy(
            qbuf.at[slot, :, part], qbuf.at[slot, :, part], send, recv,
            device_id={'cp': dest}, device_id_type=MESH)

    def kv_copy(slot, n, dest, send, recv):
        part = pl.ds(n * kc, kc)
        return pltpu.make_async_remote_copy(
            kvbuf.at[slot, :, part], kvbuf.at[slot, :, part], send, recv,
            device_id={'cp': dest}, device_id_type=MESH)

    def aux_copy(slot, dest, send):
        return pltpu.make_async_remote_copy(
            auxr.at[slot], auxr.at[slot], send, aux_recv.at[slot],
            device_id={'cp': dest}, device_id_type=MESH)

    stages = [
        pltpu.make_async_copy(k_hbm, kvbuf.at[me, 0], stage_sem.at[0]),
        pltpu.make_async_copy(v_hbm, kvbuf.at[me, 1], stage_sem.at[1]),
        pltpu.make_async_copy(q_hbm, qbuf.at[me, 0], stage_sem.at[2]),
        pltpu.make_async_copy(do_hbm, qbuf.at[me, 1], stage_sem.at[3]),
        pltpu.make_async_copy(o_hbm, obuf, stage_sem.at[4]),
        pltpu.make_async_copy(lse_hbm, lse_in, stage_sem.at[5]),
    ]
    for s in stages:
        s.start()

    barrier = pltpu.get_barrier_semaphore()
    for peer in range(n_dev):
        @pl.when(peer != me)
        def _():
            pl.semaphore_signal(barrier, inc=1, device_id={'cp': peer}, device_id_type=MESH)
    pl.semaphore_wait(barrier, n_dev - 1)

    def order(d, n):
        return (n + 2) % CHUNKS if d == 1 else n

    dests = (pair, nx, ny)
    for s in stages[:4]:
        s.wait()
    for d, dest in enumerate(dests):
        @pl.when(dest > me)
        def _():
            for n in range(CHUNKS):
                c = order(d, n)
                kv_copy(me, c, dest, own_send.at[d], recv_sem.at[me, c]).start()

        @pl.when(dest < me)
        def _():
            c = order(d, 0)
            q_copy(me, c, dest, own_send.at[d], recv_sem.at[me, c]).start()

    for s in stages[4:]:
        s.wait()

    at_row = lax.broadcasted_iota(jnp.int32, (COLS, COLS), 0)
    at_col = lax.broadcasted_iota(jnp.int32, (COLS, COLS), 1)
    weave = jnp.where(at_col == 2 * (at_row % 128) + at_row // 128, 1.0, 0.0).astype(BF16)
    sub = lax.broadcasted_iota(jnp.int32, (16, 128), 0)
    for g in range(rows // 256):
        sides = []
        for h in range(2):
            row = lse_in[h:h + 1, g * 128:(g + 1) * 128] * (1.0 / scale)
            hi, md, lo = parts(row)
            sides.append(jnp.where(sub == 0, hi, jnp.where(sub == 1, md, jnp.where(sub == 2, lo, 0.0))))
        woven = dot(beside(*sides).astype(BF16), weave)
        row = woven[0:1] + (woven[1:2] + woven[2:3])
        n, at = g // 2, (g % 2) * 2
        auxr[me, n, at:at + 1] = row[:, 0:128]
        auxr[me, n, at + 1:at + 2] = row[:, 128:256]

    def delta_rows(n, _):
        for g in range(qc // 128):
            part = pl.ds(pl.multiple_of(n * qc + g * 128, 128), 128)
            d = jnp.sum(qbuf[me, 1, part].astype(F32) * obuf[part].astype(F32), axis=1, keepdims=True)
            auxr[me, n, 4 + g:5 + g] = jnp.transpose(jnp.broadcast_to(d, (128, 128)))[0:1]
        return 0

    lax.fori_loop(0, CHUNKS, delta_rows, 0)

    def aux_lines(slot, n):
        hi, md, lo = parts(auxr[slot, n])
        sub = lax.broadcasted_iota(jnp.int32, (8, 128), 0)
        lines = []
        for g in range(qc // 128):
            m = jnp.zeros((8, 128), F32)
            for i, row in enumerate((hi[g:g + 1], md[g:g + 1], lo[g:g + 1],
                                     hi[4 + g:5 + g], md[4 + g:5 + g], lo[4 + g:5 + g])):
                m = jnp.where(sub == i, row, m)
            lines.append(jnp.concatenate([m, jnp.zeros((120, 128), F32)], axis=0))
        return lines

    def fill_aux(slot, n, dst, base):
        for g, m in enumerate(aux_lines(slot, n)):
            dst[pl.ds(base + g * 128, 128)] = jnp.transpose(m).astype(BF16)

    lane = lax.broadcasted_iota(jnp.int32, (COLS, head), 1)
    line = lax.broadcasted_iota(jnp.int32, (head, keys), 0)
    k_one[...] = jnp.where(lane < 3, -1.0, 0.0).astype(BF16)
    v_one[...] = jnp.where((lane >= 3) & (lane < 6), -1.0, 0.0).astype(BF16)
    own_kt[head:] = jnp.where(line < 3, -1.0, 0.0).astype(BF16)
    own_vt[head:] = jnp.where((line >= 3) & (line < 6), -1.0, 0.0).astype(BF16)
    dq_t[...] = jnp.zeros_like(dq_t)

    def own_fill(n, _):
        base = pl.multiple_of(n * qc, 128)
        part, kpart = pl.ds(base, qc), pl.ds(pl.multiple_of(n * kc, 128), kc)
        for g, m in enumerate(aux_lines(me, n)):
            at = pl.ds(pl.multiple_of(base + g * 128, 128), 128)
            own_aux[at] = jnp.transpose(m).astype(BF16)
            own_qt[head:, at] = m.astype(BF16)
            own_dot[head:, at] = m.astype(BF16)
        own_qt[:head, part] = jnp.transpose(qbuf[me, 0, part])
        own_dot[:head, part] = jnp.transpose(qbuf[me, 1, part])
        own_kt[:head, kpart] = jnp.transpose(kvbuf[me, 0, kpart])
        own_vt[:head, kpart] = jnp.transpose(kvbuf[me, 1, kpart])
        return 0

    lax.fori_loop(0, CHUNKS, own_fill, 0)

    for peer in range(n_dev):
        @pl.when(peer < me)
        def _():
            aux_copy(me, peer, own_aux_send.at[peer]).start()
    for d, dest in enumerate(dests):
        @pl.when(dest < me)
        def _():
            for n in range(1, CHUNKS):
                c = order(d, n)
                q_copy(me, c, dest, own_send.at[d], recv_sem.at[me, c]).start()

    def own_tiles():
        sums = {}
        for rb in range(CHUNKS):
            rpart = pl.ds(rb * qc, qc)
            aux = own_aux[rpart]
            q, do = beside(qbuf[me, 0, rpart], aux), beside(qbuf[me, 1, rpart], aux)
            for cb in range(rb + 1):
                cpart = pl.ds(cb * kc, kc)

                def first(q=q, do=do, cpart=cpart):
                    return dot(q, own_kt[:, cpart]), dot(do, own_vt[:, cpart])

                def second(s, d, rb=rb, cb=cb, rpart=rpart, cpart=cpart):
                    p = jnp.exp2(s * exp_scale)
                    if cb == rb:
                        row = lax.broadcasted_iota(jnp.int32, (qc, kc), 0)
                        col = lax.broadcasted_iota(jnp.int32, (qc, kc), 1)
                        p = jnp.where(2 * col <= row, p, 0.0)
                    ds = (p * d).astype(BF16)
                    dv, dk = dot(own_dot[:head, rpart], p.astype(BF16)), dot(own_qt[:head, rpart], ds)
                    if cb == rb:
                        dv_t[:, cpart] = dv
                        dk_t[:, cpart] = dk
                    else:
                        dv_t[:, cpart] += dv
                        dk_t[:, cpart] += dk
                    dq = dot(ds, kvbuf[me, 0, cpart])
                    sums[rb] = sums[rb] + dq if rb in sums else dq
                    if cb == rb:
                        dq_acc[rpart] = sums[rb]

                yield first, second

    def run(tiles, lead):
        waiting = []
        for first, second in tiles:
            waiting.append((second, first()))
            if len(waiting) > lead:
                second, values = waiting.pop(0)
                second(*values)
        for second, values in waiting:
            second(*values)

    run(own_tiles(), LEAD_D)

    def plan(t):
        na, ka = (t - 2) // 2, t % 2
        nb = (t - 10) // 2
        first, second = t < 2, t < 10
        hop = jnp.where(ka == 1, other, 0)

        def pick(a, b, c):
            return jnp.where(first, a, jnp.where(second, b, c))

        stream_a = pick(3, jnp.where(ka == 0, 0, 3), jnp.where(ka == 0, 2, 3))
        stream_b = pick(3, jnp.where(ka == 0, 1, 3), jnp.where(ka == 0, 2, 3))
        src_a = pick(pair, nx + hop, diag + hop)
        src_b = pick(pair, ny + hop, diag + hop)
        piece_a = pick(2 * t, (na + 2) % CHUNKS, jnp.where(mid, 2 * nb, nb))
        piece_b = pick(2 * t + 1, na, jnp.where(mid, 2 * nb + 1, nb + 2))
        swap = (src_a > me) & (src_b < me)

        def swapped(a, b):
            return jnp.where(swap, b, a), jnp.where(swap, a, b)

        stream_a, stream_b = swapped(stream_a, stream_b)
        src_a, src_b = swapped(src_a, src_b)
        piece_a, piece_b = swapped(piece_a, piece_b)
        return (stream_a, src_a, piece_a), (stream_b, src_b, piece_b)

    def arrive(item):
        stream, src, piece = item
        idx = jnp.minimum(stream, 2)
        recv = recv_sem.at[src, piece]
        to_x = (stream == 1) & (jnp.logical_not(mid) | (piece < 2))
        to_y = (stream == 0) & mid & (piece >= 2)
        for make, want in ((q_copy, src > me), (kv_copy, src < me)):
            @pl.when(want)
            def _():
                make(src, piece, me, x_send, recv).wait_recv()

                @pl.when(to_x)
                def _():
                    make(src, piece, nx, x_send, recv).start()

                @pl.when(to_y)
                def _():
                    make(src, piece, ny, y_send, recv).start()

                @pl.when(stream < 3)
                def _():
                    make(src, piece, pair, pair_send.at[idx], recv).start()

    def keys_grads(items, cur):
        loaded = []
        for idx, (_, src, piece) in items:
            part = pl.ds(pl.multiple_of(piece * qc, qc), qc)
            q, do, aux = qbuf[src, 0, part], qbuf[src, 1, part], chunk_aux[cur, idx]
            q_t[idx] = jnp.transpose(q)
            do_t[idx] = jnp.transpose(do)
            loaded.append((idx, beside(q, aux), beside(do, aux)))
        sums = {}
        for cb in range(keys // COLS):
            cpart = pl.ds(cb * COLS, COLS)
            for idx, q, do in loaded:
                def first(q=q, do=do, cpart=cpart):
                    return dot(q, own_kt[:, cpart]), dot(do, own_vt[:, cpart])

                def second(s, d, idx=idx, cpart=cpart, cb=cb):
                    p = jnp.exp2(s * exp_scale)
                    ds = (p * d).astype(BF16)
                    dv, dk = dot(do_t[idx], p.astype(BF16)), dot(q_t[idx], ds)
                    if cb in sums:
                        dv, dk = sums[cb][0] + dv, sums[cb][1] + dk
                    sums[cb] = (dv, dk)
                    if idx == items[-1][0]:
                        dv_t[:, cpart] += dv
                        dk_t[:, cpart] += dk

                yield first, second

    def rows_grad(items, width):
        ks, vs = [], []
        for idx, (_, src, piece) in items:
            part = pl.ds(pl.multiple_of(piece * kc, kc), kc)
            ks.append(kvbuf[src, 0, part])
            vs.append(kvbuf[src, 1, part])
        k_ts = [jnp.transpose(k) for k in ks]
        k = jnp.concatenate([beside(k, k_one[...]) for k in ks], axis=0)
        v = jnp.concatenate([beside(v, v_one[...]) for v in vs], axis=0)
        k_t = k_ts[0] if len(k_ts) == 1 else beside(*k_ts)
        for rb in range(rows // width):
            part = pl.ds(rb * width, width)

            def first(part=part):
                return dot(k, own_qt[:, part]), dot(v, own_dot[:, part])

            def second(s, d, part=part):
                ds = (jnp.exp2(s * exp_scale) * d).astype(BF16)
                dq_t[:, part] += dot(k_t, ds)

            yield first, second

    def mixed(xs, ys):
        xs, ys = list(xs), list(ys)
        for i in range(max(len(xs), len(ys))):
            yield from xs[i:i + 1]
            yield from ys[i:i + 1]

    def prefetch(t, idx):
        _, src, piece = plan(t)[idx]
        fill_aux(jnp.where(src > me, src, me), piece, chunk_aux.at[t % 2, idx], 0)

    @pl.when(pair > me)
    def _():
        aux_copy(pair, me, own_aux_send.at[0]).wait_recv()
        for idx in range(2):
            prefetch(0, idx)

    def step(t, _):
        a, b = plan(t)
        cur = t % 2

        @pl.when(t == 1)
        def _():
            for peer in range(n_dev):
                @pl.when((peer > me) & (peer != pair))
                def _():
                    aux_copy(peer, me, own_aux_send.at[0]).wait_recv()

        arrive(a)
        arrive(b)
        a_keys, b_keys = a[1] < me, b[1] < me
        later = jnp.minimum(t + 1, STEPS - 1)

        def ahead():
            for idx in range(2):
                _, src, piece = plan(later)[idx]
                fill_aux(jnp.where(src > me, src, me), piece, chunk_aux.at[1 - cur, idx], 0)

        @pl.when(jnp.logical_not(a_keys))
        def _():
            run(keys_grads(((0, a), (1, b)), cur), LEAD_Q)
            ahead()

        @pl.when(a_keys & b_keys)
        def _():
            run(rows_grad(((0, a), (1, b)), WIDTH_K), LEAD_K)
            ahead()

        @pl.when(a_keys & jnp.logical_not(b_keys))
        def _():
            run(mixed(rows_grad(((0, a),), WIDTH_M), keys_grads(((1, b),), cur)), LEAD_M)
            ahead()

        return 0

    lax.fori_loop(0, STEPS, step, 0)

    dq_ref[...] = ((dq_acc[...] + jnp.transpose(dq_t[...])) * scale).astype(BF16)
    dk_ref[...] = (jnp.transpose(dk_t[...]) * scale).astype(BF16)
    dv_ref[...] = jnp.transpose(dv_t[...]).astype(BF16)

    for peer in range(n_dev):
        @pl.when(peer < me)
        def _():
            aux_copy(me, peer, own_aux_send.at[peer]).wait_send()

    def left(buf, slot, length, send, want):
        @pl.when(want)
        def _():
            block = buf.at[slot, :, pl.ds(0, length)]
            pltpu.make_async_remote_copy(block, block, send, recv_sem.at[slot, 0],
                                         device_id={'cp': pair}, device_id_type=MESH).wait_send()

    for buf, size, sign in ((qbuf, rows, 1), (kvbuf, keys, -1)):
        for d, dest in enumerate(dests):
            left(buf, me, size, own_send.at[d], sign * dest < sign * me)
        for d, src in enumerate((nx, ny, diag)):
            left(buf, src, size, pair_send.at[d], sign * src > sign * me)
        left(buf, ny, size, x_send, (sign * ny > sign * me) & jnp.logical_not(mid))
        left(buf, ny, size // 2, x_send, (sign * ny > sign * me) & mid)
        left(buf, nx, size // 2, y_send, (sign * nx > sign * me) & mid)


def store(*refs):
    n = len(refs) // 2
    copies = [pltpu.make_async_copy(refs[i], refs[n + i], refs[-1].at[i]) for i in range(n)]
    for c in copies:
        c.start()
    for c in copies:
        c.wait()


def solution(mesh):
    n_dev = mesh.shape['cp']
    row_spec = P(('dp', 'cp'))

    def local_fn(q_tok, k_tok, v_tok, fwd_out, d_out, lse_row):
        tokens, groups, head = q_tok.shape
        rows = tokens * groups
        piece = rows // CHUNKS
        flat = lambda x: x.reshape(rows, head)
        dma = pltpu.SemaphoreType.DMA
        vmem = pltpu.VMEM
        grad_q, grad_k, grad_v = pl.pallas_call(
            functools.partial(kernel, rows, tokens, head, n_dev),
            out_shape=(jax.ShapeDtypeStruct((rows, head), BF16),
                       jax.ShapeDtypeStruct((tokens, head), BF16),
                       jax.ShapeDtypeStruct((tokens, head), BF16)),
            in_specs=[pl.BlockSpec(memory_space=pltpu.HBM)] * 6,
            out_specs=(pl.BlockSpec(memory_space=vmem),) * 3,
            scratch_shapes=[
                vmem((n_dev, 2, rows, head), BF16),
                vmem((n_dev, 2, tokens, head), BF16),
                vmem((rows, head), BF16),
                vmem((groups, tokens), F32),
                vmem((n_dev, CHUNKS, 8, 128), F32),
                vmem((rows, head), BF16),
                vmem((2, 2, piece, head), BF16),
                vmem((COLS, head), BF16),
                vmem((COLS, head), BF16),
                vmem((2 * head, rows), BF16),
                vmem((2 * head, rows), BF16),
                vmem((2 * head, tokens), BF16),
                vmem((2 * head, tokens), BF16),
                vmem((2, head, piece), BF16),
                vmem((2, head, piece), BF16),
                vmem((rows, head), F32),
                vmem((head, rows), F32),
                vmem((head, tokens), F32),
                vmem((head, tokens), F32),
                dma((6,)),
                dma((n_dev, CHUNKS)),
                dma((n_dev,)),
                dma((3,)),
                dma((n_dev,)),
                dma((3,)),
                dma,
                dma,
            ],
            compiler_params=pltpu.CompilerParams(
                collective_id=0, has_side_effects=True, vmem_limit_bytes=48 * 1024 * 1024),
            name='attention_backward',
        )(*[pltpu.with_memory_space_constraint(x, pltpu.HBM) for x in (flat(q_tok), k_tok, v_tok, flat(fwd_out), flat(d_out), lse_row.T)])
        grads = (grad_q, grad_k, grad_v)
        any_space = pl.BlockSpec(memory_space=pl.ANY)
        grad_q, grad_k, grad_v = pl.pallas_call(
            store,
            out_shape=tuple(jax.ShapeDtypeStruct(g.shape, g.dtype) for g in grads),
            in_specs=[any_space] * 3,
            out_specs=(any_space,) * 3,
            scratch_shapes=[dma((3,))],
            compiler_params=pltpu.CompilerParams(vmem_limit_bytes=1024 * 1024),
            name='store_grads',
        )(*[pltpu.with_memory_space_constraint(g, vmem) for g in grads])
        return grad_q.reshape(tokens, groups, head), grad_k, grad_v

    return jax.shard_map(local_fn, mesh=mesh, in_specs=(row_spec,) * 6, out_specs=(row_spec,) * 3, check_vma=False)
```

```python
import functools
import math

import jax
import jax.numpy as jnp
from jax import lax
from jax.experimental import pallas as pl
from jax.experimental.pallas import tpu as pltpu
from jax.sharding import PartitionSpec as P

BF16, F32 = jnp.bfloat16, jnp.float32
CHUNKS = 4
COLS = 256
STEPS, LAST_STEPS = 10, 8
LEAD_Q, LEAD_K, LEAD_M = 4, 4, 2
LEAD_D = 2
WIDTH_K, WIDTH_M = 256, 512
MESH = pl.DeviceIdType.MESH


def dot(a, b):
    return jnp.dot(a, b, preferred_element_type=F32)


def beside(a, b):
    return jnp.concatenate([a, b], axis=1)


def parts(x):
    hi = x.astype(BF16).astype(F32)
    rest = x - hi
    md = rest.astype(BF16).astype(F32)
    return hi, md, rest - md


def kernel(rows, keys, head, n_dev, q_hbm, k_hbm, v_hbm, o_hbm, do_hbm, lse_hbm, dq_ref, dk_ref, dv_ref,
           qbuf, kvbuf, obuf, lse_in, auxr, own_aux, chunk_aux, k_one, v_one, own_qt, own_dot, own_kt, own_vt,
           q_t, do_t, dq_acc, dq_t, dk_t, dv_t,
           stage_sem, recv_sem, half_recv, aux_recv, own_send, own_aux_send, pair_send, x_send, y_send):
    me = lax.axis_index('cp')
    core, px, py = me % 2, (me // 2) % 2, me // 4
    pair = me + 1 - 2 * core
    nx = me + 2 - 4 * px
    ny = me + 4 - 8 * py
    diag = nx + 4 - 8 * py
    other = pair - me
    mid = (px + py) == 1
    qc, kc = rows // CHUNKS, keys // CHUNKS
    scale = head ** -0.5
    exp_scale = scale * math.log2(math.e)

    def q_copy(slot, n, dest, send, recv, halves=1):
        part = pl.ds(n * (qc // halves), qc // halves)
        return pltpu.make_async_remote_copy(
            qbuf.at[slot, :, part], qbuf.at[slot, :, part], send, recv,
            device_id={'cp': dest}, device_id_type=MESH)

    def kv_copy(slot, n, dest, send, recv, halves=1):
        part = pl.ds(n * (kc // halves), kc // halves)
        return pltpu.make_async_remote_copy(
            kvbuf.at[slot, :, part], kvbuf.at[slot, :, part], send, recv,
            device_id={'cp': dest}, device_id_type=MESH)

    def aux_copy(slot, dest, send):
        return pltpu.make_async_remote_copy(
            auxr.at[slot], auxr.at[slot], send, aux_recv.at[slot],
            device_id={'cp': dest}, device_id_type=MESH)

    stages = [
        pltpu.make_async_copy(k_hbm, kvbuf.at[me, 0], stage_sem.at[0]),
        pltpu.make_async_copy(v_hbm, kvbuf.at[me, 1], stage_sem.at[1]),
        pltpu.make_async_copy(q_hbm, qbuf.at[me, 0], stage_sem.at[2]),
        pltpu.make_async_copy(do_hbm, qbuf.at[me, 1], stage_sem.at[3]),
        pltpu.make_async_copy(o_hbm, obuf, stage_sem.at[4]),
        pltpu.make_async_copy(lse_hbm, lse_in, stage_sem.at[5]),
    ]
    for s in stages:
        s.start()

    barrier = pltpu.get_barrier_semaphore()
    for peer in range(n_dev):
        @pl.when(peer != me)
        def _():
            pl.semaphore_signal(barrier, inc=1, device_id={'cp': peer}, device_id_type=MESH)
    pl.semaphore_wait(barrier, n_dev - 1)

    def order(d, n):
        return (n + 2) % CHUNKS if d == 1 else n

    dests = (pair, nx, ny)
    for s in stages[:4]:
        s.wait()
    for d, dest in enumerate(dests):
        @pl.when(dest > me)
        def _():
            for n in range(CHUNKS):
                c = order(d, n)
                kv_copy(me, c, dest, own_send.at[d], recv_sem.at[me, c]).start()

        @pl.when(dest < me)
        def _():
            c = order(d, 0)
            q_copy(me, c, dest, own_send.at[d], recv_sem.at[me, c]).start()

    for s in stages[4:]:
        s.wait()

    at_row = lax.broadcasted_iota(jnp.int32, (COLS, COLS), 0)
    at_col = lax.broadcasted_iota(jnp.int32, (COLS, COLS), 1)
    weave = jnp.where(at_col == 2 * (at_row % 128) + at_row // 128, 1.0, 0.0).astype(BF16)
    sub = lax.broadcasted_iota(jnp.int32, (16, 128), 0)
    for g in range(rows // 256):
        sides = []
        for h in range(2):
            row = lse_in[h:h + 1, g * 128:(g + 1) * 128] * (1.0 / scale)
            hi, md, lo = parts(row)
            sides.append(jnp.where(sub == 0, hi, jnp.where(sub == 1, md, jnp.where(sub == 2, lo, 0.0))))
        woven = dot(beside(*sides).astype(BF16), weave)
        row = woven[0:1] + (woven[1:2] + woven[2:3])
        n, at = g // 2, (g % 2) * 2
        auxr[me, n, at:at + 1] = row[:, 0:128]
        auxr[me, n, at + 1:at + 2] = row[:, 128:256]

    def delta_rows(n, _):
        for g in range(qc // 128):
            part = pl.ds(pl.multiple_of(n * qc + g * 128, 128), 128)
            d = jnp.sum(qbuf[me, 1, part].astype(F32) * obuf[part].astype(F32), axis=1, keepdims=True)
            auxr[me, n, 4 + g:5 + g] = jnp.transpose(jnp.broadcast_to(d, (128, 128)))[0:1]
        return 0

    lax.fori_loop(0, CHUNKS, delta_rows, 0)

    def aux_lines(slot, n):
        hi, md, lo = parts(auxr[slot, n])
        return [stack_lines((hi[g:g + 1], md[g:g + 1], lo[g:g + 1], hi[4 + g:5 + g], md[4 + g:5 + g], lo[4 + g:5 + g]))
                for g in range(qc // 128)]

    def half_lines(slot, half):
        n, at = half // 2, (half % 2) * 2
        return [stack_lines(parts(auxr[slot, n, pl.ds(at + g, 1)]) + parts(auxr[slot, n, pl.ds(4 + at + g, 1)]))
                for g in range(qc // 256)]

    def stack_lines(lines):
        sub = lax.broadcasted_iota(jnp.int32, (8, 128), 0)
        m = jnp.zeros((8, 128), F32)
        for i, line in enumerate(lines):
            m = jnp.where(sub == i, line, m)
        return jnp.concatenate([m, jnp.zeros((120, 128), F32)], axis=0)

    def fill_aux(lines, dst):
        for g, m in enumerate(lines):
            dst[pl.ds(g * 128, 128)] = jnp.transpose(m).astype(BF16)

    lane = lax.broadcasted_iota(jnp.int32, (COLS, head), 1)
    line = lax.broadcasted_iota(jnp.int32, (head, keys), 0)
    k_one[...] = jnp.where(lane < 3, -1.0, 0.0).astype(BF16)
    v_one[...] = jnp.where((lane >= 3) & (lane < 6), -1.0, 0.0).astype(BF16)
    own_kt[head:] = jnp.where(line < 3, -1.0, 0.0).astype(BF16)
    own_vt[head:] = jnp.where((line >= 3) & (line < 6), -1.0, 0.0).astype(BF16)
    dq_t[...] = jnp.zeros_like(dq_t)

    def own_fill(n, _):
        base = pl.multiple_of(n * qc, 128)
        part, kpart = pl.ds(base, qc), pl.ds(pl.multiple_of(n * kc, 128), kc)
        for g, m in enumerate(aux_lines(me, n)):
            at = pl.ds(pl.multiple_of(base + g * 128, 128), 128)
            own_aux[at] = jnp.transpose(m).astype(BF16)
            own_qt[head:, at] = m.astype(BF16)
            own_dot[head:, at] = m.astype(BF16)
        own_qt[:head, part] = jnp.transpose(qbuf[me, 0, part])
        own_dot[:head, part] = jnp.transpose(qbuf[me, 1, part])
        own_kt[:head, kpart] = jnp.transpose(kvbuf[me, 0, kpart])
        own_vt[:head, kpart] = jnp.transpose(kvbuf[me, 1, kpart])
        return 0

    lax.fori_loop(0, CHUNKS, own_fill, 0)

    for peer in range(n_dev):
        @pl.when(peer < me)
        def _():
            aux_copy(me, peer, own_aux_send.at[peer]).start()
    for d, dest in enumerate(dests):
        @pl.when(dest < me)
        def _():
            for n in range(1, CHUNKS):
                c = order(d, n)
                q_copy(me, c, dest, own_send.at[d], recv_sem.at[me, c]).start()

    def own_tiles():
        sums = {}
        for rb in range(CHUNKS):
            rpart = pl.ds(rb * qc, qc)
            aux = own_aux[rpart]
            q, do = beside(qbuf[me, 0, rpart], aux), beside(qbuf[me, 1, rpart], aux)
            for cb in range(rb + 1):
                cpart = pl.ds(cb * kc, kc)

                def first(q=q, do=do, cpart=cpart):
                    return dot(q, own_kt[:, cpart]), dot(do, own_vt[:, cpart])

                def second(s, d, rb=rb, cb=cb, rpart=rpart, cpart=cpart):
                    p = jnp.exp2(s * exp_scale)
                    if cb == rb:
                        row = lax.broadcasted_iota(jnp.int32, (qc, kc), 0)
                        col = lax.broadcasted_iota(jnp.int32, (qc, kc), 1)
                        p = jnp.where(2 * col <= row, p, 0.0)
                    ds = (p * d).astype(BF16)
                    dv, dk = dot(own_dot[:head, rpart], p.astype(BF16)), dot(own_qt[:head, rpart], ds)
                    if cb == rb:
                        dv_t[:, cpart] = dv
                        dk_t[:, cpart] = dk
                    else:
                        dv_t[:, cpart] += dv
                        dk_t[:, cpart] += dk
                    dq = dot(ds, kvbuf[me, 0, cpart])
                    sums[rb] = sums[rb] + dq if rb in sums else dq
                    if cb == rb:
                        dq_acc[rpart] = sums[rb]

                yield first, second

    def run(tiles, lead):
        waiting = []
        for first, second in tiles:
            waiting.append((second, first()))
            if len(waiting) > lead:
                second, values = waiting.pop(0)
                second(*values)
        for second, values in waiting:
            second(*values)

    run(own_tiles(), LEAD_D)

    def plan(t):
        na, ka = (t - 2) // 2, t % 2
        early = t < 2
        hop = jnp.where(ka == 1, other, 0)
        stream_a = jnp.where(early | (ka == 1), 3, 0)
        stream_b = jnp.where(early | (ka == 1), 3, 1)
        src_a = jnp.where(early, pair, nx + hop)
        src_b = jnp.where(early, pair, ny + hop)
        piece_a = jnp.where(early, 2 * t, (na + 2) % CHUNKS)
        piece_b = jnp.where(early, 2 * t + 1, na)
        swap = (src_a > me) & (src_b < me)

        def swapped(a, b):
            return jnp.where(swap, b, a), jnp.where(swap, a, b)

        stream_a, stream_b = swapped(stream_a, stream_b)
        src_a, src_b = swapped(src_a, src_b)
        piece_a, piece_b = swapped(piece_a, piece_b)
        return (stream_a, src_a, piece_a), (stream_b, src_b, piece_b)

    def last_plan(t):
        n = t // 2
        src = diag + jnp.where(t % 2 == 1, other, 0)
        half_a = jnp.where(mid, 2 * n, n)
        half_b = jnp.where(mid, 2 * n + 1, n + CHUNKS)
        return src, (half_a, half_b)

    def arrive(item):
        stream, src, piece = item
        idx = jnp.minimum(stream, 1)
        recv = recv_sem.at[src, piece]
        to_x = (stream == 1) & (jnp.logical_not(mid) | (piece < 2))
        to_y = (stream == 0) & mid & (piece >= 2)
        for make, want in ((q_copy, src > me), (kv_copy, src < me)):
            @pl.when(want)
            def _():
                make(src, piece, me, x_send, recv).wait_recv()

                @pl.when(to_x)
                def _():
                    for h in range(2):
                        half = 2 * piece + h
                        make(src, half, nx, x_send, half_recv.at[src, half], 2).start()

                @pl.when(to_y)
                def _():
                    for h in range(2):
                        half = 2 * piece + h
                        make(src, half, ny, y_send, half_recv.at[src, half], 2).start()

                @pl.when(stream < 3)
                def _():
                    make(src, piece, pair, pair_send.at[idx], recv).start()

    def arrive_half(t, src, half):
        recv = half_recv.at[src, half]
        for make, want in ((q_copy, src > me), (kv_copy, src < me)):
            @pl.when(want)
            def _():
                make(src, half, me, x_send, recv, 2).wait_recv()

                @pl.when(t % 2 == 0)
                def _():
                    make(src, half, pair, pair_send.at[2], recv, 2).start()

    def keys_grads(items, cur, size):
        loaded = []
        for idx, src, piece in items:
            part = pl.ds(pl.multiple_of(piece * size, size), size)
            q, do, aux = qbuf[src, 0, part], qbuf[src, 1, part], chunk_aux[cur, idx, :size]
            q_t[idx, :, :size] = jnp.transpose(q)
            do_t[idx, :, :size] = jnp.transpose(do)
            loaded.append((idx, beside(q, aux), beside(do, aux)))
        sums = {}
        for cb in range(keys // COLS):
            cpart = pl.ds(cb * COLS, COLS)
            for idx, q, do in loaded:
                def first(q=q, do=do, cpart=cpart):
                    return dot(q, own_kt[:, cpart]), dot(do, own_vt[:, cpart])

                def second(s, d, idx=idx, cpart=cpart, cb=cb):
                    p = jnp.exp2(s * exp_scale)
                    ds = (p * d).astype(BF16)
                    dv, dk = dot(do_t[idx, :, :size], p.astype(BF16)), dot(q_t[idx, :, :size], ds)
                    if cb in sums:
                        dv, dk = sums[cb][0] + dv, sums[cb][1] + dk
                    sums[cb] = (dv, dk)
                    if idx == items[-1][0]:
                        dv_t[:, cpart] += dv
                        dk_t[:, cpart] += dk

                yield first, second

    def rows_grad(items, width, size):
        ks, vs = [], []
        for idx, src, piece in items:
            part = pl.ds(pl.multiple_of(piece * size, size), size)
            ks.append(kvbuf[src, 0, part])
            vs.append(kvbuf[src, 1, part])
        k_ts = [jnp.transpose(k) for k in ks]
        k = jnp.concatenate([beside(k, k_one[:size]) for k in ks], axis=0)
        v = jnp.concatenate([beside(v, v_one[:size]) for v in vs], axis=0)
        k_t = k_ts[0] if len(k_ts) == 1 else beside(*k_ts)
        for rb in range(rows // width):
            part = pl.ds(rb * width, width)

            def first(part=part):
                return dot(k, own_qt[:, part]), dot(v, own_dot[:, part])

            def second(s, d, part=part):
                ds = (jnp.exp2(s * exp_scale) * d).astype(BF16)
                dq_t[:, part] += dot(k_t, ds)

            yield first, second

    def mixed(xs, ys):
        xs, ys = list(xs), list(ys)
        for i in range(max(len(xs), len(ys))):
            yield from xs[i:i + 1]
            yield from ys[i:i + 1]

    def present(src):
        return jnp.where(src > me, src, me)

    def ahead(t, slot):
        for idx, (_, src, piece) in enumerate(plan(t)):
            fill_aux(aux_lines(present(src), piece), chunk_aux.at[slot, idx])

    def last_ahead(t, slot):
        src, halves = last_plan(t)
        for idx, half in enumerate(halves):
            fill_aux(half_lines(present(src), half), chunk_aux.at[slot, idx])

    @pl.when(pair > me)
    def _():
        aux_copy(pair, me, own_aux_send.at[0]).wait_recv()
        ahead(0, 0)

    def step(t, _):
        a, b = plan(t)
        cur = t % 2

        @pl.when(t == 1)
        def _():
            for peer in range(n_dev):
                @pl.when((peer > me) & (peer != pair))
                def _():
                    aux_copy(peer, me, own_aux_send.at[0]).wait_recv()

        arrive(a)
        arrive(b)
        a_keys, b_keys = a[1] < me, b[1] < me
        later = jnp.minimum(t + 1, STEPS - 1)
        a, b = (0,) + a[1:], (1,) + b[1:]

        @pl.when(jnp.logical_not(a_keys))
        def _():
            run(keys_grads((a, b), cur, qc), LEAD_Q)
            ahead(later, 1 - cur)

        @pl.when(a_keys & b_keys)
        def _():
            run(rows_grad((a, b), WIDTH_K, kc), LEAD_K)
            ahead(later, 1 - cur)

        @pl.when(a_keys & jnp.logical_not(b_keys))
        def _():
            run(mixed(rows_grad((a,), WIDTH_M, kc), keys_grads((b,), cur, qc)), LEAD_M)
            ahead(later, 1 - cur)

        return 0

    lax.fori_loop(0, STEPS, step, 0)

    def finish_rows():
        dq_ref[...] = ((dq_acc[...] + jnp.transpose(dq_t[...])) * scale).astype(BF16)

    def finish_keys():
        dk_ref[...] = (jnp.transpose(dk_t[...]) * scale).astype(BF16)
        dv_ref[...] = jnp.transpose(dv_t[...]).astype(BF16)

    @pl.when(diag > me)
    def _():
        last_ahead(0, 0)
        finish_rows()

    @pl.when(diag < me)
    def _():
        finish_keys()

    def last_step(t, _):
        src, halves = last_plan(t)
        cur = t % 2
        for half in halves:
            arrive_half(t, src, half)
        items = [(idx, src, half) for idx, half in enumerate(halves)]

        @pl.when(src > me)
        def _():
            run(keys_grads(items, cur, qc // 2), LEAD_Q)
            last_ahead(jnp.minimum(t + 1, LAST_STEPS - 1), 1 - cur)

        @pl.when(src < me)
        def _():
            run(rows_grad(items, WIDTH_K, kc // 2), LEAD_K)

        return 0

    lax.fori_loop(0, LAST_STEPS, last_step, 0)

    @pl.when(diag > me)
    def _():
        finish_keys()

    @pl.when(diag < me)
    def _():
        finish_rows()

    for peer in range(n_dev):
        @pl.when(peer < me)
        def _():
            aux_copy(me, peer, own_aux_send.at[peer]).wait_send()

    def left(buf, slot, length, send, want):
        @pl.when(want)
        def _():
            block = buf.at[slot, :, pl.ds(0, length)]
            pltpu.make_async_remote_copy(block, block, send, recv_sem.at[slot, 0],
                                         device_id={'cp': pair}, device_id_type=MESH).wait_send()

    for buf, size, sign in ((qbuf, rows, 1), (kvbuf, keys, -1)):
        for d, dest in enumerate(dests):
            left(buf, me, size, own_send.at[d], sign * dest < sign * me)
        for d, src in enumerate((nx, ny, diag)):
            left(buf, src, size, pair_send.at[d], sign * src > sign * me)
        left(buf, ny, size, x_send, (sign * ny > sign * me) & jnp.logical_not(mid))
        left(buf, ny, size // 2, x_send, (sign * ny > sign * me) & mid)
        left(buf, nx, size // 2, y_send, (sign * nx > sign * me) & mid)


def store(*refs):
    n = len(refs) // 2
    copies = [pltpu.make_async_copy(refs[i], refs[n + i], refs[-1].at[i]) for i in range(n)]
    for c in copies:
        c.start()
    for c in copies:
        c.wait()


def solution(mesh):
    n_dev = mesh.shape['cp']
    row_spec = P(('dp', 'cp'))

    def local_fn(q_tok, k_tok, v_tok, fwd_out, d_out, lse_row):
        tokens, groups, head = q_tok.shape
        rows = tokens * groups
        piece = rows // CHUNKS
        flat = lambda x: x.reshape(rows, head)
        dma = pltpu.SemaphoreType.DMA
        vmem = pltpu.VMEM
        grad_q, grad_k, grad_v = pl.pallas_call(
            functools.partial(kernel, rows, tokens, head, n_dev),
            out_shape=(jax.ShapeDtypeStruct((rows, head), BF16),
                       jax.ShapeDtypeStruct((tokens, head), BF16),
                       jax.ShapeDtypeStruct((tokens, head), BF16)),
            in_specs=[pl.BlockSpec(memory_space=pltpu.HBM)] * 6,
            out_specs=(pl.BlockSpec(memory_space=vmem),) * 3,
            scratch_shapes=[
                vmem((n_dev, 2, rows, head), BF16),
                vmem((n_dev, 2, tokens, head), BF16),
                vmem((rows, head), BF16),
                vmem((groups, tokens), F32),
                vmem((n_dev, CHUNKS, 8, 128), F32),
                vmem((rows, head), BF16),
                vmem((2, 2, piece, head), BF16),
                vmem((COLS, head), BF16),
                vmem((COLS, head), BF16),
                vmem((2 * head, rows), BF16),
                vmem((2 * head, rows), BF16),
                vmem((2 * head, tokens), BF16),
                vmem((2 * head, tokens), BF16),
                vmem((2, head, piece), BF16),
                vmem((2, head, piece), BF16),
                vmem((rows, head), F32),
                vmem((head, rows), F32),
                vmem((head, tokens), F32),
                vmem((head, tokens), F32),
                dma((6,)),
                dma((n_dev, CHUNKS)),
                dma((n_dev, 2 * CHUNKS)),
                dma((n_dev,)),
                dma((3,)),
                dma((n_dev,)),
                dma((3,)),
                dma,
                dma,
            ],
            compiler_params=pltpu.CompilerParams(
                collective_id=0, has_side_effects=True, vmem_limit_bytes=48 * 1024 * 1024),
            name='attention_backward',
        )(*[pltpu.with_memory_space_constraint(x, pltpu.HBM) for x in (flat(q_tok), k_tok, v_tok, flat(fwd_out), flat(d_out), lse_row.T)])
        grads = (grad_q, grad_k, grad_v)
        any_space = pl.BlockSpec(memory_space=pl.ANY)
        grad_q, grad_k, grad_v = pl.pallas_call(
            store,
            out_shape=tuple(jax.ShapeDtypeStruct(g.shape, g.dtype) for g in grads),
            in_specs=[any_space] * 3,
            out_specs=(any_space,) * 3,
            scratch_shapes=[dma((3,))],
            compiler_params=pltpu.CompilerParams(vmem_limit_bytes=1024 * 1024),
            name='store_grads',
        )(*[pltpu.with_memory_space_constraint(g, vmem) for g in grads])
        return grad_q.reshape(tokens, groups, head), grad_k, grad_v

    return jax.shard_map(local_fn, mesh=mesh, in_specs=(row_spec,) * 6, out_specs=(row_spec,) * 3, check_vma=False)
```

```python
import functools
import math

import jax
import jax.numpy as jnp
from jax import lax
from jax.experimental import pallas as pl
from jax.experimental.pallas import tpu as pltpu
from jax.sharding import PartitionSpec as P

BF16, F32 = jnp.bfloat16, jnp.float32
CHUNKS = 4
COLS = 256
STEPS, LAST_STEPS = 10, 8
LEAD_Q, LEAD_K, LEAD_M = 4, 4, 2
LEAD_D = 2
WIDTH_K, WIDTH_M = 256, 512
MESH = pl.DeviceIdType.MESH


def dot(a, b):
    return jnp.dot(a, b, preferred_element_type=F32)


def beside(a, b):
    return jnp.concatenate([a, b], axis=1)


def parts(x):
    hi = x.astype(BF16).astype(F32)
    rest = x - hi
    md = rest.astype(BF16).astype(F32)
    return hi, md, rest - md


def kernel(rows, keys, head, n_dev, q_hbm, k_hbm, v_hbm, o_hbm, do_hbm, lse_hbm, dq_ref, dk_ref, dv_ref,
           qbuf, kvbuf, obuf, lse_in, auxr, own_aux, chunk_aux, k_one, v_one, own_qt, own_dot, own_kt, own_vt,
           q_t, do_t, dq_acc, dq_t, dk_t, dv_t,
           stage_sem, recv_sem, half_recv, aux_recv, own_send, own_aux_send, pair_send, x_send, y_send):
    me = lax.axis_index('cp')
    core, px, py = me % 2, (me // 2) % 2, me // 4
    pair = me + 1 - 2 * core
    nx = me + 2 - 4 * px
    ny = me + 4 - 8 * py
    diag = nx + 4 - 8 * py
    other = pair - me
    mid = (px + py) == 1
    qc, kc = rows // CHUNKS, keys // CHUNKS
    scale = head ** -0.5
    exp_scale = scale * math.log2(math.e)

    def q_copy(slot, n, dest, send, recv, halves=1):
        part = pl.ds(n * (qc // halves), qc // halves)
        return pltpu.make_async_remote_copy(
            qbuf.at[slot, :, part], qbuf.at[slot, :, part], send, recv,
            device_id={'cp': dest}, device_id_type=MESH)

    def kv_copy(slot, n, dest, send, recv, halves=1):
        part = pl.ds(n * (kc // halves), kc // halves)
        return pltpu.make_async_remote_copy(
            kvbuf.at[slot, :, part], kvbuf.at[slot, :, part], send, recv,
            device_id={'cp': dest}, device_id_type=MESH)

    def aux_copy(slot, dest, send):
        return pltpu.make_async_remote_copy(
            auxr.at[slot], auxr.at[slot], send, aux_recv.at[slot],
            device_id={'cp': dest}, device_id_type=MESH)

    stages = [
        pltpu.make_async_copy(k_hbm, kvbuf.at[me, 0], stage_sem.at[0]),
        pltpu.make_async_copy(v_hbm, kvbuf.at[me, 1], stage_sem.at[1]),
        pltpu.make_async_copy(q_hbm, qbuf.at[me, 0], stage_sem.at[2]),
        pltpu.make_async_copy(do_hbm, qbuf.at[me, 1], stage_sem.at[3]),
        pltpu.make_async_copy(o_hbm, obuf, stage_sem.at[4]),
        pltpu.make_async_copy(lse_hbm, lse_in, stage_sem.at[5]),
    ]
    for s in stages:
        s.start()

    barrier = pltpu.get_barrier_semaphore()
    for peer in range(n_dev):
        @pl.when(peer != me)
        def _():
            pl.semaphore_signal(barrier, inc=1, device_id={'cp': peer}, device_id_type=MESH)
    pl.semaphore_wait(barrier, n_dev - 1)

    def order(d, n):
        return (n + 2) % CHUNKS if d == 1 else n

    dests = (pair, nx, ny)
    for s in stages[:4]:
        s.wait()
    def send_keys(d, n):
        c = order(d, n)
        kv_copy(me, c, dests[d], own_send.at[d], recv_sem.at[me, c]).start()

    def send_rows(d, n):
        c = order(d, n)
        q_copy(me, c, dests[d], own_send.at[d], recv_sem.at[me, c]).start()

    for n in range(CHUNKS):
        for d in (1, 2, 0):
            pl.when(dests[d] > me)(functools.partial(send_keys, d, n))
            if n == 0:
                pl.when(dests[d] < me)(functools.partial(send_rows, d, n))

    for s in stages[4:]:
        s.wait()

    at_row = lax.broadcasted_iota(jnp.int32, (COLS, COLS), 0)
    at_col = lax.broadcasted_iota(jnp.int32, (COLS, COLS), 1)
    weave = jnp.where(at_col == 2 * (at_row % 128) + at_row // 128, 1.0, 0.0).astype(BF16)
    sub = lax.broadcasted_iota(jnp.int32, (16, 128), 0)
    for g in range(rows // 256):
        sides = []
        for h in range(2):
            row = lse_in[h:h + 1, g * 128:(g + 1) * 128] * (1.0 / scale)
            hi, md, lo = parts(row)
            sides.append(jnp.where(sub == 0, hi, jnp.where(sub == 1, md, jnp.where(sub == 2, lo, 0.0))))
        woven = dot(beside(*sides).astype(BF16), weave)
        row = woven[0:1] + (woven[1:2] + woven[2:3])
        n, at = g // 2, (g % 2) * 2
        auxr[me, n, at:at + 1] = row[:, 0:128]
        auxr[me, n, at + 1:at + 2] = row[:, 128:256]

    def delta_rows(n, _):
        for g in range(qc // 128):
            part = pl.ds(pl.multiple_of(n * qc + g * 128, 128), 128)
            d = jnp.sum(qbuf[me, 1, part].astype(F32) * obuf[part].astype(F32), axis=1, keepdims=True)
            auxr[me, n, 4 + g:5 + g] = jnp.transpose(jnp.broadcast_to(d, (128, 128)))[0:1]
        return 0

    lax.fori_loop(0, CHUNKS, delta_rows, 0)

    def aux_lines(slot, n):
        hi, md, lo = parts(auxr[slot, n])
        return [stack_lines((hi[g:g + 1], md[g:g + 1], lo[g:g + 1], hi[4 + g:5 + g], md[4 + g:5 + g], lo[4 + g:5 + g]))
                for g in range(qc // 128)]

    def half_lines(slot, half):
        n, at = half // 2, (half % 2) * 2
        return [stack_lines(parts(auxr[slot, n, pl.ds(at + g, 1)]) + parts(auxr[slot, n, pl.ds(4 + at + g, 1)]))
                for g in range(qc // 256)]

    def stack_lines(lines):
        sub = lax.broadcasted_iota(jnp.int32, (8, 128), 0)
        m = jnp.zeros((8, 128), F32)
        for i, line in enumerate(lines):
            m = jnp.where(sub == i, line, m)
        return jnp.concatenate([m, jnp.zeros((120, 128), F32)], axis=0)

    def fill_aux(lines, dst):
        for g, m in enumerate(lines):
            dst[pl.ds(g * 128, 128)] = jnp.transpose(m).astype(BF16)

    lane = lax.broadcasted_iota(jnp.int32, (COLS, head), 1)
    line = lax.broadcasted_iota(jnp.int32, (head, keys), 0)
    k_one[...] = jnp.where(lane < 3, -1.0, 0.0).astype(BF16)
    v_one[...] = jnp.where((lane >= 3) & (lane < 6), -1.0, 0.0).astype(BF16)
    own_kt[head:] = jnp.where(line < 3, -1.0, 0.0).astype(BF16)
    own_vt[head:] = jnp.where((line >= 3) & (line < 6), -1.0, 0.0).astype(BF16)
    dq_t[...] = jnp.zeros_like(dq_t)

    def own_fill(n, _):
        base = pl.multiple_of(n * qc, 128)
        part, kpart = pl.ds(base, qc), pl.ds(pl.multiple_of(n * kc, 128), kc)
        for g, m in enumerate(aux_lines(me, n)):
            at = pl.ds(pl.multiple_of(base + g * 128, 128), 128)
            own_aux[at] = jnp.transpose(m).astype(BF16)
            own_qt[head:, at] = m.astype(BF16)
            own_dot[head:, at] = m.astype(BF16)
        own_qt[:head, part] = jnp.transpose(qbuf[me, 0, part])
        own_dot[:head, part] = jnp.transpose(qbuf[me, 1, part])
        own_kt[:head, kpart] = jnp.transpose(kvbuf[me, 0, kpart])
        own_vt[:head, kpart] = jnp.transpose(kvbuf[me, 1, kpart])
        return 0

    lax.fori_loop(0, CHUNKS, own_fill, 0)

    for peer in range(n_dev):
        @pl.when(peer < me)
        def _():
            aux_copy(me, peer, own_aux_send.at[peer]).start()
    for n in range(1, CHUNKS):
        for d in (1, 2, 0):
            pl.when(dests[d] < me)(functools.partial(send_rows, d, n))

    def own_tiles():
        sums = {}
        for rb in range(CHUNKS):
            rpart = pl.ds(rb * qc, qc)
            aux = own_aux[rpart]
            q, do = beside(qbuf[me, 0, rpart], aux), beside(qbuf[me, 1, rpart], aux)
            for cb in range(rb + 1):
                cpart = pl.ds(cb * kc, kc)

                def first(q=q, do=do, cpart=cpart):
                    return dot(q, own_kt[:, cpart]), dot(do, own_vt[:, cpart])

                def second(s, d, rb=rb, cb=cb, rpart=rpart, cpart=cpart):
                    p = jnp.exp2(s * exp_scale)
                    if cb == rb:
                        row = lax.broadcasted_iota(jnp.int32, (qc, kc), 0)
                        col = lax.broadcasted_iota(jnp.int32, (qc, kc), 1)
                        p = jnp.where(2 * col <= row, p, 0.0)
                    ds = (p * d).astype(BF16)
                    dv, dk = dot(own_dot[:head, rpart], p.astype(BF16)), dot(own_qt[:head, rpart], ds)
                    if cb == rb:
                        dv_t[:, cpart] = dv
                        dk_t[:, cpart] = dk
                    else:
                        dv_t[:, cpart] += dv
                        dk_t[:, cpart] += dk
                    dq = dot(ds, kvbuf[me, 0, cpart])
                    sums[rb] = sums[rb] + dq if rb in sums else dq
                    if cb == rb:
                        dq_acc[rpart] = sums[rb]

                yield first, second

    def run(tiles, lead):
        waiting = []
        for first, second in tiles:
            waiting.append((second, first()))
            if len(waiting) > lead:
                second, values = waiting.pop(0)
                second(*values)
        for second, values in waiting:
            second(*values)

    run(own_tiles(), LEAD_D)

    def plan(t):
        na, ka = (t - 2) // 2, t % 2
        early = t < 2
        hop = jnp.where(ka == 1, other, 0)
        stream_a = jnp.where(early | (ka == 1), 3, 0)
        stream_b = jnp.where(early | (ka == 1), 3, 1)
        src_a = jnp.where(early, pair, nx + hop)
        src_b = jnp.where(early, pair, ny + hop)
        piece_a = jnp.where(early, 2 * t, (na + 2) % CHUNKS)
        piece_b = jnp.where(early, 2 * t + 1, na)
        swap = (src_a > me) & (src_b < me)

        def swapped(a, b):
            return jnp.where(swap, b, a), jnp.where(swap, a, b)

        stream_a, stream_b = swapped(stream_a, stream_b)
        src_a, src_b = swapped(src_a, src_b)
        piece_a, piece_b = swapped(piece_a, piece_b)
        return (stream_a, src_a, piece_a), (stream_b, src_b, piece_b)

    def last_plan(t):
        n = t // 2
        src = diag + jnp.where(t % 2 == 1, other, 0)
        half_a = jnp.where(mid, 2 * n, n)
        half_b = jnp.where(mid, 2 * n + 1, n + CHUNKS)
        return src, (half_a, half_b)

    def arrive(item):
        stream, src, piece = item
        idx = jnp.minimum(stream, 1)
        recv = recv_sem.at[src, piece]
        to_x = (stream == 1) & (jnp.logical_not(mid) | (piece < 2))
        to_y = (stream == 0) & mid & (piece >= 2)
        for make, want in ((q_copy, src > me), (kv_copy, src < me)):
            @pl.when(want)
            def _():
                make(src, piece, me, x_send, recv).wait_recv()

                @pl.when(to_x)
                def _():
                    for h in range(2):
                        half = 2 * piece + h
                        make(src, half, nx, x_send, half_recv.at[src, half], 2).start()

                @pl.when(to_y)
                def _():
                    for h in range(2):
                        half = 2 * piece + h
                        make(src, half, ny, y_send, half_recv.at[src, half], 2).start()

                @pl.when(stream < 3)
                def _():
                    make(src, piece, pair, pair_send.at[idx], recv).start()

    def arrive_half(t, src, half):
        recv = half_recv.at[src, half]
        for make, want in ((q_copy, src > me), (kv_copy, src < me)):
            @pl.when(want)
            def _():
                make(src, half, me, x_send, recv, 2).wait_recv()

                @pl.when(t % 2 == 0)
                def _():
                    make(src, half, pair, pair_send.at[2], recv, 2).start()

    def keys_grads(items, cur, size):
        loaded = []
        for idx, src, piece in items:
            part = pl.ds(pl.multiple_of(piece * size, size), size)
            q, do, aux = qbuf[src, 0, part], qbuf[src, 1, part], chunk_aux[cur, idx, :size]
            q_t[idx, :, :size] = jnp.transpose(q)
            do_t[idx, :, :size] = jnp.transpose(do)
            loaded.append((idx, beside(q, aux), beside(do, aux)))
        sums = {}
        for cb in range(keys // COLS):
            cpart = pl.ds(cb * COLS, COLS)
            for idx, q, do in loaded:
                def first(q=q, do=do, cpart=cpart):
                    return dot(q, own_kt[:, cpart]), dot(do, own_vt[:, cpart])

                def second(s, d, idx=idx, cpart=cpart, cb=cb):
                    p = jnp.exp2(s * exp_scale)
                    ds = (p * d).astype(BF16)
                    dv, dk = dot(do_t[idx, :, :size], p.astype(BF16)), dot(q_t[idx, :, :size], ds)
                    if cb in sums:
                        dv, dk = sums[cb][0] + dv, sums[cb][1] + dk
                    sums[cb] = (dv, dk)
                    if idx == items[-1][0]:
                        dv_t[:, cpart] += dv
                        dk_t[:, cpart] += dk

                yield first, second

    def rows_grad(items, width, size):
        ks, vs = [], []
        for idx, src, piece in items:
            part = pl.ds(pl.multiple_of(piece * size, size), size)
            ks.append(kvbuf[src, 0, part])
            vs.append(kvbuf[src, 1, part])
        k_ts = [jnp.transpose(k) for k in ks]
        k = jnp.concatenate([beside(k, k_one[:size]) for k in ks], axis=0)
        v = jnp.concatenate([beside(v, v_one[:size]) for v in vs], axis=0)
        k_t = k_ts[0] if len(k_ts) == 1 else beside(*k_ts)
        for rb in range(rows // width):
            part = pl.ds(rb * width, width)

            def first(part=part):
                return dot(k, own_qt[:, part]), dot(v, own_dot[:, part])

            def second(s, d, part=part):
                ds = (jnp.exp2(s * exp_scale) * d).astype(BF16)
                dq_t[:, part] += dot(k_t, ds)

            yield first, second

    def mixed(xs, ys):
        xs, ys = list(xs), list(ys)
        for i in range(max(len(xs), len(ys))):
            yield from xs[i:i + 1]
            yield from ys[i:i + 1]

    def present(src):
        return jnp.where(src > me, src, me)

    def ahead(t, slot):
        for idx, (_, src, piece) in enumerate(plan(t)):
            fill_aux(aux_lines(present(src), piece), chunk_aux.at[slot, idx])

    def last_ahead(t, slot):
        src, halves = last_plan(t)
        for idx, half in enumerate(halves):
            fill_aux(half_lines(present(src), half), chunk_aux.at[slot, idx])

    @pl.when(pair > me)
    def _():
        aux_copy(pair, me, own_aux_send.at[0]).wait_recv()
        ahead(0, 0)

    def step(t, _):
        a, b = plan(t)
        cur = t % 2

        @pl.when(t == 1)
        def _():
            for peer in range(n_dev):
                @pl.when((peer > me) & (peer != pair))
                def _():
                    aux_copy(peer, me, own_aux_send.at[0]).wait_recv()

        arrive(a)
        arrive(b)
        a_keys, b_keys = a[1] < me, b[1] < me
        later = jnp.minimum(t + 1, STEPS - 1)
        a, b = (0,) + a[1:], (1,) + b[1:]

        @pl.when(jnp.logical_not(a_keys))
        def _():
            run(keys_grads((a, b), cur, qc), LEAD_Q)
            ahead(later, 1 - cur)

        @pl.when(a_keys & b_keys)
        def _():
            run(rows_grad((a, b), WIDTH_K, kc), LEAD_K)
            ahead(later, 1 - cur)

        @pl.when(a_keys & jnp.logical_not(b_keys))
        def _():
            run(mixed(rows_grad((a,), WIDTH_M, kc), keys_grads((b,), cur, qc)), LEAD_M)
            ahead(later, 1 - cur)

        return 0

    lax.fori_loop(0, STEPS, step, 0)

    def finish_rows():
        dq_ref[...] = ((dq_acc[...] + jnp.transpose(dq_t[...])) * scale).astype(BF16)

    def finish_keys():
        dk_ref[...] = (jnp.transpose(dk_t[...]) * scale).astype(BF16)
        dv_ref[...] = jnp.transpose(dv_t[...]).astype(BF16)

    @pl.when(diag > me)
    def _():
        last_ahead(0, 0)
        finish_rows()

    @pl.when(diag < me)
    def _():
        finish_keys()

    def last_step(t, _):
        src, halves = last_plan(t)
        cur = t % 2
        for half in halves:
            arrive_half(t, src, half)
        items = [(idx, src, half) for idx, half in enumerate(halves)]

        @pl.when(src > me)
        def _():
            run(keys_grads(items, cur, qc // 2), LEAD_Q)
            last_ahead(jnp.minimum(t + 1, LAST_STEPS - 1), 1 - cur)

        @pl.when(src < me)
        def _():
            run(rows_grad(items, WIDTH_K, kc // 2), LEAD_K)

        return 0

    lax.fori_loop(0, LAST_STEPS, last_step, 0)

    @pl.when(diag > me)
    def _():
        finish_keys()

    @pl.when(diag < me)
    def _():
        finish_rows()

    for peer in range(n_dev):
        @pl.when(peer < me)
        def _():
            aux_copy(me, peer, own_aux_send.at[peer]).wait_send()

    def left(buf, slot, length, send, want):
        @pl.when(want)
        def _():
            block = buf.at[slot, :, pl.ds(0, length)]
            pltpu.make_async_remote_copy(block, block, send, recv_sem.at[slot, 0],
                                         device_id={'cp': pair}, device_id_type=MESH).wait_send()

    for buf, size, sign in ((qbuf, rows, 1), (kvbuf, keys, -1)):
        for d, dest in enumerate(dests):
            left(buf, me, size, own_send.at[d], sign * dest < sign * me)
        for d, src in enumerate((nx, ny, diag)):
            left(buf, src, size, pair_send.at[d], sign * src > sign * me)
        left(buf, ny, size, x_send, (sign * ny > sign * me) & jnp.logical_not(mid))
        left(buf, ny, size // 2, x_send, (sign * ny > sign * me) & mid)
        left(buf, nx, size // 2, y_send, (sign * nx > sign * me) & mid)


def store(*refs):
    n = len(refs) // 2
    copies = [pltpu.make_async_copy(refs[i], refs[n + i], refs[-1].at[i]) for i in range(n)]
    for c in copies:
        c.start()
    for c in copies:
        c.wait()


def solution(mesh):
    n_dev = mesh.shape['cp']
    row_spec = P(('dp', 'cp'))

    def local_fn(q_tok, k_tok, v_tok, fwd_out, d_out, lse_row):
        tokens, groups, head = q_tok.shape
        rows = tokens * groups
        piece = rows // CHUNKS
        flat = lambda x: x.reshape(rows, head)
        dma = pltpu.SemaphoreType.DMA
        vmem = pltpu.VMEM
        grad_q, grad_k, grad_v = pl.pallas_call(
            functools.partial(kernel, rows, tokens, head, n_dev),
            out_shape=(jax.ShapeDtypeStruct((rows, head), BF16),
                       jax.ShapeDtypeStruct((tokens, head), BF16),
                       jax.ShapeDtypeStruct((tokens, head), BF16)),
            in_specs=[pl.BlockSpec(memory_space=pltpu.HBM)] * 6,
            out_specs=(pl.BlockSpec(memory_space=vmem),) * 3,
            scratch_shapes=[
                vmem((n_dev, 2, rows, head), BF16),
                vmem((n_dev, 2, tokens, head), BF16),
                vmem((rows, head), BF16),
                vmem((groups, tokens), F32),
                vmem((n_dev, CHUNKS, 8, 128), F32),
                vmem((rows, head), BF16),
                vmem((2, 2, piece, head), BF16),
                vmem((COLS, head), BF16),
                vmem((COLS, head), BF16),
                vmem((2 * head, rows), BF16),
                vmem((2 * head, rows), BF16),
                vmem((2 * head, tokens), BF16),
                vmem((2 * head, tokens), BF16),
                vmem((2, head, piece), BF16),
                vmem((2, head, piece), BF16),
                vmem((rows, head), F32),
                vmem((head, rows), F32),
                vmem((head, tokens), F32),
                vmem((head, tokens), F32),
                dma((6,)),
                dma((n_dev, CHUNKS)),
                dma((n_dev, 2 * CHUNKS)),
                dma((n_dev,)),
                dma((3,)),
                dma((n_dev,)),
                dma((3,)),
                dma,
                dma,
            ],
            compiler_params=pltpu.CompilerParams(
                collective_id=0, has_side_effects=True, vmem_limit_bytes=48 * 1024 * 1024),
            name='attention_backward',
        )(*[pltpu.with_memory_space_constraint(x, pltpu.HBM) for x in (flat(q_tok), k_tok, v_tok, flat(fwd_out), flat(d_out), lse_row.T)])
        grads = (grad_q, grad_k, grad_v)
        any_space = pl.BlockSpec(memory_space=pl.ANY)
        grad_q, grad_k, grad_v = pl.pallas_call(
            store,
            out_shape=tuple(jax.ShapeDtypeStruct(g.shape, g.dtype) for g in grads),
            in_specs=[any_space] * 3,
            out_specs=(any_space,) * 3,
            scratch_shapes=[dma((3,))],
            compiler_params=pltpu.CompilerParams(vmem_limit_bytes=1024 * 1024),
            name='store_grads',
        )(*[pltpu.with_memory_space_constraint(g, vmem) for g in grads])
        return grad_q.reshape(tokens, groups, head), grad_k, grad_v

    return jax.shard_map(local_fn, mesh=mesh, in_specs=(row_spec,) * 6, out_specs=(row_spec,) * 3, check_vma=False)
```

```python
import functools
import math

import jax
import jax.numpy as jnp
from jax import lax
from jax.experimental import pallas as pl
from jax.experimental.pallas import tpu as pltpu
from jax.sharding import PartitionSpec as P

BF16, F32 = jnp.bfloat16, jnp.float32
CHUNKS = 4
COLS = 256
STEPS, LAST_STEPS = 10, 8
LEAD_Q, LEAD_K, LEAD_M = 4, 4, 2
LEAD_D = 2
WIDTH_K, WIDTH_M = 256, 512
MESH = pl.DeviceIdType.MESH


def dot(a, b):
    return jnp.dot(a, b, preferred_element_type=F32)


def beside(a, b):
    return jnp.concatenate([a, b], axis=1)


def parts(x):
    hi = x.astype(BF16).astype(F32)
    rest = x - hi
    md = rest.astype(BF16).astype(F32)
    return hi, md, rest - md


def kernel(rows, keys, head, n_dev, q_hbm, k_hbm, v_hbm, o_hbm, do_hbm, lse_hbm, dq_ref, dk_ref, dv_ref,
           qbuf, kvbuf, obuf, lse_in, auxr, own_aux, chunk_aux, k_one, v_one, own_qt, own_dot, own_kt, own_vt,
           q_t, do_t, dq_acc, dq_t, dk_t, dv_t,
           stage_sem, recv_sem, half_recv, aux_recv, own_send, own_aux_send, pair_send, pair_aux_send, x_send, y_send, x_aux_send):
    me = lax.axis_index('cp')
    core, px, py = me % 2, (me // 2) % 2, me // 4
    pair = me + 1 - 2 * core
    nx = me + 2 - 4 * px
    ny = me + 4 - 8 * py
    diag = nx + 4 - 8 * py
    other = pair - me
    mid = (px + py) == 1
    qc, kc = rows // CHUNKS, keys // CHUNKS
    scale = head ** -0.5
    exp_scale = scale * math.log2(math.e)

    def q_copy(slot, n, dest, send, recv, halves=1):
        part = pl.ds(n * (qc // halves), qc // halves)
        return pltpu.make_async_remote_copy(
            qbuf.at[slot, :, part], qbuf.at[slot, :, part], send, recv,
            device_id={'cp': dest}, device_id_type=MESH)

    def kv_copy(slot, n, dest, send, recv, halves=1):
        part = pl.ds(n * (kc // halves), kc // halves)
        return pltpu.make_async_remote_copy(
            kvbuf.at[slot, :, part], kvbuf.at[slot, :, part], send, recv,
            device_id={'cp': dest}, device_id_type=MESH)

    def aux_copy(slot, dest, send):
        return pltpu.make_async_remote_copy(
            auxr.at[slot], auxr.at[slot], send, aux_recv.at[slot],
            device_id={'cp': dest}, device_id_type=MESH)

    stages = [
        pltpu.make_async_copy(q_hbm, qbuf.at[me, 0], stage_sem.at[0]),
        pltpu.make_async_copy(do_hbm, qbuf.at[me, 1], stage_sem.at[1]),
        pltpu.make_async_copy(k_hbm, kvbuf.at[me, 0], stage_sem.at[2]),
        pltpu.make_async_copy(v_hbm, kvbuf.at[me, 1], stage_sem.at[3]),
        pltpu.make_async_copy(o_hbm, obuf, stage_sem.at[4]),
        pltpu.make_async_copy(lse_hbm, lse_in, stage_sem.at[5]),
    ]
    for s in stages:
        s.start()

    barrier = pltpu.get_barrier_semaphore()
    for peer in (nx, ny, pair):
        pl.semaphore_signal(barrier, inc=1, device_id={'cp': peer}, device_id_type=MESH)
    pl.semaphore_wait(barrier, 3)

    def order(d, n):
        return (n + 2) % CHUNKS if d == 1 else n

    dests = (pair, nx, ny)
    for s in stages[:2]:
        s.wait()
    def send_keys(d, n):
        c = order(d, n)
        kv_copy(me, c, dests[d], own_send.at[d], recv_sem.at[me, c]).start()

    def send_rows(d, n):
        c = order(d, n)
        q_copy(me, c, dests[d], own_send.at[d], recv_sem.at[me, c]).start()

    for d in (1, 2):
        pl.when(dests[d] < me)(functools.partial(send_rows, d, 0))
    for s in stages[2:4]:
        s.wait()
    for n in range(CHUNKS):
        for d in (1, 2, 0):
            pl.when(dests[d] > me)(functools.partial(send_keys, d, n))
    pl.when(pair < me)(functools.partial(send_rows, 0, 0))

    for s in stages[4:]:
        s.wait()

    at_row = lax.broadcasted_iota(jnp.int32, (COLS, COLS), 0)
    at_col = lax.broadcasted_iota(jnp.int32, (COLS, COLS), 1)
    weave = jnp.where(at_col == 2 * (at_row % 128) + at_row // 128, 1.0, 0.0).astype(BF16)
    sub = lax.broadcasted_iota(jnp.int32, (16, 128), 0)
    for g in range(rows // 256):
        sides = []
        for h in range(2):
            row = lse_in[h:h + 1, g * 128:(g + 1) * 128] * (1.0 / scale)
            hi, md, lo = parts(row)
            sides.append(jnp.where(sub == 0, hi, jnp.where(sub == 1, md, jnp.where(sub == 2, lo, 0.0))))
        woven = dot(beside(*sides).astype(BF16), weave)
        row = woven[0:1] + (woven[1:2] + woven[2:3])
        n, at = g // 2, (g % 2) * 2
        auxr[me, n, at:at + 1] = row[:, 0:128]
        auxr[me, n, at + 1:at + 2] = row[:, 128:256]

    def delta_rows(n, _):
        for g in range(qc // 128):
            part = pl.ds(pl.multiple_of(n * qc + g * 128, 128), 128)
            d = jnp.sum(qbuf[me, 1, part].astype(F32) * obuf[part].astype(F32), axis=1, keepdims=True)
            auxr[me, n, 4 + g:5 + g] = jnp.transpose(jnp.broadcast_to(d, (128, 128)))[0:1]
        return 0

    lax.fori_loop(0, CHUNKS, delta_rows, 0)

    def aux_lines(slot, n):
        hi, md, lo = parts(auxr[slot, n])
        return [stack_lines((hi[g:g + 1], md[g:g + 1], lo[g:g + 1], hi[4 + g:5 + g], md[4 + g:5 + g], lo[4 + g:5 + g]))
                for g in range(qc // 128)]

    def half_lines(slot, half):
        n, at = half // 2, (half % 2) * 2
        return [stack_lines(parts(auxr[slot, n, pl.ds(at + g, 1)]) + parts(auxr[slot, n, pl.ds(4 + at + g, 1)]))
                for g in range(qc // 256)]

    def stack_lines(lines):
        sub = lax.broadcasted_iota(jnp.int32, (8, 128), 0)
        m = jnp.zeros((8, 128), F32)
        for i, line in enumerate(lines):
            m = jnp.where(sub == i, line, m)
        return jnp.concatenate([m, jnp.zeros((120, 128), F32)], axis=0)

    def fill_aux(lines, dst):
        for g, m in enumerate(lines):
            dst[pl.ds(g * 128, 128)] = jnp.transpose(m).astype(BF16)

    lane = lax.broadcasted_iota(jnp.int32, (COLS, head), 1)
    line = lax.broadcasted_iota(jnp.int32, (head, keys), 0)
    k_one[...] = jnp.where(lane < 3, -1.0, 0.0).astype(BF16)
    v_one[...] = jnp.where((lane >= 3) & (lane < 6), -1.0, 0.0).astype(BF16)
    own_kt[head:] = jnp.where(line < 3, -1.0, 0.0).astype(BF16)
    own_vt[head:] = jnp.where((line >= 3) & (line < 6), -1.0, 0.0).astype(BF16)
    dq_t[...] = jnp.zeros_like(dq_t)

    def own_fill(n, _):
        base = pl.multiple_of(n * qc, 128)
        part, kpart = pl.ds(base, qc), pl.ds(pl.multiple_of(n * kc, 128), kc)
        for g, m in enumerate(aux_lines(me, n)):
            at = pl.ds(pl.multiple_of(base + g * 128, 128), 128)
            own_aux[at] = jnp.transpose(m).astype(BF16)
            own_qt[head:, at] = m.astype(BF16)
            own_dot[head:, at] = m.astype(BF16)
        own_qt[:head, part] = jnp.transpose(qbuf[me, 0, part])
        own_dot[:head, part] = jnp.transpose(qbuf[me, 1, part])
        own_kt[:head, kpart] = jnp.transpose(kvbuf[me, 0, kpart])
        own_vt[:head, kpart] = jnp.transpose(kvbuf[me, 1, kpart])
        return 0

    lax.fori_loop(0, CHUNKS, own_fill, 0)

    for d, dest in enumerate(dests):
        @pl.when(dest < me)
        def _():
            aux_copy(me, dest, own_aux_send.at[d]).start()
    for n in range(1, CHUNKS):
        for d in (1, 2, 0):
            pl.when(dests[d] < me)(functools.partial(send_rows, d, n))

    def own_tiles():
        sums = {}
        for rb in range(CHUNKS):
            rpart = pl.ds(rb * qc, qc)
            aux = own_aux[rpart]
            q, do = beside(qbuf[me, 0, rpart], aux), beside(qbuf[me, 1, rpart], aux)
            for cb in range(rb + 1):
                cpart = pl.ds(cb * kc, kc)

                def first(q=q, do=do, cpart=cpart):
                    return dot(q, own_kt[:, cpart]), dot(do, own_vt[:, cpart])

                def second(s, d, rb=rb, cb=cb, rpart=rpart, cpart=cpart):
                    p = jnp.exp2(s * exp_scale)
                    if cb == rb:
                        row = lax.broadcasted_iota(jnp.int32, (qc, kc), 0)
                        col = lax.broadcasted_iota(jnp.int32, (qc, kc), 1)
                        p = jnp.where(2 * col <= row, p, 0.0)
                    ds = (p * d).astype(BF16)
                    dv, dk = dot(own_dot[:head, rpart], p.astype(BF16)), dot(own_qt[:head, rpart], ds)
                    if cb == rb:
                        dv_t[:, cpart] = dv
                        dk_t[:, cpart] = dk
                    else:
                        dv_t[:, cpart] += dv
                        dk_t[:, cpart] += dk
                    dq = dot(ds, kvbuf[me, 0, cpart])
                    sums[rb] = sums[rb] + dq if rb in sums else dq
                    if cb == rb:
                        dq_acc[rpart] = sums[rb]

                yield first, second

    def run(tiles, lead):
        waiting = []
        for first, second in tiles:
            waiting.append((second, first()))
            if len(waiting) > lead:
                second, values = waiting.pop(0)
                second(*values)
        for second, values in waiting:
            second(*values)

    run(own_tiles(), LEAD_D)

    def plan(t):
        na, ka = (t - 2) // 2, t % 2
        early = t < 2
        hop = jnp.where(ka == 1, other, 0)
        stream_a = jnp.where(early | (ka == 1), 3, 0)
        stream_b = jnp.where(early | (ka == 1), 3, 1)
        src_a = jnp.where(early, pair, nx + hop)
        src_b = jnp.where(early, pair, ny + hop)
        piece_a = jnp.where(early, 2 * t, (na + 2) % CHUNKS)
        piece_b = jnp.where(early, 2 * t + 1, na)
        swap = (src_a > me) & (src_b < me)

        def swapped(a, b):
            return jnp.where(swap, b, a), jnp.where(swap, a, b)

        stream_a, stream_b = swapped(stream_a, stream_b)
        src_a, src_b = swapped(src_a, src_b)
        piece_a, piece_b = swapped(piece_a, piece_b)
        return (stream_a, src_a, piece_a), (stream_b, src_b, piece_b)

    def last_plan(t):
        n = t // 2
        src = diag + jnp.where(t % 2 == 1, other, 0)
        half_a = jnp.where(mid, 2 * n, n)
        half_b = jnp.where(mid, 2 * n + 1, n + CHUNKS)
        return src, (half_a, half_b)

    def arrive(item):
        stream, src, piece = item
        idx = jnp.minimum(stream, 1)
        recv = recv_sem.at[src, piece]
        to_x = (stream == 1) & (jnp.logical_not(mid) | (piece < 2))
        to_y = (stream == 0) & mid & (piece >= 2)
        for make, want in ((q_copy, src > me), (kv_copy, src < me)):
            @pl.when(want)
            def _():
                make(src, piece, me, x_send, recv).wait_recv()

                @pl.when(to_x)
                def _():
                    for h in range(2):
                        half = 2 * piece + h
                        make(src, half, nx, x_send, half_recv.at[src, half], 2).start()

                @pl.when(to_y)
                def _():
                    for h in range(2):
                        half = 2 * piece + h
                        make(src, half, ny, y_send, half_recv.at[src, half], 2).start()

                @pl.when(stream < 3)
                def _():
                    make(src, piece, pair, pair_send.at[idx], recv).start()

    def arrive_half(t, src, half):
        recv = half_recv.at[src, half]
        for make, want in ((q_copy, src > me), (kv_copy, src < me)):
            @pl.when(want)
            def _():
                make(src, half, me, x_send, recv, 2).wait_recv()

                @pl.when(t % 2 == 0)
                def _():
                    make(src, half, pair, pair_send.at[2], recv, 2).start()

    def keys_grads(items, cur, size):
        loaded = []
        for idx, src, piece in items:
            part = pl.ds(pl.multiple_of(piece * size, size), size)
            q, do, aux = qbuf[src, 0, part], qbuf[src, 1, part], chunk_aux[cur, idx, :size]
            q_t[idx, :, :size] = jnp.transpose(q)
            do_t[idx, :, :size] = jnp.transpose(do)
            loaded.append((idx, beside(q, aux), beside(do, aux)))
        sums = {}
        for cb in range(keys // COLS):
            cpart = pl.ds(cb * COLS, COLS)
            for idx, q, do in loaded:
                def first(q=q, do=do, cpart=cpart):
                    return dot(q, own_kt[:, cpart]), dot(do, own_vt[:, cpart])

                def second(s, d, idx=idx, cpart=cpart, cb=cb):
                    p = jnp.exp2(s * exp_scale)
                    ds = (p * d).astype(BF16)
                    dv, dk = dot(do_t[idx, :, :size], p.astype(BF16)), dot(q_t[idx, :, :size], ds)
                    if cb in sums:
                        dv, dk = sums[cb][0] + dv, sums[cb][1] + dk
                    sums[cb] = (dv, dk)
                    if idx == items[-1][0]:
                        dv_t[:, cpart] += dv
                        dk_t[:, cpart] += dk

                yield first, second

    def rows_grad(items, width, size):
        ks, vs = [], []
        for idx, src, piece in items:
            part = pl.ds(pl.multiple_of(piece * size, size), size)
            ks.append(kvbuf[src, 0, part])
            vs.append(kvbuf[src, 1, part])
        k_ts = [jnp.transpose(k) for k in ks]
        k = jnp.concatenate([beside(k, k_one[:size]) for k in ks], axis=0)
        v = jnp.concatenate([beside(v, v_one[:size]) for v in vs], axis=0)
        k_t = k_ts[0] if len(k_ts) == 1 else beside(*k_ts)
        for rb in range(rows // width):
            part = pl.ds(rb * width, width)

            def first(part=part):
                return dot(k, own_qt[:, part]), dot(v, own_dot[:, part])

            def second(s, d, part=part):
                ds = (jnp.exp2(s * exp_scale) * d).astype(BF16)
                dq_t[:, part] += dot(k_t, ds)

            yield first, second

    def mixed(xs, ys):
        xs, ys = list(xs), list(ys)
        for i in range(max(len(xs), len(ys))):
            yield from xs[i:i + 1]
            yield from ys[i:i + 1]

    def present(src):
        return jnp.where(src > me, src, me)

    def ahead(t, slot):
        for idx, (_, src, piece) in enumerate(plan(t)):
            fill_aux(aux_lines(present(src), piece), chunk_aux.at[slot, idx])

    def last_ahead(t, slot):
        src, halves = last_plan(t)
        for idx, half in enumerate(halves):
            fill_aux(half_lines(present(src), half), chunk_aux.at[slot, idx])

    def take_lines(src, to_pair=None):
        @pl.when(src > me)
        def _():
            aux_copy(src, me, x_aux_send).wait_recv()
            if to_pair is not None:
                aux_copy(src, pair, pair_aux_send.at[to_pair]).start()

    take_lines(pair)

    @pl.when(pair > me)
    def _():
        ahead(0, 0)

    def step(t, _):
        a, b = plan(t)
        cur = t % 2

        @pl.when(t == 1)
        def _():
            take_lines(nx, 0)
            take_lines(ny, 1)

            @pl.when(ny > me)
            def _():
                aux_copy(ny, nx, x_aux_send).start()

        @pl.when(t == 2)
        def _():
            take_lines(nx + other)
            take_lines(ny + other)

        arrive(a)
        arrive(b)
        a_keys, b_keys = a[1] < me, b[1] < me
        later = jnp.minimum(t + 1, STEPS - 1)
        a, b = (0,) + a[1:], (1,) + b[1:]

        @pl.when(jnp.logical_not(a_keys))
        def _():
            run(keys_grads((a, b), cur, qc), LEAD_Q)
            ahead(later, 1 - cur)

        @pl.when(a_keys & b_keys)
        def _():
            run(rows_grad((a, b), WIDTH_K, kc), LEAD_K)
            ahead(later, 1 - cur)

        @pl.when(a_keys & jnp.logical_not(b_keys))
        def _():
            run(mixed(rows_grad((a,), WIDTH_M, kc), keys_grads((b,), cur, qc)), LEAD_M)
            ahead(later, 1 - cur)

        return 0

    lax.fori_loop(0, STEPS, step, 0)

    def finish_rows():
        dq_ref[...] = ((dq_acc[...] + jnp.transpose(dq_t[...])) * scale).astype(BF16)

    def finish_keys():
        dk_ref[...] = (jnp.transpose(dk_t[...]) * scale).astype(BF16)
        dv_ref[...] = jnp.transpose(dv_t[...]).astype(BF16)

    take_lines(diag, 2)
    def left(buf, slot, length, send, want):
        @pl.when(want)
        def _():
            block = buf.at[slot, :, pl.ds(0, length)]
            pltpu.make_async_remote_copy(block, block, send, recv_sem.at[slot, 0],
                                         device_id={'cp': pair}, device_id_type=MESH).wait_send()

    sides = ((qbuf, rows, 1), (kvbuf, keys, -1))
    for buf, size, sign in sides:
        for d, dest in enumerate(dests):
            left(buf, me, size, own_send.at[d], sign * dest < sign * me)
        for d, src in enumerate((nx, ny)):
            left(buf, src, size, pair_send.at[d], sign * src > sign * me)
    for d, dest in enumerate(dests):
        @pl.when(dest < me)
        def _():
            aux_copy(me, dest, own_aux_send.at[d]).wait_send()
    for d, src in enumerate((nx, ny)):
        @pl.when(src > me)
        def _():
            aux_copy(src, pair, pair_aux_send.at[d]).wait_send()

            if d == 1:
                aux_copy(src, nx, x_aux_send).wait_send()

    @pl.when(diag > me)
    def _():
        last_ahead(0, 0)
        finish_rows()

    @pl.when(diag < me)
    def _():
        finish_keys()

    take_lines(diag + other)

    def last_step(t, _):
        src, halves = last_plan(t)
        cur = t % 2
        for half in halves:
            arrive_half(t, src, half)
        items = [(idx, src, half) for idx, half in enumerate(halves)]

        @pl.when(src > me)
        def _():
            run(keys_grads(items, cur, qc // 2), LEAD_Q)
            last_ahead(jnp.minimum(t + 1, LAST_STEPS - 1), 1 - cur)

        @pl.when(src < me)
        def _():
            run(rows_grad(items, WIDTH_K, kc // 2), LEAD_K)

        return 0

    lax.fori_loop(0, LAST_STEPS, last_step, 0)

    @pl.when(diag > me)
    def _():
        finish_keys()

    @pl.when(diag < me)
    def _():
        finish_rows()

    for buf, size, sign in sides:
        left(buf, diag, size, pair_send.at[2], sign * diag > sign * me)
        left(buf, ny, size, x_send, (sign * ny > sign * me) & jnp.logical_not(mid))
        left(buf, ny, size // 2, x_send, (sign * ny > sign * me) & mid)
        left(buf, nx, size // 2, y_send, (sign * nx > sign * me) & mid)

    @pl.when(diag > me)
    def _():
        aux_copy(diag, pair, pair_aux_send.at[2]).wait_send()


def store(*refs):
    n = len(refs) // 2
    copies = [pltpu.make_async_copy(refs[i], refs[n + i], refs[-1].at[i]) for i in range(n)]
    for c in copies:
        c.start()
    for c in copies:
        c.wait()


def solution(mesh):
    n_dev = mesh.shape['cp']
    row_spec = P(('dp', 'cp'))

    def local_fn(q_tok, k_tok, v_tok, fwd_out, d_out, lse_row):
        tokens, groups, head = q_tok.shape
        rows = tokens * groups
        piece = rows // CHUNKS
        flat = lambda x: x.reshape(rows, head)
        dma = pltpu.SemaphoreType.DMA
        vmem = pltpu.VMEM
        grad_q, grad_k, grad_v = pl.pallas_call(
            functools.partial(kernel, rows, tokens, head, n_dev),
            out_shape=(jax.ShapeDtypeStruct((rows, head), BF16),
                       jax.ShapeDtypeStruct((tokens, head), BF16),
                       jax.ShapeDtypeStruct((tokens, head), BF16)),
            in_specs=[pl.BlockSpec(memory_space=pltpu.HBM)] * 6,
            out_specs=(pl.BlockSpec(memory_space=vmem),) * 3,
            scratch_shapes=[
                vmem((n_dev, 2, rows, head), BF16),
                vmem((n_dev, 2, tokens, head), BF16),
                vmem((rows, head), BF16),
                vmem((groups, tokens), F32),
                vmem((n_dev, CHUNKS, 8, 128), F32),
                vmem((rows, head), BF16),
                vmem((2, 2, piece, head), BF16),
                vmem((COLS, head), BF16),
                vmem((COLS, head), BF16),
                vmem((2 * head, rows), BF16),
                vmem((2 * head, rows), BF16),
                vmem((2 * head, tokens), BF16),
                vmem((2 * head, tokens), BF16),
                vmem((2, head, piece), BF16),
                vmem((2, head, piece), BF16),
                vmem((rows, head), F32),
                vmem((head, rows), F32),
                vmem((head, tokens), F32),
                vmem((head, tokens), F32),
                dma((6,)),
                dma((n_dev, CHUNKS)),
                dma((n_dev, 2 * CHUNKS)),
                dma((n_dev,)),
                dma((3,)),
                dma((3,)),
                dma((3,)),
                dma((3,)),
                dma,
                dma,
                dma,
            ],
            compiler_params=pltpu.CompilerParams(
                collective_id=0, has_side_effects=True, vmem_limit_bytes=48 * 1024 * 1024),
            name='attention_backward',
        )(*[pltpu.with_memory_space_constraint(x, pltpu.HBM) for x in (flat(q_tok), k_tok, v_tok, flat(fwd_out), flat(d_out), lse_row.T)])
        grads = (grad_q, grad_k, grad_v)
        any_space = pl.BlockSpec(memory_space=pl.ANY)
        grad_q, grad_k, grad_v = pl.pallas_call(
            store,
            out_shape=tuple(jax.ShapeDtypeStruct(g.shape, g.dtype) for g in grads),
            in_specs=[any_space] * 3,
            out_specs=(any_space,) * 3,
            scratch_shapes=[dma((3,))],
            compiler_params=pltpu.CompilerParams(vmem_limit_bytes=1024 * 1024),
            name='store_grads',
        )(*[pltpu.with_memory_space_constraint(g, vmem) for g in grads])
        return grad_q.reshape(tokens, groups, head), grad_k, grad_v

    return jax.shard_map(local_fn, mesh=mesh, in_specs=(row_spec,) * 6, out_specs=(row_spec,) * 3, check_vma=False)
```

```python
import functools
import math

import jax
import jax.numpy as jnp
from jax import lax
from jax.experimental import pallas as pl
from jax.experimental.pallas import tpu as pltpu
from jax.sharding import PartitionSpec as P

BF16, F32 = jnp.bfloat16, jnp.float32
CHUNKS = 4
COLS = 256
STEPS, LAST_STEPS = 10, 8
LEAD_Q, LEAD_K, LEAD_M = 2, 4, 2
LEAD_D = 2
ROWS_Q = 256
WIDTH_K, WIDTH_M = 256, 512
MESH = pl.DeviceIdType.MESH


def dot(a, b):
    return jnp.dot(a, b, preferred_element_type=F32)


def beside(a, b):
    return jnp.concatenate([a, b], axis=1)


def parts(x):
    hi = x.astype(BF16).astype(F32)
    rest = x - hi
    md = rest.astype(BF16).astype(F32)
    return hi, md, rest - md


def kernel(rows, keys, head, n_dev, q_hbm, k_hbm, v_hbm, o_hbm, do_hbm, lse_hbm, dq_ref, dk_ref, dv_ref,
           qbuf, kvbuf, obuf, lse_in, auxr, own_aux, chunk_aux, k_one, v_one, own_qt, own_dot, own_kt, own_vt,
           q_t, do_t, dq_acc, dq_t, dk_t, dv_t,
           stage_sem, recv_sem, half_recv, aux_recv, own_send, own_aux_send, pair_send, pair_aux_send, x_send, y_send, x_aux_send):
    me = lax.axis_index('cp')
    core, px, py = me % 2, (me // 2) % 2, me // 4
    pair = me + 1 - 2 * core
    nx = me + 2 - 4 * px
    ny = me + 4 - 8 * py
    diag = nx + 4 - 8 * py
    other = pair - me
    mid = (px + py) == 1
    qc, kc = rows // CHUNKS, keys // CHUNKS
    scale = head ** -0.5
    exp_scale = scale * math.log2(math.e)

    def q_copy(slot, n, dest, send, recv, halves=1):
        part = pl.ds(n * (qc // halves), qc // halves)
        return pltpu.make_async_remote_copy(
            qbuf.at[slot, :, part], qbuf.at[slot, :, part], send, recv,
            device_id={'cp': dest}, device_id_type=MESH)

    def kv_copy(slot, n, dest, send, recv, halves=1):
        part = pl.ds(n * (kc // halves), kc // halves)
        return pltpu.make_async_remote_copy(
            kvbuf.at[slot, :, part], kvbuf.at[slot, :, part], send, recv,
            device_id={'cp': dest}, device_id_type=MESH)

    def aux_copy(slot, dest, send):
        return pltpu.make_async_remote_copy(
            auxr.at[slot], auxr.at[slot], send, aux_recv.at[slot],
            device_id={'cp': dest}, device_id_type=MESH)

    stages = [
        pltpu.make_async_copy(q_hbm, qbuf.at[me, 0], stage_sem.at[0]),
        pltpu.make_async_copy(do_hbm, qbuf.at[me, 1], stage_sem.at[1]),
        pltpu.make_async_copy(k_hbm, kvbuf.at[me, 0], stage_sem.at[2]),
        pltpu.make_async_copy(v_hbm, kvbuf.at[me, 1], stage_sem.at[3]),
        pltpu.make_async_copy(o_hbm, obuf, stage_sem.at[4]),
        pltpu.make_async_copy(lse_hbm, lse_in, stage_sem.at[5]),
    ]
    for s in stages:
        s.start()

    barrier = pltpu.get_barrier_semaphore()
    for peer in (nx, ny, pair):
        pl.semaphore_signal(barrier, inc=1, device_id={'cp': peer}, device_id_type=MESH)
    pl.semaphore_wait(barrier, 3)

    def order(d, n):
        return (n + 2) % CHUNKS if d == 1 else n

    dests = (pair, nx, ny)
    for s in stages[:2]:
        s.wait()
    def send_keys(d, n):
        c = order(d, n)
        kv_copy(me, c, dests[d], own_send.at[d], recv_sem.at[me, c]).start()

    def send_rows(d, n):
        c = order(d, n)
        q_copy(me, c, dests[d], own_send.at[d], recv_sem.at[me, c]).start()

    for d in (1, 2):
        pl.when(dests[d] < me)(functools.partial(send_rows, d, 0))
    for s in stages[2:4]:
        s.wait()
    for n in range(CHUNKS):
        for d in (1, 2, 0):
            pl.when(dests[d] > me)(functools.partial(send_keys, d, n))
    pl.when(pair < me)(functools.partial(send_rows, 0, 0))

    for s in stages[4:]:
        s.wait()

    def aux_lines(slot, n):
        hi, md, lo = parts(auxr[slot, n])
        return [stack_lines((hi[g:g + 1], md[g:g + 1], lo[g:g + 1], hi[4 + g:5 + g], md[4 + g:5 + g], lo[4 + g:5 + g]))
                for g in range(qc // 128)]

    def half_lines(slot, half):
        n, at = half // 2, (half % 2) * 2
        return [stack_lines(parts(auxr[slot, n, pl.ds(at + g, 1)]) + parts(auxr[slot, n, pl.ds(4 + at + g, 1)]))
                for g in range(qc // 256)]

    def stack_lines(lines):
        sub = lax.broadcasted_iota(jnp.int32, (8, 128), 0)
        m = jnp.zeros((8, 128), F32)
        for i, line in enumerate(lines):
            m = jnp.where(sub == i, line, m)
        return m

    def fill_aux(lines, dst):
        for g, m in enumerate(lines):
            m = jnp.concatenate([m, jnp.zeros((120, 128), F32)], axis=0)
            dst[pl.ds(g * 128, 128)] = jnp.transpose(m).astype(BF16)

    at_row = lax.broadcasted_iota(jnp.int32, (COLS, COLS), 0)
    at_col = lax.broadcasted_iota(jnp.int32, (COLS, COLS), 1)
    weave = jnp.where(at_col == 2 * (at_row % 128) + at_row // 128, 1.0, 0.0).astype(BF16)
    sub = lax.broadcasted_iota(jnp.int32, (16, 128), 0)
    for n in range(CHUNKS):
        part = pl.ds(n * qc, qc)
        do_turned = jnp.transpose(qbuf[me, 1, part])
        own_dot[:head, part] = do_turned
        sums = jnp.sum(do_turned.astype(F32) * jnp.transpose(obuf[part]).astype(F32), axis=0, keepdims=True)
        for g in range(qc // 128):
            auxr[me, n, 4 + g:5 + g] = sums[:, g * 128:(g + 1) * 128]
        for g in range(qc // 256):
            sides = []
            for h in range(2):
                at = n * (qc // 2) + g * 128
                hi, md, lo = parts(lse_in[h:h + 1, at:at + 128] * (1.0 / scale))
                sides.append(jnp.where(sub == 0, hi, jnp.where(sub == 1, md, jnp.where(sub == 2, lo, 0.0))))
            woven = dot(beside(*sides).astype(BF16), weave)
            row = woven[0:1] + (woven[1:2] + woven[2:3])
            auxr[me, n, 2 * g:2 * g + 1] = row[:, 0:128]
            auxr[me, n, 2 * g + 1:2 * g + 2] = row[:, 128:256]

    for n in range(1, CHUNKS):
        pl.when(pair < me)(functools.partial(send_rows, 0, n))

    lane = lax.broadcasted_iota(jnp.int32, (COLS, head), 1)
    line = lax.broadcasted_iota(jnp.int32, (head, keys), 0)
    k_one[...] = jnp.where(lane < 3, -1.0, 0.0).astype(BF16)
    v_one[...] = jnp.where((lane >= 3) & (lane < 6), -1.0, 0.0).astype(BF16)
    own_kt[head:] = jnp.where(line < 3, -1.0, 0.0).astype(BF16)
    own_vt[head:] = jnp.where((line >= 3) & (line < 6), -1.0, 0.0).astype(BF16)
    dq_t[...] = jnp.zeros_like(dq_t)
    for n in range(CHUNKS):
        part, kpart = pl.ds(n * qc, qc), pl.ds(n * kc, kc)
        lines = aux_lines(me, n)
        fill_aux(lines, own_aux.at[part])
        for g, m in enumerate(lines):
            m = jnp.concatenate([m, jnp.zeros((120, 128), F32)], axis=0).astype(BF16)
            own_qt[head:, pl.ds(n * qc + g * 128, 128)] = m
            own_dot[head:, pl.ds(n * qc + g * 128, 128)] = m
        own_qt[:head, part] = jnp.transpose(qbuf[me, 0, part])
        own_kt[:head, kpart] = jnp.transpose(kvbuf[me, 0, kpart])
        own_vt[:head, kpart] = jnp.transpose(kvbuf[me, 1, kpart])

    for d, dest in enumerate(dests):
        @pl.when(dest < me)
        def _():
            aux_copy(me, dest, own_aux_send.at[d]).start()
    for n in range(1, CHUNKS):
        for d in (1, 2):
            pl.when(dests[d] < me)(functools.partial(send_rows, d, n))

    def own_tiles():
        sums = {}
        for rb in range(CHUNKS):
            rpart = pl.ds(rb * qc, qc)
            aux = own_aux[rpart]
            q, do = beside(qbuf[me, 0, rpart], aux), beside(qbuf[me, 1, rpart], aux)
            for cb in range(rb + 1):
                cpart = pl.ds(cb * kc, kc)

                def first(q=q, do=do, cpart=cpart):
                    return dot(q, own_kt[:, cpart]), dot(do, own_vt[:, cpart])

                def second(s, d, rb=rb, cb=cb, rpart=rpart, cpart=cpart):
                    p = jnp.exp2(s * exp_scale)
                    if cb == rb:
                        row = lax.broadcasted_iota(jnp.int32, (qc, kc), 0)
                        col = lax.broadcasted_iota(jnp.int32, (qc, kc), 1)
                        p = jnp.where(2 * col <= row, p, 0.0)
                    ds = (p * d).astype(BF16)
                    dv, dk = dot(own_dot[:head, rpart], p.astype(BF16)), dot(own_qt[:head, rpart], ds)
                    if cb == rb:
                        dv_t[:, cpart] = dv
                        dk_t[:, cpart] = dk
                    else:
                        dv_t[:, cpart] += dv
                        dk_t[:, cpart] += dk
                    dq = dot(ds, kvbuf[me, 0, cpart])
                    sums[rb] = sums[rb] + dq if rb in sums else dq
                    if cb == rb:
                        dq_acc[rpart] = sums[rb]

                yield first, second

    def run(tiles, lead):
        waiting = []
        for first, second in tiles:
            waiting.append((second, first()))
            if len(waiting) > lead:
                second, values = waiting.pop(0)
                second(*values)
        for second, values in waiting:
            second(*values)

    run(own_tiles(), LEAD_D)

    def plan(t):
        na, ka = (t - 2) // 2, t % 2
        early = t < 2
        hop = jnp.where(ka == 1, other, 0)
        stream_a = jnp.where(early | (ka == 1), 3, 0)
        stream_b = jnp.where(early | (ka == 1), 3, 1)
        src_a = jnp.where(early, pair, nx + hop)
        src_b = jnp.where(early, pair, ny + hop)
        piece_a = jnp.where(early, 2 * t, (na + 2) % CHUNKS)
        piece_b = jnp.where(early, 2 * t + 1, na)
        swap = (src_a > me) & (src_b < me)

        def swapped(a, b):
            return jnp.where(swap, b, a), jnp.where(swap, a, b)

        stream_a, stream_b = swapped(stream_a, stream_b)
        src_a, src_b = swapped(src_a, src_b)
        piece_a, piece_b = swapped(piece_a, piece_b)
        return (stream_a, src_a, piece_a), (stream_b, src_b, piece_b)

    def last_plan(t):
        n = t // 2
        src = diag + jnp.where(t % 2 == 1, other, 0)
        half_a = jnp.where(mid, 2 * n, n)
        half_b = jnp.where(mid, 2 * n + 1, n + CHUNKS)
        return src, (half_a, half_b)

    def arrive(item):
        stream, src, piece = item
        idx = jnp.minimum(stream, 1)
        recv = recv_sem.at[src, piece]
        to_x = (stream == 1) & (jnp.logical_not(mid) | (piece < 2))
        to_y = (stream == 0) & mid & (piece >= 2)
        for make, want in ((q_copy, src > me), (kv_copy, src < me)):
            @pl.when(want)
            def _():
                make(src, piece, me, x_send, recv).wait_recv()

                @pl.when(to_x)
                def _():
                    for h in range(2):
                        half = 2 * piece + h
                        make(src, half, nx, x_send, half_recv.at[src, half], 2).start()

                @pl.when(to_y)
                def _():
                    for h in range(2):
                        half = 2 * piece + h
                        make(src, half, ny, y_send, half_recv.at[src, half], 2).start()

                @pl.when(stream < 3)
                def _():
                    make(src, piece, pair, pair_send.at[idx], recv).start()

    def arrive_half(t, src, half):
        recv = half_recv.at[src, half]
        for make, want in ((q_copy, src > me), (kv_copy, src < me)):
            @pl.when(want)
            def _():
                make(src, half, me, x_send, recv, 2).wait_recv()

                @pl.when(t % 2 == 0)
                def _():
                    make(src, half, pair, pair_send.at[2], recv, 2).start()

    def keys_grads(items, cur, size):
        loaded = []
        for idx, src, piece in items:
            part = pl.ds(pl.multiple_of(piece * size, size), size)
            q, do, aux = qbuf[src, 0, part], qbuf[src, 1, part], chunk_aux[cur, idx, :size]
            q_t[idx, :, :size] = jnp.transpose(q)
            do_t[idx, :, :size] = jnp.transpose(do)
            loaded.append((idx, beside(q, aux), beside(do, aux)))
        sums = {}
        last = (items[-1][0], size - min(size, ROWS_Q))
        for cb in range(keys // COLS):
            cpart = pl.ds(cb * COLS, COLS)
            for idx, q, do in loaded:
                for at in range(0, size, ROWS_Q):
                    part = slice(at, min(size, at + ROWS_Q))

                    def first(q=q, do=do, part=part, cpart=cpart):
                        return dot(q[part], own_kt[:, cpart]), dot(do[part], own_vt[:, cpart])

                    def second(s, d, idx=idx, part=part, cpart=cpart, cb=cb):
                        p = jnp.exp2(s * exp_scale)
                        ds = (p * d).astype(BF16)
                        dv, dk = dot(do_t[idx, :, part], p.astype(BF16)), dot(q_t[idx, :, part], ds)
                        if cb in sums:
                            dv, dk = sums[cb][0] + dv, sums[cb][1] + dk
                        sums[cb] = (dv, dk)
                        if (idx, part.start) == last:
                            dv_t[:, cpart] += dv
                            dk_t[:, cpart] += dk

                    yield first, second

    def rows_grad(items, width, size):
        ks, vs = [], []
        for idx, src, piece in items:
            part = pl.ds(pl.multiple_of(piece * size, size), size)
            ks.append(kvbuf[src, 0, part])
            vs.append(kvbuf[src, 1, part])
        k_ts = [jnp.transpose(k) for k in ks]
        k = jnp.concatenate([beside(k, k_one[:size]) for k in ks], axis=0)
        v = jnp.concatenate([beside(v, v_one[:size]) for v in vs], axis=0)
        k_t = k_ts[0] if len(k_ts) == 1 else beside(*k_ts)
        for rb in range(rows // width):
            part = pl.ds(rb * width, width)

            def first(part=part):
                return dot(k, own_qt[:, part]), dot(v, own_dot[:, part])

            def second(s, d, part=part):
                ds = (jnp.exp2(s * exp_scale) * d).astype(BF16)
                dq_t[:, part] += dot(k_t, ds)

            yield first, second

    def mixed(xs, ys):
        xs, ys = list(xs), list(ys)
        for i in range(max(len(xs), len(ys))):
            yield from xs[i:i + 1]
            yield from ys[i:i + 1]

    def present(src):
        return jnp.where(src > me, src, me)

    def ahead(t, slot):
        for idx, (_, src, piece) in enumerate(plan(t)):
            fill_aux(aux_lines(present(src), piece), chunk_aux.at[slot, idx])

    def last_ahead(t, slot):
        src, halves = last_plan(t)
        for idx, half in enumerate(halves):
            fill_aux(half_lines(present(src), half), chunk_aux.at[slot, idx])

    def take_lines(src, to_pair=None):
        @pl.when(src > me)
        def _():
            aux_copy(src, me, x_aux_send).wait_recv()
            if to_pair is not None:
                aux_copy(src, pair, pair_aux_send.at[to_pair]).start()

    take_lines(pair)

    @pl.when(pair > me)
    def _():
        ahead(0, 0)

    def step(t, _):
        a, b = plan(t)
        cur = t % 2

        @pl.when(t == 1)
        def _():
            take_lines(nx, 0)
            take_lines(ny, 1)

            @pl.when(ny > me)
            def _():
                aux_copy(ny, nx, x_aux_send).start()

        @pl.when(t == 2)
        def _():
            take_lines(nx + other)
            take_lines(ny + other)

        arrive(a)
        arrive(b)
        a_keys, b_keys = a[1] < me, b[1] < me
        later = jnp.minimum(t + 1, STEPS - 1)
        a, b = (0,) + a[1:], (1,) + b[1:]

        @pl.when(jnp.logical_not(a_keys))
        def _():
            run(keys_grads((a, b), cur, qc), LEAD_Q)
            ahead(later, 1 - cur)

        @pl.when(a_keys & b_keys)
        def _():
            run(rows_grad((a, b), WIDTH_K, kc), LEAD_K)
            ahead(later, 1 - cur)

        @pl.when(a_keys & jnp.logical_not(b_keys))
        def _():
            run(mixed(rows_grad((a,), WIDTH_M, kc), keys_grads((b,), cur, qc)), LEAD_M)
            ahead(later, 1 - cur)

        return 0

    lax.fori_loop(0, STEPS, step, 0)

    def finish_rows():
        dq_ref[...] = ((dq_acc[...] + jnp.transpose(dq_t[...])) * scale).astype(BF16)

    def finish_keys():
        dk_ref[...] = (jnp.transpose(dk_t[...]) * scale).astype(BF16)
        dv_ref[...] = jnp.transpose(dv_t[...]).astype(BF16)

    take_lines(diag, 2)
    def left(buf, slot, length, send, want):
        @pl.when(want)
        def _():
            block = buf.at[slot, :, pl.ds(0, length)]
            pltpu.make_async_remote_copy(block, block, send, recv_sem.at[slot, 0],
                                         device_id={'cp': pair}, device_id_type=MESH).wait_send()

    sides = ((qbuf, rows, 1), (kvbuf, keys, -1))
    for buf, size, sign in sides:
        for d, dest in enumerate(dests):
            left(buf, me, size, own_send.at[d], sign * dest < sign * me)
        for d, src in enumerate((nx, ny)):
            left(buf, src, size, pair_send.at[d], sign * src > sign * me)
    for d, dest in enumerate(dests):
        @pl.when(dest < me)
        def _():
            aux_copy(me, dest, own_aux_send.at[d]).wait_send()
    for d, src in enumerate((nx, ny)):
        @pl.when(src > me)
        def _():
            aux_copy(src, pair, pair_aux_send.at[d]).wait_send()

            if d == 1:
                aux_copy(src, nx, x_aux_send).wait_send()

    @pl.when(diag > me)
    def _():
        last_ahead(0, 0)
        finish_rows()

    @pl.when(diag < me)
    def _():
        finish_keys()

    take_lines(diag + other)

    def last_step(t, _):
        src, halves = last_plan(t)
        cur = t % 2
        for half in halves:
            arrive_half(t, src, half)
        items = [(idx, src, half) for idx, half in enumerate(halves)]

        @pl.when(src > me)
        def _():
            run(keys_grads(items, cur, qc // 2), LEAD_Q)
            last_ahead(jnp.minimum(t + 1, LAST_STEPS - 1), 1 - cur)

        @pl.when(src < me)
        def _():
            run(rows_grad(items, WIDTH_K, kc // 2), LEAD_K)

        return 0

    lax.fori_loop(0, LAST_STEPS, last_step, 0)

    @pl.when(diag > me)
    def _():
        finish_keys()

    @pl.when(diag < me)
    def _():
        finish_rows()

    for buf, size, sign in sides:
        left(buf, diag, size, pair_send.at[2], sign * diag > sign * me)
        left(buf, ny, size, x_send, (sign * ny > sign * me) & jnp.logical_not(mid))
        left(buf, ny, size // 2, x_send, (sign * ny > sign * me) & mid)
        left(buf, nx, size // 2, y_send, (sign * nx > sign * me) & mid)

    @pl.when(diag > me)
    def _():
        aux_copy(diag, pair, pair_aux_send.at[2]).wait_send()


def store(*refs):
    n = len(refs) // 2
    copies = [pltpu.make_async_copy(refs[i], refs[n + i], refs[-1].at[i]) for i in range(n)]
    for c in copies:
        c.start()
    for c in copies:
        c.wait()


def solution(mesh):
    n_dev = mesh.shape['cp']
    row_spec = P(('dp', 'cp'))

    def local_fn(q_tok, k_tok, v_tok, fwd_out, d_out, lse_row):
        tokens, groups, head = q_tok.shape
        rows = tokens * groups
        piece = rows // CHUNKS
        flat = lambda x: x.reshape(rows, head)
        dma = pltpu.SemaphoreType.DMA
        vmem = pltpu.VMEM
        grad_q, grad_k, grad_v = pl.pallas_call(
            functools.partial(kernel, rows, tokens, head, n_dev),
            out_shape=(jax.ShapeDtypeStruct((rows, head), BF16),
                       jax.ShapeDtypeStruct((tokens, head), BF16),
                       jax.ShapeDtypeStruct((tokens, head), BF16)),
            in_specs=[pl.BlockSpec(memory_space=pltpu.HBM)] * 6,
            out_specs=(pl.BlockSpec(memory_space=vmem),) * 3,
            scratch_shapes=[
                vmem((n_dev, 2, rows, head), BF16),
                vmem((n_dev, 2, tokens, head), BF16),
                vmem((rows, head), BF16),
                vmem((groups, tokens), F32),
                vmem((n_dev, CHUNKS, 8, 128), F32),
                vmem((rows, head), BF16),
                vmem((2, 2, piece, head), BF16),
                vmem((COLS, head), BF16),
                vmem((COLS, head), BF16),
                vmem((2 * head, rows), BF16),
                vmem((2 * head, rows), BF16),
                vmem((2 * head, tokens), BF16),
                vmem((2 * head, tokens), BF16),
                vmem((2, head, piece), BF16),
                vmem((2, head, piece), BF16),
                vmem((rows, head), F32),
                vmem((head, rows), F32),
                vmem((head, tokens), F32),
                vmem((head, tokens), F32),
                dma((6,)),
                dma((n_dev, CHUNKS)),
                dma((n_dev, 2 * CHUNKS)),
                dma((n_dev,)),
                dma((3,)),
                dma((3,)),
                dma((3,)),
                dma((3,)),
                dma,
                dma,
                dma,
            ],
            compiler_params=pltpu.CompilerParams(
                collective_id=0, has_side_effects=True, vmem_limit_bytes=48 * 1024 * 1024),
            name='attention_backward',
        )(*[pltpu.with_memory_space_constraint(x, pltpu.HBM) for x in (flat(q_tok), k_tok, v_tok, flat(fwd_out), flat(d_out), lse_row.T)])
        grads = (grad_q, grad_k, grad_v)
        any_space = pl.BlockSpec(memory_space=pl.ANY)
        grad_q, grad_k, grad_v = pl.pallas_call(
            store,
            out_shape=tuple(jax.ShapeDtypeStruct(g.shape, g.dtype) for g in grads),
            in_specs=[any_space] * 3,
            out_specs=(any_space,) * 3,
            scratch_shapes=[dma((3,))],
            compiler_params=pltpu.CompilerParams(vmem_limit_bytes=1024 * 1024),
            name='store_grads',
        )(*[pltpu.with_memory_space_constraint(g, vmem) for g in grads])
        return grad_q.reshape(tokens, groups, head), grad_k, grad_v

    return jax.shard_map(local_fn, mesh=mesh, in_specs=(row_spec,) * 6, out_specs=(row_spec,) * 3, check_vma=False)
```

```python
import functools
import math

import jax
import jax.numpy as jnp
from jax import lax
from jax.experimental import pallas as pl
from jax.experimental.pallas import tpu as pltpu
from jax.sharding import PartitionSpec as P

BF16, F32 = jnp.bfloat16, jnp.float32
CHUNKS = 4
COLS = 256
STEPS, LAST_STEPS = 10, 8
LEAD_Q, LEAD_K, LEAD_M = 4, 4, 2
LEAD_D = 2
LEAD_LQ, LEAD_LK, WIDTH_L = 6, 3, 512
ROWS_Q = 512
WIDTH_K, WIDTH_M = 256, 512
MESH = pl.DeviceIdType.MESH


def dot(a, b):
    return jnp.dot(a, b, preferred_element_type=F32)


def beside(a, b):
    return jnp.concatenate([a, b], axis=1)


def parts(x):
    hi = x.astype(BF16).astype(F32)
    rest = x - hi
    md = rest.astype(BF16).astype(F32)
    return hi, md, rest - md


def kernel(rows, keys, head, n_dev, q_hbm, k_hbm, v_hbm, o_hbm, do_hbm, lse_hbm, dq_ref, dk_ref, dv_ref,
           qbuf, kvbuf, obuf, lse_in, auxr, own_aux, chunk_aux, k_one, v_one, own_qt, own_dot, own_kt, own_vt,
           q_t, do_t, dq_acc, dq_t, dk_t, dv_t,
           stage_sem, recv_sem, half_recv, aux_recv, own_send, own_aux_send, pair_send, pair_aux_send, x_send, y_send, x_aux_send):
    me = lax.axis_index('cp')
    core, px, py = me % 2, (me // 2) % 2, me // 4
    pair = me + 1 - 2 * core
    nx = me + 2 - 4 * px
    ny = me + 4 - 8 * py
    diag = nx + 4 - 8 * py
    other = pair - me
    mid = (px + py) == 1
    qc, kc = rows // CHUNKS, keys // CHUNKS
    scale = head ** -0.5
    exp_scale = scale * math.log2(math.e)

    def q_copy(slot, n, dest, send, recv, halves=1):
        part = pl.ds(n * (qc // halves), qc // halves)
        return pltpu.make_async_remote_copy(
            qbuf.at[slot, :, part], qbuf.at[slot, :, part], send, recv,
            device_id={'cp': dest}, device_id_type=MESH)

    def kv_copy(slot, n, dest, send, recv, halves=1):
        part = pl.ds(n * (kc // halves), kc // halves)
        return pltpu.make_async_remote_copy(
            kvbuf.at[slot, :, part], kvbuf.at[slot, :, part], send, recv,
            device_id={'cp': dest}, device_id_type=MESH)

    def aux_copy(slot, dest, send):
        return pltpu.make_async_remote_copy(
            auxr.at[slot], auxr.at[slot], send, aux_recv.at[slot],
            device_id={'cp': dest}, device_id_type=MESH)

    stages = [
        pltpu.make_async_copy(q_hbm, qbuf.at[me, 0], stage_sem.at[0]),
        pltpu.make_async_copy(do_hbm, qbuf.at[me, 1], stage_sem.at[1]),
        pltpu.make_async_copy(k_hbm, kvbuf.at[me, 0], stage_sem.at[2]),
        pltpu.make_async_copy(v_hbm, kvbuf.at[me, 1], stage_sem.at[3]),
        pltpu.make_async_copy(o_hbm, obuf, stage_sem.at[4]),
        pltpu.make_async_copy(lse_hbm, lse_in, stage_sem.at[5]),
    ]
    for s in stages:
        s.start()

    barrier = pltpu.get_barrier_semaphore()
    for peer in (nx, ny, pair):
        pl.semaphore_signal(barrier, inc=1, device_id={'cp': peer}, device_id_type=MESH)
    pl.semaphore_wait(barrier, 3)

    def order(d, n):
        return (n + 2) % CHUNKS if d == 1 else n

    dests = (pair, nx, ny)
    for s in stages[:2]:
        s.wait()
    def send_keys(d, n):
        c = order(d, n)
        kv_copy(me, c, dests[d], own_send.at[d], recv_sem.at[me, c]).start()

    def send_rows(d, n):
        c = order(d, n)
        q_copy(me, c, dests[d], own_send.at[d], recv_sem.at[me, c]).start()

    for d in (1, 2):
        pl.when(dests[d] < me)(functools.partial(send_rows, d, 0))
    for s in stages[2:4]:
        s.wait()
    for n in range(CHUNKS):
        for d in (1, 2, 0):
            pl.when(dests[d] > me)(functools.partial(send_keys, d, n))
    pl.when(pair < me)(functools.partial(send_rows, 0, 0))

    for s in stages[4:]:
        s.wait()

    def aux_lines(slot, n):
        hi, md, lo = parts(auxr[slot, n])
        return [stack_lines((hi[g:g + 1], md[g:g + 1], lo[g:g + 1], hi[4 + g:5 + g], md[4 + g:5 + g], lo[4 + g:5 + g]))
                for g in range(qc // 128)]

    def half_lines(slot, half):
        n, at = half // 2, (half % 2) * 2
        return [stack_lines(parts(auxr[slot, n, pl.ds(at + g, 1)]) + parts(auxr[slot, n, pl.ds(4 + at + g, 1)]))
                for g in range(qc // 256)]

    def stack_lines(lines):
        sub = lax.broadcasted_iota(jnp.int32, (8, 128), 0)
        m = jnp.zeros((8, 128), F32)
        for i, line in enumerate(lines):
            m = jnp.where(sub == i, line, m)
        return m

    def fill_aux(lines, dst):
        for g, m in enumerate(lines):
            m = jnp.concatenate([m, jnp.zeros((120, 128), F32)], axis=0)
            dst[pl.ds(g * 128, 128)] = jnp.transpose(m).astype(BF16)

    at_row = lax.broadcasted_iota(jnp.int32, (COLS, COLS), 0)
    at_col = lax.broadcasted_iota(jnp.int32, (COLS, COLS), 1)
    weave = jnp.where(at_col == 2 * (at_row % 128) + at_row // 128, 1.0, 0.0).astype(BF16)
    sub = lax.broadcasted_iota(jnp.int32, (16, 128), 0)
    for n in range(CHUNKS):
        part = pl.ds(n * qc, qc)
        do_turned = jnp.transpose(qbuf[me, 1, part])
        own_dot[:head, part] = do_turned
        sums = jnp.sum(do_turned.astype(F32) * jnp.transpose(obuf[part]).astype(F32), axis=0, keepdims=True)
        for g in range(qc // 128):
            auxr[me, n, 4 + g:5 + g] = sums[:, g * 128:(g + 1) * 128]
        for g in range(qc // 256):
            sides = []
            for h in range(2):
                at = n * (qc // 2) + g * 128
                hi, md, lo = parts(lse_in[h:h + 1, at:at + 128] * (1.0 / scale))
                sides.append(jnp.where(sub == 0, hi, jnp.where(sub == 1, md, jnp.where(sub == 2, lo, 0.0))))
            woven = dot(beside(*sides).astype(BF16), weave)
            row = woven[0:1] + (woven[1:2] + woven[2:3])
            auxr[me, n, 2 * g:2 * g + 1] = row[:, 0:128]
            auxr[me, n, 2 * g + 1:2 * g + 2] = row[:, 128:256]

    for n in range(1, CHUNKS):
        pl.when(pair < me)(functools.partial(send_rows, 0, n))

    lane = lax.broadcasted_iota(jnp.int32, (COLS, head), 1)
    line = lax.broadcasted_iota(jnp.int32, (head, keys), 0)
    k_one[...] = jnp.where(lane < 3, -1.0, 0.0).astype(BF16)
    v_one[...] = jnp.where((lane >= 3) & (lane < 6), -1.0, 0.0).astype(BF16)
    own_kt[head:] = jnp.where(line < 3, -1.0, 0.0).astype(BF16)
    own_vt[head:] = jnp.where((line >= 3) & (line < 6), -1.0, 0.0).astype(BF16)
    dq_t[...] = jnp.zeros_like(dq_t)
    for n in range(CHUNKS):
        part, kpart = pl.ds(n * qc, qc), pl.ds(n * kc, kc)
        lines = aux_lines(me, n)
        fill_aux(lines, own_aux.at[part])
        for g, m in enumerate(lines):
            m = jnp.concatenate([m, jnp.zeros((120, 128), F32)], axis=0).astype(BF16)
            own_qt[head:, pl.ds(n * qc + g * 128, 128)] = m
            own_dot[head:, pl.ds(n * qc + g * 128, 128)] = m
        own_qt[:head, part] = jnp.transpose(qbuf[me, 0, part])
        own_kt[:head, kpart] = jnp.transpose(kvbuf[me, 0, kpart])
        own_vt[:head, kpart] = jnp.transpose(kvbuf[me, 1, kpart])

    for d, dest in enumerate(dests):
        @pl.when(dest < me)
        def _():
            aux_copy(me, dest, own_aux_send.at[d]).start()
    for n in range(1, CHUNKS):
        for d in (1, 2):
            pl.when(dests[d] < me)(functools.partial(send_rows, d, n))

    def own_tiles():
        sums = {}
        for rb in range(CHUNKS):
            rpart = pl.ds(rb * qc, qc)
            aux = own_aux[rpart]
            q, do = beside(qbuf[me, 0, rpart], aux), beside(qbuf[me, 1, rpart], aux)
            for cb in range(rb + 1):
                cpart = pl.ds(cb * kc, kc)

                def first(q=q, do=do, cpart=cpart):
                    return dot(q, own_kt[:, cpart]), dot(do, own_vt[:, cpart])

                def second(s, d, rb=rb, cb=cb, rpart=rpart, cpart=cpart):
                    p = jnp.exp2(s * exp_scale)
                    if cb == rb:
                        row = lax.broadcasted_iota(jnp.int32, (qc, kc), 0)
                        col = lax.broadcasted_iota(jnp.int32, (qc, kc), 1)
                        p = jnp.where(2 * col <= row, p, 0.0)
                    ds = (p * d).astype(BF16)
                    dv, dk = dot(own_dot[:head, rpart], p.astype(BF16)), dot(own_qt[:head, rpart], ds)
                    if cb == rb:
                        dv_t[:, cpart] = dv
                        dk_t[:, cpart] = dk
                    else:
                        dv_t[:, cpart] += dv
                        dk_t[:, cpart] += dk
                    dq = dot(ds, kvbuf[me, 0, cpart])
                    sums[rb] = sums[rb] + dq if rb in sums else dq
                    if cb == rb:
                        dq_acc[rpart] = sums[rb]

                yield first, second

    def run(tiles, lead):
        waiting = []
        for first, second in tiles:
            waiting.append((second, first()))
            if len(waiting) > lead:
                second, values = waiting.pop(0)
                second(*values)
        for second, values in waiting:
            second(*values)

    run(own_tiles(), LEAD_D)

    def plan(t):
        na, ka = (t - 2) // 2, t % 2
        early = t < 2
        hop = jnp.where(ka == 1, other, 0)
        stream_a = jnp.where(early | (ka == 1), 3, 0)
        stream_b = jnp.where(early | (ka == 1), 3, 1)
        src_a = jnp.where(early, pair, nx + hop)
        src_b = jnp.where(early, pair, ny + hop)
        piece_a = jnp.where(early, 2 * t, (na + 2) % CHUNKS)
        piece_b = jnp.where(early, 2 * t + 1, na)
        swap = (src_a > me) & (src_b < me)

        def swapped(a, b):
            return jnp.where(swap, b, a), jnp.where(swap, a, b)

        stream_a, stream_b = swapped(stream_a, stream_b)
        src_a, src_b = swapped(src_a, src_b)
        piece_a, piece_b = swapped(piece_a, piece_b)
        return (stream_a, src_a, piece_a), (stream_b, src_b, piece_b)

    def last_plan(t):
        n = t // 2
        src = diag + jnp.where(t % 2 == 1, other, 0)
        half_a = jnp.where(mid, 2 * n, n)
        half_b = jnp.where(mid, 2 * n + 1, n + CHUNKS)
        return src, (half_a, half_b)

    def arrive(item):
        stream, src, piece = item
        idx = jnp.minimum(stream, 1)
        recv = recv_sem.at[src, piece]
        to_x = (stream == 1) & (jnp.logical_not(mid) | (piece < 2))
        to_y = (stream == 0) & mid & (piece >= 2)
        for make, want in ((q_copy, src > me), (kv_copy, src < me)):
            @pl.when(want)
            def _():
                make(src, piece, me, x_send, recv).wait_recv()

                @pl.when(to_x)
                def _():
                    for h in range(2):
                        half = 2 * piece + h
                        make(src, half, nx, x_send, half_recv.at[src % 2, half], 2).start()

                @pl.when(to_y)
                def _():
                    for h in range(2):
                        half = 2 * piece + h
                        make(src, half, ny, y_send, half_recv.at[src % 2, half], 2).start()

                @pl.when(stream < 3)
                def _():
                    make(src, piece, pair, pair_send.at[idx], recv).start()

    def arrive_half(t, src, half):
        recv = half_recv.at[src % 2, half]
        for make, want in ((q_copy, src > me), (kv_copy, src < me)):
            @pl.when(want)
            def _():
                make(src, half, me, x_send, recv, 2).wait_recv()

                @pl.when(t % 2 == 0)
                def _():
                    make(src, half, pair, pair_send.at[2], recv, 2).start()

    def keys_grads(items, cur, size):
        loaded = []
        for idx, src, piece in items:
            part = pl.ds(pl.multiple_of(piece * size, size), size)
            q, do, aux = qbuf[src, 0, part], qbuf[src, 1, part], chunk_aux[cur, idx, :size]
            q_t[idx, :, :size] = jnp.transpose(q)
            do_t[idx, :, :size] = jnp.transpose(do)
            loaded.append((idx, beside(q, aux), beside(do, aux)))
        sums = {}
        last = (items[-1][0], size - min(size, ROWS_Q))
        for cb in range(keys // COLS):
            cpart = pl.ds(cb * COLS, COLS)
            for idx, q, do in loaded:
                for at in range(0, size, ROWS_Q):
                    part = slice(at, min(size, at + ROWS_Q))

                    def first(q=q, do=do, part=part, cpart=cpart):
                        return dot(q[part], own_kt[:, cpart]), dot(do[part], own_vt[:, cpart])

                    def second(s, d, idx=idx, part=part, cpart=cpart, cb=cb):
                        p = jnp.exp2(s * exp_scale)
                        ds = (p * d).astype(BF16)
                        dv, dk = dot(do_t[idx, :, part], p.astype(BF16)), dot(q_t[idx, :, part], ds)
                        if cb in sums:
                            dv, dk = sums[cb][0] + dv, sums[cb][1] + dk
                        sums[cb] = (dv, dk)
                        if (idx, part.start) == last:
                            dv_t[:, cpart] += dv
                            dk_t[:, cpart] += dk

                    yield first, second

    def rows_grad(items, width, size):
        ks, vs = [], []
        for idx, src, piece in items:
            part = pl.ds(pl.multiple_of(piece * size, size), size)
            ks.append(kvbuf[src, 0, part])
            vs.append(kvbuf[src, 1, part])
        k_ts = [jnp.transpose(k) for k in ks]
        k = jnp.concatenate([beside(k, k_one[:size]) for k in ks], axis=0)
        v = jnp.concatenate([beside(v, v_one[:size]) for v in vs], axis=0)
        k_t = k_ts[0] if len(k_ts) == 1 else beside(*k_ts)
        for rb in range(rows // width):
            part = pl.ds(rb * width, width)

            def first(part=part):
                return dot(k, own_qt[:, part]), dot(v, own_dot[:, part])

            def second(s, d, part=part):
                ds = (jnp.exp2(s * exp_scale) * d).astype(BF16)
                dq_t[:, part] += dot(k_t, ds)

            yield first, second

    def mixed(xs, ys):
        xs, ys = list(xs), list(ys)
        for i in range(max(len(xs), len(ys))):
            yield from xs[i:i + 1]
            yield from ys[i:i + 1]

    def present(src):
        return jnp.where(src > me, src, me)

    def ahead(t, slot):
        for idx, (_, src, piece) in enumerate(plan(t)):
            fill_aux(aux_lines(present(src), piece), chunk_aux.at[slot, idx])

    def last_ahead(t, slot):
        src, halves = last_plan(t)
        for idx, half in enumerate(halves):
            fill_aux(half_lines(present(src), half), chunk_aux.at[slot, idx])

    def take_lines(src, to_pair=None):
        @pl.when(src > me)
        def _():
            aux_copy(src, me, x_aux_send).wait_recv()
            if to_pair is not None:
                aux_copy(src, pair, pair_aux_send.at[to_pair]).start()

    take_lines(pair)

    @pl.when(pair > me)
    def _():
        ahead(0, 0)

    def step(t, _):
        a, b = plan(t)
        cur = t % 2

        @pl.when(t == 1)
        def _():
            take_lines(nx, 0)
            take_lines(ny, 1)

            @pl.when(ny > me)
            def _():
                aux_copy(ny, nx, x_aux_send).start()

        @pl.when(t == 2)
        def _():
            take_lines(nx + other)
            take_lines(ny + other)

        arrive(a)
        arrive(b)
        a_keys, b_keys = a[1] < me, b[1] < me
        later = jnp.minimum(t + 1, STEPS - 1)
        a, b = (0,) + a[1:], (1,) + b[1:]

        @pl.when(jnp.logical_not(a_keys))
        def _():
            run(keys_grads((a, b), cur, qc), LEAD_Q)
            ahead(later, 1 - cur)

        @pl.when(a_keys & b_keys)
        def _():
            run(rows_grad((a, b), WIDTH_K, kc), LEAD_K)
            ahead(later, 1 - cur)

        @pl.when(a_keys & jnp.logical_not(b_keys))
        def _():
            run(mixed(rows_grad((a,), WIDTH_M, kc), keys_grads((b,), cur, qc)), LEAD_M)
            ahead(later, 1 - cur)

        return 0

    lax.fori_loop(0, STEPS, step, 0)

    def finish_rows():
        dq_ref[...] = ((dq_acc[...] + jnp.transpose(dq_t[...])) * scale).astype(BF16)

    def finish_keys():
        dk_ref[...] = (jnp.transpose(dk_t[...]) * scale).astype(BF16)
        dv_ref[...] = jnp.transpose(dv_t[...]).astype(BF16)

    take_lines(diag, 2)
    def left(buf, slot, length, send, want):
        @pl.when(want)
        def _():
            block = buf.at[slot, :, pl.ds(0, length)]
            pltpu.make_async_remote_copy(block, block, send, recv_sem.at[slot, 0],
                                         device_id={'cp': pair}, device_id_type=MESH).wait_send()

    sides = ((qbuf, rows, 1), (kvbuf, keys, -1))
    for buf, size, sign in sides:
        for d, dest in enumerate(dests):
            left(buf, me, size, own_send.at[d], sign * dest < sign * me)
        for d, src in enumerate((nx, ny)):
            left(buf, src, size, pair_send.at[d], sign * src > sign * me)
    for d, dest in enumerate(dests):
        @pl.when(dest < me)
        def _():
            aux_copy(me, dest, own_aux_send.at[d]).wait_send()
    for d, src in enumerate((nx, ny)):
        @pl.when(src > me)
        def _():
            aux_copy(src, pair, pair_aux_send.at[d]).wait_send()

            if d == 1:
                aux_copy(src, nx, x_aux_send).wait_send()

    @pl.when(diag > me)
    def _():
        last_ahead(0, 0)
        finish_rows()

    @pl.when(diag < me)
    def _():
        finish_keys()

    take_lines(diag + other)

    def last_step(t, _):
        src, halves = last_plan(t)
        cur = t % 2
        for half in halves:
            arrive_half(t, src, half)
        items = [(idx, src, half) for idx, half in enumerate(halves)]

        @pl.when(src > me)
        def _():
            run(keys_grads(items, cur, qc // 2), LEAD_LQ)
            last_ahead(jnp.minimum(t + 1, LAST_STEPS - 1), 1 - cur)

        @pl.when(src < me)
        def _():
            run(rows_grad(items, WIDTH_L, kc // 2), LEAD_LK)

        return 0

    lax.fori_loop(0, LAST_STEPS, last_step, 0)

    @pl.when(diag > me)
    def _():
        finish_keys()

    @pl.when(diag < me)
    def _():
        finish_rows()

    for buf, size, sign in sides:
        left(buf, diag, size, pair_send.at[2], sign * diag > sign * me)
        left(buf, ny, size, x_send, (sign * ny > sign * me) & jnp.logical_not(mid))
        left(buf, ny, size // 2, x_send, (sign * ny > sign * me) & mid)
        left(buf, nx, size // 2, y_send, (sign * nx > sign * me) & mid)

    @pl.when(diag > me)
    def _():
        aux_copy(diag, pair, pair_aux_send.at[2]).wait_send()


def store(*refs):
    n = len(refs) // 2
    copies = [pltpu.make_async_copy(refs[i], refs[n + i], refs[-1].at[i]) for i in range(n)]
    for c in copies:
        c.start()
    for c in copies:
        c.wait()


def solution(mesh):
    n_dev = mesh.shape['cp']
    row_spec = P(('dp', 'cp'))

    def local_fn(q_tok, k_tok, v_tok, fwd_out, d_out, lse_row):
        tokens, groups, head = q_tok.shape
        rows = tokens * groups
        piece = rows // CHUNKS
        flat = lambda x: x.reshape(rows, head)
        dma = pltpu.SemaphoreType.DMA
        vmem = pltpu.VMEM
        grad_q, grad_k, grad_v = pl.pallas_call(
            functools.partial(kernel, rows, tokens, head, n_dev),
            out_shape=(jax.ShapeDtypeStruct((rows, head), BF16),
                       jax.ShapeDtypeStruct((tokens, head), BF16),
                       jax.ShapeDtypeStruct((tokens, head), BF16)),
            in_specs=[pl.BlockSpec(memory_space=pltpu.HBM)] * 6,
            out_specs=(pl.BlockSpec(memory_space=vmem),) * 3,
            scratch_shapes=[
                vmem((n_dev, 2, rows, head), BF16),
                vmem((n_dev, 2, tokens, head), BF16),
                vmem((rows, head), BF16),
                vmem((groups, tokens), F32),
                vmem((n_dev, CHUNKS, 8, 128), F32),
                vmem((rows, head), BF16),
                vmem((2, 2, piece, head), BF16),
                vmem((COLS, head), BF16),
                vmem((COLS, head), BF16),
                vmem((2 * head, rows), BF16),
                vmem((2 * head, rows), BF16),
                vmem((2 * head, tokens), BF16),
                vmem((2 * head, tokens), BF16),
                vmem((2, head, piece), BF16),
                vmem((2, head, piece), BF16),
                vmem((rows, head), F32),
                vmem((head, rows), F32),
                vmem((head, tokens), F32),
                vmem((head, tokens), F32),
                dma((6,)),
                dma((n_dev, CHUNKS)),
                dma((2, 2 * CHUNKS)),
                dma((n_dev,)),
                dma((3,)),
                dma((3,)),
                dma((3,)),
                dma((3,)),
                dma,
                dma,
                dma,
            ],
            compiler_params=pltpu.CompilerParams(
                collective_id=0, has_side_effects=True, vmem_limit_bytes=48 * 1024 * 1024),
            name='attention_backward',
        )(*[pltpu.with_memory_space_constraint(x, pltpu.HBM) for x in (flat(q_tok), k_tok, v_tok, flat(fwd_out), flat(d_out), lse_row.T)])
        grads = (grad_q, grad_k, grad_v)
        any_space = pl.BlockSpec(memory_space=pl.ANY)
        grad_q, grad_k, grad_v = pl.pallas_call(
            store,
            out_shape=tuple(jax.ShapeDtypeStruct(g.shape, g.dtype) for g in grads),
            in_specs=[any_space] * 3,
            out_specs=(any_space,) * 3,
            scratch_shapes=[dma((3,))],
            compiler_params=pltpu.CompilerParams(vmem_limit_bytes=1024 * 1024),
            name='store_grads',
        )(*[pltpu.with_memory_space_constraint(g, vmem) for g in grads])
        return grad_q.reshape(tokens, groups, head), grad_k, grad_v

    return jax.shard_map(local_fn, mesh=mesh, in_specs=(row_spec,) * 6, out_specs=(row_spec,) * 3, check_vma=False)
```
